256 devices in a mesh: group: 16 (over z_hi, x), shard: 16 (over z_lo, y, core).
Axes of the slice: x: 4, y: 4, z: 8 (z_hi: 4, z_lo: 2; z = z_hi * 2 + z_lo), core: 2. Of those that a mesh axis runs over, the one named last changes fastest.
Arguments:
- entity: float32 [131072, 400], P(('group', 'shard')), may hold values from -6 to 6
- entity_state: float32 [131072], P(('group', 'shard')), may hold values from 0.1 to 10
- relation: float32 [1345, 400], replicated, may hold values from -6 to 6
- relation_state: float32 [1345], replicated, may hold values from 10 to 1000
- src_send: int32 [256, 16, 64], P(('group', 'shard')), may hold values from 0 to 511
- dst_send: int32 [256, 16, 64], P(('group', 'shard')), may hold values from 0 to 511
- edge_source: int32 [262144], P(('group', 'shard')), may hold values from 0 to 1023
- edge_relation: int32 [262144], P(('group', 'shard')), may hold values from 0 to 1344
- edge_target: int32 [262144], P(('group', 'shard')), may hold values from 0 to 1023
- neg_slots: int32 [512, 1000], P(('group', 'shard')), may hold values from 0 to 1023
- edge_count: int32 [256], P(('group', 'shard')), may hold values from 1 to 1024, 87381 in all
Outputs:
- entity_new: float32 [131072, 400], P(('group', 'shard'))
- relation_new: float32 [1345, 400], replicated
- edge_loss: float32 [262144], P(('group', 'shard'))
The draws below stay inside these ranges and needn't reach their ends.
Inputs may be any that keep to these rules, and one draw needn't show every extreme that they name: The live edges of a device are its first edge_count slots; some device has all 1024 live.
All inputs are finite; a program needn't handle non-finite values.
Results may differ from the reference program's by a relative error of at most 0.0003.
Values sent between devices are 32-bit elements; how exact they have to be, the bound alone decides.
A program may use at most 128 MiB of HBM per device.

```python
import math
import jax
import jax.numpy as jnp
import numpy as np
from jax import lax

D = 400
NEG = 1000
RELS = 1345
SPAN = 512
ROWS_DEV = 512
EDGES_DEV = 1024
TABLE = 1024
BLOCK = 64
ENTITIES = 131072
EDGES = 262144
SPANS = 512
N_GROUP = 16
N_SHARD = 16
DEVICES = 256


def draw_entity(key, part):
    values = jnp.clip(0.5 * jax.random.normal(jax.random.fold_in(key, 13), (ENTITIES, D), jnp.float32), -3.0, 3.0)
    return values


def plant(entries, key, low, high):
    place = [jax.random.randint(jax.random.fold_in(key, axis), (), 0, length) for axis, length in enumerate(entries.shape)]
    longest = entries.shape.index(max(entries.shape))
    next_to = place[:longest] + [(place[longest] + 1) % entries.shape[longest]] + place[longest + 1:]
    return entries.at[tuple(place)].set(low).at[tuple(next_to)].set(high)


def steps_of(own_key, extent, cuts, smallest, high):
    def one(axis_at, shards_of):
        steps = jax.random.uniform(jax.random.fold_in(jax.random.fold_in(own_key, 6), axis_at), (shards_of,), jnp.float32, smallest / len(cuts), high / len(cuts))
        return jnp.repeat(jnp.exp(steps), extent[axis_at] // shards_of).reshape((-1,) + (1,) * (len(extent) - axis_at - 1))

    gain = one(*cuts[0])
    for cut in cuts[1:]:
        gain = gain * one(*cut)
    return gain


def length_profile(number_of, total, reach, skew):
    weights = [(1 << 20) // math.isqrt(grade ** skew) + 1 for grade in range(2, number_of + 1)]
    rest, counts = total - reach - (number_of - 1), [1] * (number_of - 1)
    while rest > 0:
        free = [i for i in range(number_of - 1) if counts[i] < reach]
        mass, left = sum([weights[i] for i in free]), rest
        for i in free:
            extra = min(reach - counts[i], max(1, left * weights[i] // mass), rest)
            counts[i] = counts[i] + extra
            rest = rest - extra
    return np.array([reach] + counts)


def uneven_parts(own_key, amount, total, reach, slope):
    if amount == 2:
        one = jax.random.randint(own_key, (), max(1, total - reach), min(reach, total - 1) + 1)
        return jnp.stack([one, total - one])
    tallies = jnp.asarray(length_profile(amount, total, reach, slope), jnp.int32)
    twos = (amount - 1) // 2
    giver, sink = tallies[1:1 + 2 * twos:2], tallies[2:2 + 2 * twos:2]
    slack = jnp.minimum(giver - 1, reach - sink)
    moved = jax.random.randint(jax.random.fold_in(own_key, 1), (twos,), 0, 1 << 20) % (slack + 1)
    tallies = tallies.at[1:1 + 2 * twos:2].set(giver - moved).at[2:2 + 2 * twos:2].set(sink + moved)
    return tallies[jax.random.permutation(jax.random.fold_in(own_key, 2), amount)]


def noise(own_key, shape, scale, limit, kind=jnp.bfloat16):
    return jnp.clip(scale * jax.random.normal(own_key, shape, jnp.float32), -limit, limit).astype(kind)


def setup_inputs(seed: int = 0) -> dict:
    arg_keys = jax.random.split(jax.random.key(seed), 12)
    entity = draw_entity(jax.random.fold_in(arg_keys[11], 71), 0)
    entity_state = jnp.clip(jnp.exp(math.log(10.0) - 4.6051702 * jax.random.uniform(arg_keys[1], (ENTITIES,), jnp.float32) ** steps_of(arg_keys[1], (ENTITIES,), ((0, 256),), -0.2, 0.2)), 0.1, 10.0)
    relation = noise(arg_keys[2], (RELS, D), 1.0, 6.0, jnp.float32)
    relation_state = jnp.clip(jnp.exp(jax.random.uniform(arg_keys[3], (RELS,), jnp.float32, math.log(10.0), math.log(1000.0))), 10.0, 1000.0)
    src_send = plant(jax.random.randint(arg_keys[4], (DEVICES, N_SHARD, BLOCK), 0, ROWS_DEV), jax.random.fold_in(arg_keys[4], 1), 0, ROWS_DEV - 1).astype(jnp.int32)
    dst_send = plant(jax.random.randint(arg_keys[5], (DEVICES, N_SHARD, BLOCK), 0, ROWS_DEV), jax.random.fold_in(arg_keys[5], 1), 0, ROWS_DEV - 1).astype(jnp.int32)
    edge_source = plant(jax.random.randint(arg_keys[6], (EDGES,), 0, TABLE), jax.random.fold_in(arg_keys[6], 1), 0, TABLE - 1).astype(jnp.int32)
    edge_relation = plant(jax.random.randint(arg_keys[7], (EDGES,), 0, RELS), jax.random.fold_in(arg_keys[7], 1), 0, RELS - 1).astype(jnp.int32)
    edge_target = plant(jax.random.randint(arg_keys[8], (EDGES,), 0, TABLE), jax.random.fold_in(arg_keys[8], 1), 0, TABLE - 1).astype(jnp.int32)
    neg_slots = plant(jax.random.randint(arg_keys[9], (SPANS, NEG), 0, TABLE), jax.random.fold_in(arg_keys[9], 1), 0, TABLE - 1).astype(jnp.int32)
    edge_count = uneven_parts(arg_keys[10], DEVICES, DEVICES * EDGES_DEV // 3, EDGES_DEV, 2).astype(jnp.int32)
    return dict(entity=entity, entity_state=entity_state, relation=relation, relation_state=relation_state, src_send=src_send, dst_send=dst_send, edge_source=edge_source, edge_relation=edge_relation, edge_target=edge_target, neg_slots=neg_slots, edge_count=edge_count)


learn_rate = 0.5

def complex_product(multiplier, multiplicand):
    half_width = multiplier.shape[1] // 2
    first_real, first_imag = (multiplier[:, :half_width], multiplier[:, half_width:])
    second_real, second_imag = (multiplicand[:, :half_width], multiplicand[:, half_width:])
    return jnp.concatenate([first_real * second_real - first_imag * second_imag, first_real * second_imag + first_imag * second_real], axis=1)

def conj_product(multiplier, multiplicand):
    half_width = multiplier.shape[1] // 2
    first_real, first_imag = (multiplier[:, :half_width], multiplier[:, half_width:])
    second_real, second_imag = (multiplicand[:, :half_width], multiplicand[:, half_width:])
    return jnp.concatenate([first_real * second_real + first_imag * second_imag, first_imag * second_real - first_real * second_imag], axis=1)

def span_terms(queries, tail_rows, negatives, live_mask):
    pos_score = lax.optimization_barrier(jnp.sum(queries * tail_rows, axis=1))
    neg_score = jnp.dot(queries, negatives.T, precision=lax.Precision.HIGHEST)
    score_peak = jnp.maximum(pos_score, lax.optimization_barrier(jnp.max(neg_score, axis=1)))
    exp_total = jnp.exp(pos_score - score_peak) + lax.optimization_barrier(jnp.sum(jnp.exp(neg_score - score_peak[:, None]), axis=1))
    log_total = score_peak + jnp.log(exp_total)
    edge_loss = (log_total - pos_score) * live_mask
    pos_grad = (jnp.exp(pos_score - log_total) - 1.0) * live_mask
    neg_grad = jnp.exp(neg_score - log_total[:, None]) * live_mask[:, None]
    neg_query = jnp.dot(neg_grad, negatives, precision=lax.Precision.HIGHEST)
    negative_grad = lax.dot_general(neg_grad, queries, (((0,), (0,)), ((), ())), precision=lax.Precision.HIGHEST)
    return (edge_loss, pos_grad, neg_query, negative_grad)

def adagrad(params, accumulator, gradient):
    new_state = accumulator + lax.optimization_barrier(jnp.mean(gradient * gradient, axis=1))
    return params - learn_rate * gradient / jnp.sqrt(new_state)[:, None]

def reference(entity, entity_state, relation, relation_state, src_send, dst_send, edge_source, edge_relation, edge_target, neg_slots, edge_count):
    devices = N_GROUP * N_SHARD
    spans = EDGES_DEV // SPAN
    owners = jnp.arange(N_SHARD, dtype=jnp.int32)

    def device_step(carried, device):
        entity_grad, relation_grad = carried
        group_id = device // N_SHARD
        shard_id = device % N_SHARD
        next_group = (group_id + 1) % N_GROUP
        source_owner = group_id * N_SHARD + owners
        target_owner = next_group * N_SHARD + owners
        source_global = (source_owner[:, None] * ROWS_DEV + src_send[source_owner, shard_id, :]).reshape(-1)
        target_global = (target_owner[:, None] * ROWS_DEV + dst_send[target_owner, shard_id, :]).reshape(-1)
        source_table = entity[source_global]
        target_table = entity[target_global]
        first_edge = device * EDGES_DEV
        slot_source = lax.dynamic_slice_in_dim(edge_source, first_edge, EDGES_DEV)
        slot_relation = lax.dynamic_slice_in_dim(edge_relation, first_edge, EDGES_DEV)
        slot_target = lax.dynamic_slice_in_dim(edge_target, first_edge, EDGES_DEV)
        slot_negative = lax.dynamic_slice_in_dim(neg_slots, device * spans, spans, 0)
        live_mask = (jnp.arange(EDGES_DEV, dtype=jnp.int32) < edge_count[device]).astype(jnp.float32)
        head_rows = source_table[slot_source]
        tail_rows = target_table[slot_target]
        rel_rows = relation[slot_relation]
        queries = complex_product(head_rows, rel_rows)

        def per_span(position):
            first_row = position * SPAN
            return span_terms(lax.dynamic_slice_in_dim(queries, first_row, SPAN), lax.dynamic_slice_in_dim(tail_rows, first_row, SPAN), target_table[slot_negative[position]], lax.dynamic_slice_in_dim(live_mask, first_row, SPAN))
        edge_loss, pos_grad, neg_query, negative_grad = lax.map(per_span, jnp.arange(spans, dtype=jnp.int32))
        feature_count = entity.shape[1]
        edge_loss = edge_loss.reshape(-1)
        pos_grad = pos_grad.reshape(-1)
        neg_query = neg_query.reshape(EDGES_DEV, feature_count)
        negative_grad = negative_grad.reshape(spans * NEG, feature_count)
        query_grad = pos_grad[:, None] * tail_rows + neg_query
        tail_grad = pos_grad[:, None] * queries
        entity_grad = entity_grad.at[source_global[slot_source]].add(conj_product(query_grad, rel_rows))
        entity_grad = entity_grad.at[target_global[slot_target]].add(tail_grad)
        entity_grad = entity_grad.at[target_global[slot_negative.reshape(-1)]].add(negative_grad)
        relation_grad = relation_grad.at[slot_relation].add(conj_product(query_grad, head_rows))
        return ((entity_grad, relation_grad), edge_loss)
    initial = (jnp.zeros(entity.shape, jnp.float32), jnp.zeros(relation.shape, jnp.float32))
    (entity_grad, relation_grad), losses = lax.scan(device_step, initial, jnp.arange(devices, dtype=jnp.int32))
    return (adagrad(entity, entity_state, entity_grad), adagrad(relation, relation_state, relation_grad), losses.reshape(-1))
```

```python
import functools

import jax
import jax.numpy as jnp
from jax import lax
from jax.experimental import pallas as pl
from jax.experimental.pallas import tpu as pltpu
from jax.sharding import PartitionSpec as P

SPAN = 512
LEARN_RATE = 0.5
HALF = 256
WIDE = 2 * HALF

NT = (((1,), (1,)), ((), ()))
NN = (((1,), (0,)), ((), ()))
TN = (((0,), (0,)), ((), ()))


def split2(x):
    hi = x.astype(jnp.bfloat16)
    lo = (x - hi.astype(jnp.float32)).astype(jnp.bfloat16)
    return hi, lo


def split3(x):
    hi = x.astype(jnp.bfloat16)
    rest = x - hi.astype(jnp.float32)
    mid = rest.astype(jnp.bfloat16)
    lo = (rest - mid.astype(jnp.float32)).astype(jnp.bfloat16)
    return hi, mid, lo


def mxu(a, b, dims):
    return lax.dot_general(a, b, dims, preferred_element_type=jnp.float32)


def wide(x):
    half = x.shape[1] // 2
    pad = ((0, 0), (0, HALF - half))
    return jnp.concatenate([jnp.pad(x[:, :half], pad), jnp.pad(x[:, half:], pad)], axis=1)


def narrow(x, width):
    half = width // 2
    return jnp.concatenate([x[:, :half], x[:, HALF : HALF + half]], axis=1)


def product(a, b):
    ar, ai, br, bi = a[:, :HALF], a[:, HALF:], b[:, :HALF], b[:, HALF:]
    return jnp.concatenate([ar * br - ai * bi, ar * bi + ai * br], axis=1)


def conj_product(a, b):
    ar, ai, br, bi = a[:, :HALF], a[:, HALF:], b[:, :HALF], b[:, HALF:]
    return jnp.concatenate([ar * br + ai * bi, ai * br - ar * bi], axis=1)


def chosen(index, count):
    lanes = lax.broadcasted_iota(jnp.int32, (index.shape[0], count), 1)
    return jnp.where(lanes == index, 1.0, 0.0).astype(jnp.bfloat16)


def vmem(shape, index_map):
    return pl.BlockSpec(shape, index_map, memory_space=pltpu.VMEM)


def params(limit=48 << 20):
    return pltpu.CompilerParams(vmem_limit_bytes=limit)


def take_kernel(index_ref, table_ref, out_ref, parts_ref):
    @pl.when(pl.program_id(0) == 0)
    def _():
        for k, part in enumerate(split3(table_ref[...])):
            parts_ref[k] = part

    pick = chosen(index_ref[...], table_ref.shape[0])
    out_ref[...] = (
        mxu(pick, parts_ref[0], NN) + mxu(pick, parts_ref[1], NN)
    ) + mxu(pick, parts_ref[2], NN)


def take_rows(table, index):
    rows, count = index.shape[0], table.shape[0]
    tile = min(256, rows)
    return pl.pallas_call(
        take_kernel,
        grid=(rows // tile,),
        in_specs=[vmem((tile, 1), lambda i: (i, 0)), vmem((count, WIDE), lambda i: (0, 0))],
        out_specs=vmem((tile, WIDE), lambda i: (i, 0)),
        out_shape=jax.ShapeDtypeStruct((rows, WIDE), jnp.float32),
        scratch_shapes=[pltpu.VMEM((3, count, WIDE), jnp.bfloat16)],
        compiler_params=params(),
        cost_estimate=pl.CostEstimate(
            flops=6 * rows * count * WIDE, bytes_accessed=4 * (rows + count) * WIDE, transcendentals=0
        ),
        name="take_rows",
    )(index, table)


def query_kernel(index_ref, table_ref, rel_ref, head_ref, query_ref, parts_ref):
    @pl.when(pl.program_id(0) == 0)
    def _():
        for k, part in enumerate(split3(table_ref[...])):
            parts_ref[k] = part

    pick = chosen(index_ref[...], table_ref.shape[0])
    heads = (mxu(pick, parts_ref[0], NN) + mxu(pick, parts_ref[1], NN)) + mxu(pick, parts_ref[2], NN)
    head_ref[...] = heads
    query_ref[...] = product(heads, rel_ref[...])


def make_queries(table, index, rels):
    rows, count = index.shape[0], table.shape[0]
    tile = min(256, rows)
    block = vmem((tile, WIDE), lambda i: (i, 0))
    shape = jax.ShapeDtypeStruct((rows, WIDE), jnp.float32)
    return pl.pallas_call(
        query_kernel,
        grid=(rows // tile,),
        in_specs=[vmem((tile, 1), lambda i: (i, 0)), vmem((count, WIDE), lambda i: (0, 0)), block],
        out_specs=[block, block],
        out_shape=[shape, shape],
        scratch_shapes=[pltpu.VMEM((3, count, WIDE), jnp.bfloat16)],
        compiler_params=params(),
        cost_estimate=pl.CostEstimate(
            flops=6 * rows * count * WIDE, bytes_accessed=4 * (4 * rows + count) * WIDE, transcendentals=0
        ),
        name="make_queries",
    )(index, table, rels)


def span_kernel(
    count_ref, target_ref, slots_ref, query_ref, table_ref,
    loss_ref, query_grad_ref, target_grad_ref,
    score_ref, times_ref, parts_ref, query_parts_ref,
):
    span = pl.program_id(0)
    table_rows = table_ref.shape[0]
    tile = min(256, table_rows)
    tiles = table_rows // tile

    @pl.when(span == 0)
    def _():
        for k, part in enumerate(split3(table_ref[...])):
            parts_ref[k] = part

    for k, part in enumerate(split3(query_ref[...])):
        query_parts_ref[k] = part

    edge = lax.broadcasted_iota(jnp.int32, (1, SPAN), 1) + span * SPAN
    live = jnp.where(edge < count_ref[0], 1.0, 0.0)
    target = target_ref[0]
    slots = slots_ref[0]

    def score_turn(t, carried):
        peak, pos = carried
        rows = pl.ds(pl.multiple_of(t * tile, tile), tile)
        t0, t1, t2 = parts_ref[0, rows], parts_ref[1, rows], parts_ref[2, rows]
        q0, q1, q2 = query_parts_ref[0], query_parts_ref[1], query_parts_ref[2]
        small = mxu(t0, q2, NT) + mxu(t2, q0, NT) + mxu(t1, q1, NT)
        score = (small + (mxu(t0, q1, NT) + mxu(t1, q0, NT))) + mxu(t0, q0, NT)
        score_ref[rows] = score
        number = lax.broadcasted_iota(jnp.int32, (tile, 1), 0) + t * tile
        times = jnp.sum(jnp.where(slots == number, 1.0, 0.0), axis=1, keepdims=True)
        times_ref[rows] = times
        used = jnp.where(times > 0.0, score, -jnp.inf)
        peak = jnp.maximum(peak, jnp.max(used, axis=0, keepdims=True))
        pos = pos + jnp.sum(jnp.where(target == number, score, 0.0), axis=0, keepdims=True)
        return peak, pos

    start = (jnp.full((1, SPAN), -jnp.inf, jnp.float32), jnp.zeros((1, SPAN), jnp.float32))
    peak, pos = lax.fori_loop(0, tiles, score_turn, start)
    peak = jnp.maximum(peak, pos)

    def total_turn(t, total):
        rows = pl.ds(pl.multiple_of(t * tile, tile), tile)
        times = times_ref[rows]
        value = jnp.where(times > 0.0, times * jnp.exp(score_ref[rows] - peak), 0.0)
        score_ref[rows] = value
        return total + jnp.sum(value, axis=0, keepdims=True)

    total = lax.fori_loop(0, tiles, total_turn, jnp.exp(pos - peak))
    log_total = peak + jnp.log(total)
    loss_ref[0] = (log_total - pos) * live
    pos_grad = (jnp.exp(pos - log_total) - 1.0) * live
    scale = jnp.exp(peak - log_total) * live
    query_grad_ref[...] = jnp.zeros_like(query_grad_ref)

    @pl.when(span == 0)
    def _():
        target_grad_ref[...] = jnp.zeros_like(target_grad_ref)

    def grad_turn(t, carried):
        rows = pl.ds(pl.multiple_of(t * tile, tile), tile)
        number = lax.broadcasted_iota(jnp.int32, (tile, 1), 0) + t * tile
        weight = score_ref[rows] * scale + jnp.where(target == number, pos_grad, 0.0)
        w0, w1 = split2(weight)
        t0, t1 = parts_ref[0, rows], parts_ref[1, rows]
        q0, q1 = query_parts_ref[0], query_parts_ref[1]
        query_grad_ref[...] += (mxu(w0, t1, TN) + mxu(w1, t0, TN)) + mxu(w0, t0, TN)
        target_grad_ref[rows] += (mxu(w0, q1, NN) + mxu(w1, q0, NN)) + mxu(w0, q0, NN)
        return carried

    lax.fori_loop(0, tiles, grad_turn, 0)


def span_step(edge_count, target, slots, queries, table):
    spans, negatives = slots.shape[0], slots.shape[2]
    table_rows = table.shape[0]
    f32 = jnp.float32
    return pl.pallas_call(
        span_kernel,
        grid=(spans,),
        in_specs=[
            pl.BlockSpec(memory_space=pltpu.SMEM),
            vmem((1, 1, SPAN), lambda i: (i, 0, 0)),
            vmem((1, 1, negatives), lambda i: (i, 0, 0)),
            vmem((SPAN, WIDE), lambda i: (i, 0)),
            vmem((table_rows, WIDE), lambda i: (0, 0)),
        ],
        out_specs=[
            vmem((1, 1, SPAN), lambda i: (i, 0, 0)),
            vmem((SPAN, WIDE), lambda i: (i, 0)),
            vmem((table_rows, WIDE), lambda i: (0, 0)),
        ],
        out_shape=[
            jax.ShapeDtypeStruct((spans, 1, SPAN), f32),
            jax.ShapeDtypeStruct((spans * SPAN, WIDE), f32),
            jax.ShapeDtypeStruct((table_rows, WIDE), f32),
        ],
        scratch_shapes=[
            pltpu.VMEM((table_rows, SPAN), f32),
            pltpu.VMEM((table_rows, 1), f32),
            pltpu.VMEM((3, table_rows, WIDE), jnp.bfloat16),
            pltpu.VMEM((3, SPAN, WIDE), jnp.bfloat16),
        ],
        compiler_params=params(),
        cost_estimate=pl.CostEstimate(
            flops=24 * spans * SPAN * table_rows * WIDE,
            bytes_accessed=16 * table_rows * WIDE,
            transcendentals=spans * SPAN * table_rows,
        ),
        name="span_step",
    )(edge_count, target, slots, queries, table)


def put_kernel(with_product, index_ref, value_ref, *rest):
    if with_product:
        other_ref, out_ref, parts_ref = rest
    else:
        out_ref, parts_ref = rest

    @pl.when(pl.program_id(0) == 0)
    def _():
        value = value_ref[...]
        if with_product:
            value = conj_product(value, other_ref[...])
        for k, part in enumerate(split2(value)):
            parts_ref[k] = part

    tile = out_ref.shape[0]
    rows = lax.broadcasted_iota(jnp.int32, (tile, index_ref.shape[1]), 0) + pl.program_id(0) * tile
    pick = jnp.where(rows == index_ref[...], 1.0, 0.0).astype(jnp.bfloat16)
    out_ref[...] = mxu(pick, parts_ref[1], NN) + mxu(pick, parts_ref[0], NN)


def put_rows(index, rows, value, other=None):
    count = value.shape[0]
    tile = min(256, rows)
    whole = vmem((count, WIDE), lambda i: (0, 0))
    operands = (index, value) if other is None else (index, value, other)
    return pl.pallas_call(
        functools.partial(put_kernel, other is not None),
        grid=(rows // tile,),
        in_specs=[vmem((1, count), lambda i: (0, 0))] + [whole] * (len(operands) - 1),
        out_specs=vmem((tile, WIDE), lambda i: (i, 0)),
        out_shape=jax.ShapeDtypeStruct((rows, WIDE), jnp.float32),
        scratch_shapes=[pltpu.VMEM((2, count, WIDE), jnp.bfloat16)],
        compiler_params=params(),
        cost_estimate=pl.CostEstimate(
            flops=4 * rows * count * WIDE, bytes_accessed=4 * (rows + count) * WIDE, transcendentals=0
        ),
        name="put_rows",
    )(*operands)


def passed_along(value, axis, by):
    count = lax.axis_size(axis)
    return lax.ppermute(value, axis, [(i, (i + by) % count) for i in range(count)])


def exchanged(value, axis):
    return lax.all_to_all(value, axis, split_axis=0, concat_axis=0, tiled=True)


def adagrad(params_, accumulator, gradient, width):
    new_state = accumulator + jnp.sum(gradient * gradient, axis=1) / width
    return params_ - LEARN_RATE * gradient / jnp.sqrt(new_state)[:, None]


def on_device(
    entity,
    entity_state,
    relation,
    relation_state,
    src_send,
    dst_send,
    edge_source,
    edge_relation,
    edge_target,
    neg_slots,
    edge_count,
):
    width = entity.shape[1]
    owned = entity.shape[0]
    relations = relation.shape[0]
    peers, block = src_send.shape[1], src_send.shape[2]
    table_rows = peers * block
    edges = edge_source.shape[0]
    spans = edges // SPAN
    groups, shards = lax.axis_size("group"), lax.axis_size("shard")
    share = -(-relations // (groups * shards))
    padded = share * groups * shards

    entity_wide = wide(entity)
    moved_index = passed_along(dst_send, "group", -1)
    moved_entity = passed_along(entity_wide, "group", -1)
    src_rows = take_rows(entity_wide, src_send.reshape(table_rows, 1))
    source_table = exchanged(src_rows.reshape(peers, block, WIDE), "shard").reshape(table_rows, WIDE)
    relation_wide = jnp.pad(wide(relation), ((0, padded - relations), (0, 0)))
    relation_state_wide = jnp.pad(relation_state, (0, padded - relations), constant_values=1.0)
    rels = take_rows(relation_wide, edge_relation.reshape(edges, 1))
    target_rows = take_rows(moved_entity, moved_index.reshape(table_rows, 1))
    target_table = exchanged(target_rows.reshape(peers, block, WIDE), "shard").reshape(table_rows, WIDE)
    heads, queries = make_queries(source_table, edge_source.reshape(edges, 1), rels)

    loss, query_grad, target_grad = span_step(
        edge_count,
        edge_target.reshape(spans, 1, SPAN),
        neg_slots.reshape(spans, 1, neg_slots.shape[1]),
        queries,
        target_table,
    )
    returned_target = exchanged(target_grad.reshape(peers, block, WIDE), "shard").reshape(table_rows, WIDE)

    relation_part = put_rows(edge_relation.reshape(1, edges), padded, query_grad, heads)
    relation_blocks = exchanged(relation_part.reshape(shards, groups * share, WIDE), "shard")
    relation_some = jnp.sum(relation_blocks, axis=0)
    relation_own = jnp.sum(exchanged(relation_some.reshape(groups, share, WIDE), "group"), axis=0)

    dense_grad = put_rows(moved_index.reshape(1, table_rows), owned, returned_target)
    moved_grad = passed_along(dense_grad, "group", 1)

    source_grad = put_rows(edge_source.reshape(1, edges), table_rows, query_grad, rels)
    returned_source = exchanged(source_grad.reshape(peers, block, WIDE), "shard").reshape(table_rows, WIDE)
    own_grad = put_rows(src_send.reshape(1, table_rows), owned, returned_source)

    first = (lax.axis_index("shard") * groups + lax.axis_index("group")) * share
    relation_mine = adagrad(
        lax.dynamic_slice_in_dim(relation_wide, first, share),
        lax.dynamic_slice_in_dim(relation_state_wide, first, share),
        relation_own,
        width,
    )
    relation_some_new = lax.all_gather(narrow(relation_mine, width), "group", axis=0, tiled=True)
    relation_new = lax.all_gather(relation_some_new, "shard", axis=0, tiled=True)[:relations]

    entity_grad = narrow(own_grad + moved_grad, width)
    entity_new = adagrad(entity, entity_state, entity_grad, width)
    return entity_new, relation_new, loss.reshape(edges)


def solution(mesh):
    return jax.shard_map(
        on_device,
        mesh=mesh,
        in_specs=(
            P(("group", "shard"), None),
            P(("group", "shard")),
            P(),
            P(),
            P(("group", "shard"), None, None),
            P(("group", "shard"), None, None),
            P(("group", "shard")),
            P(("group", "shard")),
            P(("group", "shard")),
            P(("group", "shard"), None),
            P(("group", "shard")),
        ),
        out_specs=(P(("group", "shard"), None), P(), P(("group", "shard"))),
        check_vma=False,
    )
```

```python
import functools

import jax
import jax.numpy as jnp
from jax import lax
from jax.experimental import pallas as pl
from jax.experimental.pallas import tpu as pltpu
from jax.sharding import PartitionSpec as P

SPAN = 512
LEARN_RATE = 0.5
WIDE = 512
TAIL = 8
MESH = pl.DeviceIdType.MESH

NT = (((1,), (1,)), ((), ()))
NN = (((1,), (0,)), ((), ()))
TN = (((0,), (0,)), ((), ()))


def split2(x):
    hi = x.astype(jnp.bfloat16)
    lo = (x - hi.astype(jnp.float32)).astype(jnp.bfloat16)
    return hi, lo


def split3(x):
    hi = x.astype(jnp.bfloat16)
    rest = x - hi.astype(jnp.float32)
    mid = rest.astype(jnp.bfloat16)
    lo = (rest - mid.astype(jnp.float32)).astype(jnp.bfloat16)
    return hi, mid, lo


def mxu(a, b, dims):
    return lax.dot_general(a, b, dims, preferred_element_type=jnp.float32)


def wide(x):
    half = x.shape[1] // 2
    re, im = x[:, :half], x[:, half:]
    zeros = jnp.zeros((x.shape[0], WIDE - x.shape[1]), x.dtype)
    return jnp.concatenate(
        [re[:, :128], im[:, :128], re[:, 128:192], im[:, 128:192], re[:, 192:], im[:, 192:], zeros], axis=1
    )


def narrow(x, width):
    tail = width // 2 - 192
    return jnp.concatenate(
        [
            x[:, :128], x[:, 256:320], x[:, 384 : 384 + tail],
            x[:, 128:256], x[:, 320:384], x[:, 384 + tail : 384 + 2 * tail],
        ],
        axis=1,
    )


def swapped(x, half):
    lane = lax.broadcasted_iota(jnp.int32, x.shape, 1)
    if half == 64:
        return pltpu.roll(x, 64, 1), lane < half
    left, right = pltpu.roll(x, 128 - half, 1), pltpu.roll(x, half, 1)
    mixed = jnp.where(lane < half, left, jnp.where(lane < 2 * half, right, 0.0))
    return mixed, lane < half


def mixed_product(a, b, half, sign):
    other_a, low = swapped(a, half)
    other_b, _ = swapped(b, half)
    real = jnp.where(low, b, other_b)
    imag = jnp.where(low, -other_b, b)
    return a * real + sign * (other_a * imag)


def product_of(a, b, sign):
    ar, ai, br, bi = a[:, :128], a[:, 128:256], b[:, :128], b[:, 128:256]
    return jnp.concatenate(
        [
            ar * br - sign * (ai * bi),
            ai * br + sign * (ar * bi),
            mixed_product(a[:, 256:384], b[:, 256:384], 64, sign),
            mixed_product(a[:, 384:], b[:, 384:], TAIL, sign),
        ],
        axis=1,
    )


def product(a, b):
    return product_of(a, b, 1.0)


def conj_product(a, b):
    return product_of(a, b, -1.0)


def chosen(index, count):
    lanes = lax.broadcasted_iota(jnp.int32, (index.shape[0], count), 1)
    return jnp.where(lanes == index, 1.0, 0.0).astype(jnp.bfloat16)


def vmem(shape, index_map):
    return pl.BlockSpec(shape, index_map, memory_space=pltpu.VMEM)


def params(limit=48 << 20):
    return pltpu.CompilerParams(vmem_limit_bytes=limit)


def take_kernel(index_ref, table_ref, out_ref, parts_ref):
    @pl.when(pl.program_id(0) == 0)
    def _():
        for k, part in enumerate(split3(table_ref[...])):
            parts_ref[k] = part

    pick = chosen(index_ref[...], table_ref.shape[0])
    out_ref[...] = (
        mxu(pick, parts_ref[0], NN) + mxu(pick, parts_ref[1], NN)
    ) + mxu(pick, parts_ref[2], NN)


def take_rows(table, index):
    rows, count = index.shape[0], table.shape[0]
    tile = min(256, rows)
    return pl.pallas_call(
        take_kernel,
        grid=(rows // tile,),
        in_specs=[vmem((tile, 1), lambda i: (i, 0)), vmem((count, WIDE), lambda i: (0, 0))],
        out_specs=vmem((tile, WIDE), lambda i: (i, 0)),
        out_shape=jax.ShapeDtypeStruct((rows, WIDE), jnp.float32),
        scratch_shapes=[pltpu.VMEM((3, count, WIDE), jnp.bfloat16)],
        compiler_params=params(),
        cost_estimate=pl.CostEstimate(
            flops=6 * rows * count * WIDE, bytes_accessed=4 * (rows + count) * WIDE, transcendentals=0
        ),
        name="take_rows",
    )(index, table)


def query_kernel(index_ref, table_ref, rel_ref, head_ref, query_ref, parts_ref):
    @pl.when(pl.program_id(0) == 0)
    def _():
        for k, part in enumerate(split3(table_ref[...])):
            parts_ref[k] = part

    pick = chosen(index_ref[...], table_ref.shape[0])
    heads = (mxu(pick, parts_ref[0], NN) + mxu(pick, parts_ref[1], NN)) + mxu(pick, parts_ref[2], NN)
    head_ref[...] = heads
    query_ref[...] = product(heads, rel_ref[...])


def make_queries(table, index, rels):
    rows, count = index.shape[0], table.shape[0]
    tile = min(256, rows)
    block = vmem((tile, WIDE), lambda i: (i, 0))
    shape = jax.ShapeDtypeStruct((rows, WIDE), jnp.float32)
    return pl.pallas_call(
        query_kernel,
        grid=(rows // tile,),
        in_specs=[vmem((tile, 1), lambda i: (i, 0)), vmem((count, WIDE), lambda i: (0, 0)), block],
        out_specs=[block, block],
        out_shape=[shape, shape],
        scratch_shapes=[pltpu.VMEM((3, count, WIDE), jnp.bfloat16)],
        compiler_params=params(),
        cost_estimate=pl.CostEstimate(
            flops=6 * rows * count * WIDE, bytes_accessed=4 * (4 * rows + count) * WIDE, transcendentals=0
        ),
        name="make_queries",
    )(index, table, rels)


def span_kernel(
    count_ref, target_ref, slots_ref, query_ref, table_ref,
    loss_ref, query_grad_ref, target_grad_ref,
    score_ref, times_ref, parts_ref, query_parts_ref,
):
    span = pl.program_id(0)
    table_rows = table_ref.shape[0]
    tile = min(256, table_rows)
    tiles = table_rows // tile

    @pl.when(span == 0)
    def _():
        for k, part in enumerate(split3(table_ref[...])):
            parts_ref[k] = part

    for k, part in enumerate(split3(query_ref[...])):
        query_parts_ref[k] = part

    edge = lax.broadcasted_iota(jnp.int32, (1, SPAN), 1) + span * SPAN
    live = jnp.where(edge < count_ref[0], 1.0, 0.0)
    target = target_ref[0]
    slots = slots_ref[0]

    def score_turn(t, carried):
        peak, pos = carried
        rows = pl.ds(pl.multiple_of(t * tile, tile), tile)
        t0, t1, t2 = parts_ref[0, rows], parts_ref[1, rows], parts_ref[2, rows]
        q0, q1, q2 = query_parts_ref[0], query_parts_ref[1], query_parts_ref[2]
        small = mxu(t0, q2, NT) + mxu(t2, q0, NT) + mxu(t1, q1, NT)
        score = (small + (mxu(t0, q1, NT) + mxu(t1, q0, NT))) + mxu(t0, q0, NT)
        score_ref[rows] = score
        number = lax.broadcasted_iota(jnp.int32, (tile, 1), 0) + t * tile
        times = jnp.sum(jnp.where(slots == number, 1.0, 0.0), axis=1, keepdims=True)
        times_ref[rows] = times
        used = jnp.where(times > 0.0, score, -jnp.inf)
        peak = jnp.maximum(peak, jnp.max(used, axis=0, keepdims=True))
        pos = pos + jnp.sum(jnp.where(target == number, score, 0.0), axis=0, keepdims=True)
        return peak, pos

    start = (jnp.full((1, SPAN), -jnp.inf, jnp.float32), jnp.zeros((1, SPAN), jnp.float32))
    peak, pos = lax.fori_loop(0, tiles, score_turn, start)
    peak = jnp.maximum(peak, pos)

    def total_turn(t, total):
        rows = pl.ds(pl.multiple_of(t * tile, tile), tile)
        times = times_ref[rows]
        value = jnp.where(times > 0.0, times * jnp.exp(score_ref[rows] - peak), 0.0)
        score_ref[rows] = value
        return total + jnp.sum(value, axis=0, keepdims=True)

    total = lax.fori_loop(0, tiles, total_turn, jnp.exp(pos - peak))
    log_total = peak + jnp.log(total)
    loss_ref[0] = (log_total - pos) * live
    pos_grad = (jnp.exp(pos - log_total) - 1.0) * live
    scale = jnp.exp(peak - log_total) * live
    query_grad_ref[...] = jnp.zeros_like(query_grad_ref)

    @pl.when(span == 0)
    def _():
        target_grad_ref[...] = jnp.zeros_like(target_grad_ref)

    def grad_turn(t, carried):
        rows = pl.ds(pl.multiple_of(t * tile, tile), tile)
        number = lax.broadcasted_iota(jnp.int32, (tile, 1), 0) + t * tile
        weight = score_ref[rows] * scale + jnp.where(target == number, pos_grad, 0.0)
        w0, w1 = split2(weight)
        t0, t1 = parts_ref[0, rows], parts_ref[1, rows]
        q0, q1 = query_parts_ref[0], query_parts_ref[1]
        query_grad_ref[...] += (mxu(w0, t1, TN) + mxu(w1, t0, TN)) + mxu(w0, t0, TN)
        target_grad_ref[rows] += (mxu(w0, q1, NN) + mxu(w1, q0, NN)) + mxu(w0, q0, NN)
        return carried

    lax.fori_loop(0, tiles, grad_turn, 0)


def span_step(edge_count, target, slots, queries, table):
    spans, negatives = slots.shape[0], slots.shape[2]
    table_rows = table.shape[0]
    f32 = jnp.float32
    return pl.pallas_call(
        span_kernel,
        grid=(spans,),
        in_specs=[
            pl.BlockSpec(memory_space=pltpu.SMEM),
            vmem((1, 1, SPAN), lambda i: (i, 0, 0)),
            vmem((1, 1, negatives), lambda i: (i, 0, 0)),
            vmem((SPAN, WIDE), lambda i: (i, 0)),
            vmem((table_rows, WIDE), lambda i: (0, 0)),
        ],
        out_specs=[
            vmem((1, 1, SPAN), lambda i: (i, 0, 0)),
            vmem((SPAN, WIDE), lambda i: (i, 0)),
            vmem((table_rows, WIDE), lambda i: (0, 0)),
        ],
        out_shape=[
            jax.ShapeDtypeStruct((spans, 1, SPAN), f32),
            jax.ShapeDtypeStruct((spans * SPAN, WIDE), f32),
            jax.ShapeDtypeStruct((table_rows, WIDE), f32),
        ],
        scratch_shapes=[
            pltpu.VMEM((table_rows, SPAN), f32),
            pltpu.VMEM((table_rows, 1), f32),
            pltpu.VMEM((3, table_rows, WIDE), jnp.bfloat16),
            pltpu.VMEM((3, SPAN, WIDE), jnp.bfloat16),
        ],
        compiler_params=params(),
        cost_estimate=pl.CostEstimate(
            flops=24 * spans * SPAN * table_rows * WIDE,
            bytes_accessed=16 * table_rows * WIDE,
            transcendentals=spans * SPAN * table_rows,
        ),
        name="span_step",
    )(edge_count, target, slots, queries, table)


def put_kernel(with_product, index_ref, value_ref, *rest):
    if with_product:
        other_ref, out_ref, parts_ref = rest
    else:
        out_ref, parts_ref = rest

    @pl.when(pl.program_id(0) == 0)
    def _():
        value = value_ref[...]
        if with_product:
            value = conj_product(value, other_ref[...])
        for k, part in enumerate(split2(value)):
            parts_ref[k] = part

    tile = out_ref.shape[0]
    rows = lax.broadcasted_iota(jnp.int32, (tile, index_ref.shape[1]), 0) + pl.program_id(0) * tile
    pick = jnp.where(rows == index_ref[...], 1.0, 0.0).astype(jnp.bfloat16)
    out_ref[...] = mxu(pick, parts_ref[1], NN) + mxu(pick, parts_ref[0], NN)


def put_rows(index, rows, value, other=None):
    count = value.shape[0]
    tile = next(t for t in (256, 176, 128, 64, 32, 16, 8) if rows % t == 0)
    whole = vmem((count, WIDE), lambda i: (0, 0))
    operands = (index, value) if other is None else (index, value, other)
    return pl.pallas_call(
        functools.partial(put_kernel, other is not None),
        grid=(rows // tile,),
        in_specs=[vmem((1, count), lambda i: (0, 0))] + [whole] * (len(operands) - 1),
        out_specs=vmem((tile, WIDE), lambda i: (i, 0)),
        out_shape=jax.ShapeDtypeStruct((rows, WIDE), jnp.float32),
        scratch_shapes=[pltpu.VMEM((2, count, WIDE), jnp.bfloat16)],
        compiler_params=params(),
        cost_estimate=pl.CostEstimate(
            flops=4 * rows * count * WIDE, bytes_accessed=4 * (rows + count) * WIDE, transcendentals=0
        ),
        name="put_rows",
    )(*operands)


def pack_tail(x):
    rows = x.shape[0]
    packed = []
    for first in range(0, rows, 64):
        total = x[first : first + 8]
        for k in range(1, min(8, (rows - first) // 8)):
            total = total + pltpu.roll(x[first + 8 * k : first + 8 * k + 8], 16 * k, 1)
        packed.append(total)
    return packed[0] if len(packed) == 1 else jnp.concatenate(packed, axis=0)


def unpack_tail(x, rows):
    lane = lax.broadcasted_iota(jnp.int32, (8, 128), 1)
    tiles = []
    for t in range(rows // 8):
        part = x[8 * (t // 8) : 8 * (t // 8) + 8]
        k = t % 8
        part = part if k == 0 else pltpu.roll(part, 128 - 16 * k, 1)
        tiles.append(jnp.where(lane < 16, part, 0.0))
    return tiles[0] if len(tiles) == 1 else jnp.concatenate(tiles, axis=0)


def packed_rows(rows):
    return 3 * rows + 8 * (-(-rows // 64))


def store_packed(ref, x):
    n = x.shape[0]
    for c in range(3):
        ref[c * n : (c + 1) * n] = x[:, 128 * c : 128 * c + 128]
    ref[3 * n :] = pack_tail(x[:, 384:])


def load_packed(ref, n):
    parts = [ref[c * n : (c + 1) * n] for c in range(3)]
    return parts, unpack_tail(ref[3 * n :], n)


def remote(src, dst, send, recv, **device):
    return pltpu.make_async_remote_copy(
        src_ref=src, dst_ref=dst, send_sem=send, recv_sem=recv, device_id=device, device_id_type=MESH
    )


def greet(shards, groups, shard, group):
    barrier = pltpu.get_barrier_semaphore()

    def near(k, carried):
        pl.semaphore_signal(
            barrier, inc=1, device_id={"shard": lax.rem(shard + k, shards)}, device_id_type=MESH
        )
        return carried

    def far(k, carried):
        pl.semaphore_signal(
            barrier, inc=1, device_id={"group": lax.rem(group + k, groups)}, device_id_type=MESH
        )
        return carried

    lax.fori_loop(1, shards, near, 0)
    lax.fori_loop(1, groups, far, 0)
    pl.semaphore_wait(barrier, shards + groups - 2)


def back_kernel(
    sizes,
    target_ref, source_ref, part_ref, relation_ref, relation_state_ref,
    moved_index_ref, source_index_ref, entity_ref, entity_state_ref,
    entity_new_ref, relation_new_ref,
    tsend, trecv, ssend, srecv, dense, moved, pick, values,
    r0send, r0recv, r1, r1recv, r2, r2recv, r3, r3recv, r4, r5,
    t_s, t_r, s_s, s_r, p_s, p_r, r0_s, r0_r, r1_s, r1_r, r2_s, r2_r, r3_s, r3_r, r4_s, r4_r, r5_s, r5_r,
):
    shards, groups, block, owned, width = sizes
    chips = shards // 2
    shard, group = lax.axis_index("shard"), lax.axis_index("group")
    core, chip = lax.rem(shard, 2), lax.div(shard, 2)
    partner = shard + 1 - 2 * core
    after = lax.rem(group + 1, groups)
    rb = part_ref.shape[0] // shards
    piece = r2.shape[1]
    stages = ((0, block), (block, block), (2 * block, packed_rows(block) - 2 * block))
    moves = ((0, owned), (owned, owned), (2 * owned, packed_rows(owned) - 2 * owned))

    greet(shards, groups, shard, group)

    def pack_target(p, carried):
        rows = pl.ds(pl.multiple_of(p * block, block), block)
        store_packed(tsend.at[p], target_ref[rows])
        return carried

    lax.fori_loop(0, shards, pack_target, 0)

    def target_copy(stage, to, slot):
        first, size = stages[stage]
        rows = pl.ds(first, size)
        return remote(
            tsend.at[to, rows], trecv.at[slot, rows], t_s.at[stage, to], t_r.at[stage, slot], shard=to
        )

    for stage in range(3):
        def send_target(k, carried, stage=stage):
            to = lax.rem(shard + k, shards)
            target_copy(stage, to, shard).start()
            return carried

        lax.fori_loop(1, shards, send_target, 0)

    def half_block(which, q):
        return pl.ds(pl.multiple_of((which * chips + q) * rb, rb), rb)

    def pack_other(q, carried):
        store_packed(r0send.at[q], part_ref[half_block(1 - core, q)])
        return carried

    lax.fori_loop(0, chips, pack_other, 0)
    pair = remote(r0send, r0recv, r0_s, r0_r, shard=partner)
    pair.start()

    def pack_own(q, carried):
        store_packed(r1.at[q], part_ref[half_block(core, q)])
        return carried

    lax.fori_loop(0, chips, pack_own, 0)
    trecv[shard] = tsend[shard]
    pair.wait_recv()

    def add_pair(q, carried):
        r1[q] = r1[q] + r0recv[q]
        return carried

    lax.fori_loop(0, chips, add_pair, 0)

    def chip_copy(to, slot):
        return remote(r1.at[to], r1recv.at[slot], r1_s.at[to], r1_r.at[slot], shard=2 * to + core)

    def send_chip(k, carried):
        chip_copy(lax.rem(chip + k, chips), chip).start()
        return carried

    lax.fori_loop(1, chips, send_chip, 0)

    def pack_source(p, carried):
        rows = pl.ds(pl.multiple_of(p * block, block), block)
        store_packed(ssend.at[p], source_ref[rows])
        return carried

    lax.fori_loop(0, shards, pack_source, 0)

    def source_copy(to, slot):
        return remote(ssend.at[to], srecv.at[slot], s_s.at[to], s_r.at[slot], shard=to)

    def send_source(k, carried):
        source_copy(lax.rem(shard + k, shards), shard).start()
        return carried

    lax.fori_loop(1, shards, send_source, 0)
    srecv[shard] = ssend[shard]

    number = lax.broadcasted_iota(jnp.int32, (owned, 1), 0)
    pick[...] = jnp.where(number == moved_index_ref[...], 1.0, 0.0).astype(jnp.bfloat16)

    def placed(value):
        v0, v1 = split2(value)
        return mxu(pick[...], v1, NN) + mxu(pick[...], v0, NN)

    def tails(ref):
        def turn(p, carried):
            values[pl.ds(pl.multiple_of(p * block, block), block)] = unpack_tail(ref[p, 3 * block :], block)
            return carried

        lax.fori_loop(0, shards, turn, 0)
        return values[...]

    def move(stage):
        first, size = moves[stage]
        rows = pl.ds(first, size)
        return remote(dense.at[rows], moved.at[rows], p_s.at[stage], p_r.at[stage], group=after)

    for stage in range(3):
        def wait_target(k, carried, stage=stage):
            frm = lax.rem(shard + k, shards)
            target_copy(stage, frm, frm).wait_recv()
            return carried

        lax.fori_loop(1, shards, wait_target, 0)
        chunk = trecv[:, stage * block : (stage + 1) * block].reshape(shards * block, 128)
        dense[stage * owned : (stage + 1) * owned] = placed(chunk)
        if stage == 2:
            dense[3 * owned :] = pack_tail(placed(tails(trecv)))
        move(stage).start()

    r2[...] = jnp.zeros_like(r2)

    def wait_chip(k, carried):
        frm = lax.rem(chip + k, chips)
        chip_copy(frm, frm).wait_recv()
        return carried

    lax.fori_loop(1, chips, wait_chip, 0)
    r1recv[chip] = r1[chip]
    total = r1recv[0]
    for q in range(1, chips):
        total = total + r1recv[q]
    size = total.shape[0]
    for h in range(groups):
        count = min(piece, size - h * piece)
        if count > 0:
            r2[h, :count] = total[h * piece : h * piece + count]

    def group_copy(to, slot):
        return remote(r2.at[to], r2recv.at[slot], r2_s.at[to], r2_r.at[slot], group=to)

    def send_group(k, carried):
        group_copy(lax.rem(group + k, groups), group).start()
        return carried

    def wait_group(k, carried):
        frm = lax.rem(group + k, groups)
        group_copy(frm, frm).wait_recv()
        return carried

    lax.fori_loop(1, groups, send_group, 0)
    r2recv[group] = r2[group]
    lax.fori_loop(1, groups, wait_group, 0)
    r3[...] = jnp.sum(r2recv[...], axis=0)

    def share_copy(to, slot):
        return remote(r3, r3recv.at[slot], r3_s.at[to], r3_r.at[slot], group=to)

    def send_share(k, carried):
        share_copy(lax.rem(group + k, groups), group).start()
        return carried

    def wait_share(k, carried):
        frm = lax.rem(group + k, groups)
        share_copy(frm, frm).wait_recv()
        return carried

    lax.fori_loop(1, groups, send_share, 0)
    r3recv[group] = r3[...]
    lax.fori_loop(1, groups, wait_share, 0)

    def updated(param_ref, rows, state, gradient):
        squares = sum(jnp.sum(g * g, axis=1, keepdims=True) for g in gradient)
        root = jnp.sqrt(state + squares / width)
        return [
            param_ref[rows, 128 * c : 128 * c + 128] - LEARN_RATE * g / root for c, g in enumerate(gradient)
        ]

    summed = r3recv[...].reshape(groups * piece, 128)
    gradient = [summed[c * rb : (c + 1) * rb] for c in range(3)]
    gradient.append(unpack_tail(summed[3 * rb : size], rb))
    mine = half_block(core, chip)
    fresh = updated(relation_ref, mine, relation_state_ref[mine], gradient)
    store_packed(r4.at[chip], jnp.concatenate(fresh, axis=1))

    def spread_copy(to, slot):
        return remote(r4.at[chip], r4.at[chip], r4_s.at[to], r4_r.at[chip], shard=2 * to + core)

    def spread_wait(frm):
        return remote(r4.at[frm], r4.at[frm], r4_s.at[frm], r4_r.at[frm], shard=2 * frm + core)

    def hand_copy(q):
        return remote(r4.at[q], r5.at[q], r5_s.at[q], r5_r.at[q], shard=partner)

    def send_spread(k, carried):
        spread_copy(lax.rem(chip + k, chips), chip).start()
        return carried

    lax.fori_loop(1, chips, send_spread, 0)
    hand_copy(chip).start()

    def wait_source(k, carried):
        frm = lax.rem(shard + k, shards)
        source_copy(frm, frm).wait_recv()
        return carried

    lax.fori_loop(1, shards, wait_source, 0)
    pick[...] = jnp.where(number == source_index_ref[...], 1.0, 0.0).astype(jnp.bfloat16)
    own = []
    for c in range(3):
        own.append(placed(srecv[:, c * block : (c + 1) * block].reshape(shards * block, 128)))
    own.append(placed(tails(srecv)))
    for c in range(4):
        entity_new_ref[:, 128 * c : 128 * c + 128] = own[c]
    for stage in range(3):
        move(stage).wait_recv()
    parts, tail = load_packed(moved, owned)
    parts.append(tail)
    gradient = [entity_new_ref[:, 128 * c : 128 * c + 128] + parts[c] for c in range(4)]
    fresh = updated(entity_ref, slice(None), entity_state_ref[...], gradient)
    for c in range(4):
        entity_new_ref[:, 128 * c : 128 * c + 128] = fresh[c]

    def forward(k, carried):
        frm = lax.rem(chip + k, chips)
        spread_wait(frm).wait_recv()
        hand_copy(frm).start()
        return carried

    lax.fori_loop(1, chips, forward, 0)

    def put_out(which, ref):
        def turn(q, carried):
            rows = half_block(which, q)
            got, tail_ = load_packed(ref.at[q], rb)
            for c in range(3):
                relation_new_ref[rows, 128 * c : 128 * c + 128] = got[c]
            relation_new_ref[rows, 384:] = tail_
            return carried

        lax.fori_loop(0, chips, turn, 0)

    put_out(core, r4)

    def take_hand(q, carried):
        hand_copy(q).wait_recv()
        return carried

    lax.fori_loop(0, chips, take_hand, 0)
    put_out(1 - core, r5)

    for stage in range(3):
        def end_target(k, carried, stage=stage):
            to = lax.rem(shard + k, shards)
            target_copy(stage, to, shard).wait_send()
            return carried

        lax.fori_loop(1, shards, end_target, 0)
        move(stage).wait_send()

    def end_shard(k, carried):
        source_copy(lax.rem(shard + k, shards), shard).wait_send()
        return carried

    def end_chip(k, carried):
        to = lax.rem(chip + k, chips)
        chip_copy(to, chip).wait_send()
        spread_copy(to, chip).wait_send()
        return carried

    def end_group(k, carried):
        to = lax.rem(group + k, groups)
        group_copy(to, group).wait_send()
        share_copy(to, group).wait_send()
        return carried

    def end_hand(q, carried):
        hand_copy(q).wait_send()
        return carried

    lax.fori_loop(1, shards, end_shard, 0)
    lax.fori_loop(1, chips, end_chip, 0)
    lax.fori_loop(1, groups, end_group, 0)
    lax.fori_loop(0, chips, end_hand, 0)
    pair.wait_send()


def back_step(sizes, *operands):
    shards, groups, block, owned, width = sizes
    padded = operands[2].shape[0]
    chips, rb = shards // 2, padded // shards
    size = packed_rows(rb)
    piece = 8 * (-(-size // (8 * groups)))
    f32 = jnp.float32
    table = pltpu.VMEM((shards, packed_rows(block), 128), f32)
    flat = pltpu.VMEM((packed_rows(owned), 128), f32)
    half = pltpu.VMEM((chips, size, 128), f32)
    pieces = pltpu.VMEM((groups, piece, 128), f32)
    dma = pltpu.SemaphoreType.DMA
    return pl.pallas_call(
        functools.partial(back_kernel, sizes),
        in_specs=[pl.BlockSpec(memory_space=pltpu.VMEM)] * len(operands),
        out_specs=[pl.BlockSpec(memory_space=pltpu.VMEM)] * 2,
        out_shape=[jax.ShapeDtypeStruct((owned, WIDE), f32), jax.ShapeDtypeStruct((padded, WIDE), f32)],
        scratch_shapes=[
            table, table, table, table, flat, flat,
            pltpu.VMEM((owned, shards * block), jnp.bfloat16),
            pltpu.VMEM((shards * block, 128), f32),
            half, half, half, half, pieces, pieces, pltpu.VMEM((piece, 128), f32), pieces, half, half,
            dma((3, shards)), dma((3, shards)), dma((shards,)), dma((shards,)), dma((3,)), dma((3,)),
            dma, dma, dma((chips,)), dma((chips,)), dma((groups,)), dma((groups,)),
            dma((groups,)), dma((groups,)), dma((chips,)), dma((chips,)), dma((chips,)), dma((chips,)),
        ],
        compiler_params=pltpu.CompilerParams(
            collective_id=1, has_side_effects=True, vmem_limit_bytes=60 << 20
        ),
        name="back_step",
    )(*operands)


def passed_along(value, axis, by):
    count = lax.axis_size(axis)
    return lax.ppermute(value, axis, [(i, (i + by) % count) for i in range(count)])


def exchanged(value, axis):
    return lax.all_to_all(value, axis, split_axis=0, concat_axis=0, tiled=True)


def on_device(
    entity,
    entity_state,
    relation,
    relation_state,
    src_send,
    dst_send,
    edge_source,
    edge_relation,
    edge_target,
    neg_slots,
    edge_count,
):
    width = entity.shape[1]
    owned = entity.shape[0]
    relations = relation.shape[0]
    peers, block = src_send.shape[1], src_send.shape[2]
    table_rows = peers * block
    edges = edge_source.shape[0]
    spans = edges // SPAN
    groups, shards = lax.axis_size("group"), lax.axis_size("shard")
    padded = 8 * shards * (-(-relations // (8 * shards)))

    entity_wide = wide(entity)
    moved_index = passed_along(dst_send, "group", -1)
    moved_entity = passed_along(entity_wide, "group", -1)
    src_rows = take_rows(entity_wide, src_send.reshape(table_rows, 1))
    source_table = exchanged(src_rows.reshape(peers, block, WIDE), "shard").reshape(table_rows, WIDE)
    relation_wide = jnp.pad(wide(relation), ((0, padded - relations), (0, 0)))
    relation_state_wide = jnp.pad(relation_state[:, None], ((0, padded - relations), (0, 0)), constant_values=1.0)
    rels = take_rows(relation_wide, edge_relation.reshape(edges, 1))
    target_rows = take_rows(moved_entity, moved_index.reshape(table_rows, 1))
    target_table = exchanged(target_rows.reshape(peers, block, WIDE), "shard").reshape(table_rows, WIDE)
    heads, queries = make_queries(source_table, edge_source.reshape(edges, 1), rels)

    loss, query_grad, target_grad = span_step(
        edge_count,
        edge_target.reshape(spans, 1, SPAN),
        neg_slots.reshape(spans, 1, neg_slots.shape[1]),
        queries,
        target_table,
    )
    relation_part = put_rows(edge_relation.reshape(1, edges), padded, query_grad, heads)
    source_grad = put_rows(edge_source.reshape(1, edges), table_rows, query_grad, rels)
    entity_new, relation_new = back_step(
        (shards, groups, block, owned, width),
        target_grad,
        source_grad,
        relation_part,
        relation_wide,
        relation_state_wide,
        moved_index.reshape(1, table_rows),
        src_send.reshape(1, table_rows),
        entity_wide,
        entity_state.reshape(owned, 1),
    )
    return narrow(entity_new, width), narrow(relation_new[:relations], width), loss.reshape(edges)


def solution(mesh):
    return jax.shard_map(
        on_device,
        mesh=mesh,
        in_specs=(
            P(("group", "shard"), None),
            P(("group", "shard")),
            P(),
            P(),
            P(("group", "shard"), None, None),
            P(("group", "shard"), None, None),
            P(("group", "shard")),
            P(("group", "shard")),
            P(("group", "shard")),
            P(("group", "shard"), None),
            P(("group", "shard")),
        ),
        out_specs=(P(("group", "shard"), None), P(), P(("group", "shard"))),
        check_vma=False,
    )
```

```python
import functools

import jax
import jax.numpy as jnp
from jax import lax
from jax.experimental import pallas as pl
from jax.experimental.pallas import tpu as pltpu
from jax.sharding import PartitionSpec as P

SPAN = 512
LEARN_RATE = 0.5
WIDE = 512
TAIL = 8
MESH = pl.DeviceIdType.MESH

NT = (((1,), (1,)), ((), ()))
NN = (((1,), (0,)), ((), ()))
TN = (((0,), (0,)), ((), ()))


def split2(x):
    hi = x.astype(jnp.bfloat16)
    lo = (x - hi.astype(jnp.float32)).astype(jnp.bfloat16)
    return hi, lo


def split3(x):
    hi = x.astype(jnp.bfloat16)
    rest = x - hi.astype(jnp.float32)
    mid = rest.astype(jnp.bfloat16)
    lo = (rest - mid.astype(jnp.float32)).astype(jnp.bfloat16)
    return hi, mid, lo


def mxu(a, b, dims):
    return lax.dot_general(a, b, dims, preferred_element_type=jnp.float32)


def lane_of(x):
    return lax.broadcasted_iota(jnp.int32, x.shape, 1)


def widened(x0, x1, x2, x3):
    lane = lane_of(x0)
    imag = jnp.where(lane < 56, pltpu.roll(x1, 56, 1), pltpu.roll(x2, 56, 1))
    both = jnp.where(
        lane < 64, x1, jnp.where(lane < 120, pltpu.roll(x2, 120, 1), pltpu.roll(x3, 120, 1))
    )
    tail = jnp.where(lane < 8, pltpu.roll(x1, 64, 1), jnp.where(lane < 16, x3, 0.0))
    return x0, imag, both, tail


def narrowed(real, imag, both, tail):
    lane = lane_of(real)
    imag_on, both_on = pltpu.roll(imag, 72, 1), pltpu.roll(both, 8, 1)
    x1 = jnp.where(lane < 64, both, jnp.where(lane < 72, pltpu.roll(tail, 64, 1), imag_on))
    x2 = jnp.where(lane < 72, imag_on, both_on)
    return real, x1, x2, jnp.where(lane < 8, both_on, tail)


def load_wide(ref, rows, count, last):
    last[:count] = jnp.zeros((count, 128), jnp.float32)
    last[:count, :16] = ref[rows, 384:400]
    return widened(ref[rows, 0:128], ref[rows, 128:256], ref[rows, 256:384], last[:count])


def store_narrow(ref, rows, parts):
    x = narrowed(*parts)
    for c in range(3):
        ref[rows, 128 * c : 128 * c + 128] = x[c]
    ref[rows, 384:400] = x[3][:, :16]


def column_of(row_ref, first, count):
    n = row_ref.shape[1]
    lane = lax.broadcasted_iota(jnp.int32, (count, n), 1)
    own = lax.broadcasted_iota(jnp.int32, (count, n), 0) + first
    return jnp.sum(jnp.where(lane == own, row_ref[...], 0.0), axis=1, keepdims=True)


def swapped(x, half):
    lane = lax.broadcasted_iota(jnp.int32, x.shape, 1)
    if half == 64:
        return pltpu.roll(x, 64, 1), lane < half
    left, right = pltpu.roll(x, 128 - half, 1), pltpu.roll(x, half, 1)
    mixed = jnp.where(lane < half, left, jnp.where(lane < 2 * half, right, 0.0))
    return mixed, lane < half


def mixed_product(a, b, half, sign):
    other_a, low = swapped(a, half)
    other_b, _ = swapped(b, half)
    real = jnp.where(low, b, other_b)
    imag = jnp.where(low, -other_b, b)
    return a * real + sign * (other_a * imag)


def product_of(a, b, sign):
    ar, ai, br, bi = a[:, :128], a[:, 128:256], b[:, :128], b[:, 128:256]
    return jnp.concatenate(
        [
            ar * br - sign * (ai * bi),
            ai * br + sign * (ar * bi),
            mixed_product(a[:, 256:384], b[:, 256:384], 64, sign),
            mixed_product(a[:, 384:], b[:, 384:], TAIL, sign),
        ],
        axis=1,
    )


def product(a, b):
    return product_of(a, b, 1.0)


def conj_product(a, b):
    return product_of(a, b, -1.0)


def picked(index, count):
    rows = lax.broadcasted_iota(jnp.int32, (count, index.shape[1]), 0)
    return jnp.where(rows == index, 1.0, 0.0).astype(jnp.bfloat16)


def vmem(shape, index_map):
    return pl.BlockSpec(shape, index_map, memory_space=pltpu.VMEM)


def params(limit=48 << 20):
    return pltpu.CompilerParams(vmem_limit_bytes=limit)


def span_kernel(
    count_ref, target_ref, slots_ref, query_ref, table_ref,
    loss_ref, query_grad_ref, target_grad_ref,
    score_ref, times_ref, parts_ref, query_parts_ref,
):
    span = pl.program_id(0)
    table_rows = table_ref.shape[0]
    tile = min(256, table_rows)
    tiles = table_rows // tile

    @pl.when(span == 0)
    def _():
        for k, part in enumerate(split3(table_ref[...])):
            parts_ref[k] = part

    for k, part in enumerate(split3(query_ref[...])):
        query_parts_ref[k] = part

    edge = lax.broadcasted_iota(jnp.int32, (1, SPAN), 1) + span * SPAN
    live = jnp.where(edge < count_ref[0], 1.0, 0.0)
    target = target_ref[0]
    slots = slots_ref[0]

    def score_turn(t, carried):
        peak, pos = carried
        rows = pl.ds(pl.multiple_of(t * tile, tile), tile)
        t0, t1, t2 = parts_ref[0, rows], parts_ref[1, rows], parts_ref[2, rows]
        q0, q1, q2 = query_parts_ref[0], query_parts_ref[1], query_parts_ref[2]
        small = mxu(t0, q2, NT) + mxu(t2, q0, NT) + mxu(t1, q1, NT)
        score = (small + (mxu(t0, q1, NT) + mxu(t1, q0, NT))) + mxu(t0, q0, NT)
        score_ref[rows] = score
        number = lax.broadcasted_iota(jnp.int32, (tile, 1), 0) + t * tile
        times = jnp.sum(jnp.where(slots == number, 1.0, 0.0), axis=1, keepdims=True)
        times_ref[rows] = times
        used = jnp.where(times > 0.0, score, -jnp.inf)
        peak = jnp.maximum(peak, jnp.max(used, axis=0, keepdims=True))
        pos = pos + jnp.sum(jnp.where(target == number, score, 0.0), axis=0, keepdims=True)
        return peak, pos

    start = (jnp.full((1, SPAN), -jnp.inf, jnp.float32), jnp.zeros((1, SPAN), jnp.float32))
    peak, pos = lax.fori_loop(0, tiles, score_turn, start)
    peak = jnp.maximum(peak, pos)

    def total_turn(t, total):
        rows = pl.ds(pl.multiple_of(t * tile, tile), tile)
        times = times_ref[rows]
        value = jnp.where(times > 0.0, times * jnp.exp(score_ref[rows] - peak), 0.0)
        score_ref[rows] = value
        return total + jnp.sum(value, axis=0, keepdims=True)

    total = lax.fori_loop(0, tiles, total_turn, jnp.exp(pos - peak))
    log_total = peak + jnp.log(total)
    loss_ref[0] = (log_total - pos) * live
    pos_grad = (jnp.exp(pos - log_total) - 1.0) * live
    scale = jnp.exp(peak - log_total) * live
    query_grad_ref[...] = jnp.zeros_like(query_grad_ref)

    @pl.when(span == 0)
    def _():
        target_grad_ref[...] = jnp.zeros_like(target_grad_ref)

    def grad_turn(t, carried):
        rows = pl.ds(pl.multiple_of(t * tile, tile), tile)
        number = lax.broadcasted_iota(jnp.int32, (tile, 1), 0) + t * tile
        weight = score_ref[rows] * scale + jnp.where(target == number, pos_grad, 0.0)
        w0, w1 = split2(weight)
        t0, t1 = parts_ref[0, rows], parts_ref[1, rows]
        q0, q1 = query_parts_ref[0], query_parts_ref[1]
        query_grad_ref[...] += (mxu(w0, t1, TN) + mxu(w1, t0, TN)) + mxu(w0, t0, TN)
        target_grad_ref[rows] += (mxu(w0, q1, NN) + mxu(w1, q0, NN)) + mxu(w0, q0, NN)
        return carried

    lax.fori_loop(0, tiles, grad_turn, 0)


def span_step(edge_count, target, slots, queries, table):
    spans, negatives = slots.shape[0], slots.shape[2]
    table_rows = table.shape[0]
    f32 = jnp.float32
    return pl.pallas_call(
        span_kernel,
        grid=(spans,),
        in_specs=[
            pl.BlockSpec(memory_space=pltpu.SMEM),
            vmem((1, 1, SPAN), lambda i: (i, 0, 0)),
            vmem((1, 1, negatives), lambda i: (i, 0, 0)),
            vmem((SPAN, WIDE), lambda i: (i, 0)),
            vmem((table_rows, WIDE), lambda i: (0, 0)),
        ],
        out_specs=[
            vmem((1, 1, SPAN), lambda i: (i, 0, 0)),
            vmem((SPAN, WIDE), lambda i: (i, 0)),
            vmem((table_rows, WIDE), lambda i: (0, 0)),
        ],
        out_shape=[
            jax.ShapeDtypeStruct((spans, 1, SPAN), f32),
            jax.ShapeDtypeStruct((spans * SPAN, WIDE), f32),
            jax.ShapeDtypeStruct((table_rows, WIDE), f32),
        ],
        scratch_shapes=[
            pltpu.VMEM((table_rows, SPAN), f32),
            pltpu.VMEM((table_rows, 1), f32),
            pltpu.VMEM((3, table_rows, WIDE), jnp.bfloat16),
            pltpu.VMEM((3, SPAN, WIDE), jnp.bfloat16),
        ],
        compiler_params=params(),
        cost_estimate=pl.CostEstimate(
            flops=24 * spans * SPAN * table_rows * WIDE,
            bytes_accessed=16 * table_rows * WIDE,
            transcendentals=spans * SPAN * table_rows,
        ),
        name="span_step",
    )(edge_count, target, slots, queries, table)


def pack_tail(x):
    rows = x.shape[0]
    packed = []
    for first in range(0, rows, 64):
        total = x[first : first + 8]
        for k in range(1, min(8, (rows - first) // 8)):
            total = total + pltpu.roll(x[first + 8 * k : first + 8 * k + 8], 16 * k, 1)
        packed.append(total)
    return packed[0] if len(packed) == 1 else jnp.concatenate(packed, axis=0)


def unpack_tail(x, rows):
    lane = lax.broadcasted_iota(jnp.int32, (8, 128), 1)
    tiles = []
    for t in range(rows // 8):
        part = x[8 * (t // 8) : 8 * (t // 8) + 8]
        k = t % 8
        part = part if k == 0 else pltpu.roll(part, 128 - 16 * k, 1)
        tiles.append(jnp.where(lane < 16, part, 0.0))
    return tiles[0] if len(tiles) == 1 else jnp.concatenate(tiles, axis=0)


def packed_rows(rows):
    return 3 * rows + 8 * (-(-rows // 64))


def store_packed(ref, x):
    n = x.shape[0]
    for c in range(3):
        ref[c * n : (c + 1) * n] = x[:, 128 * c : 128 * c + 128]
    ref[3 * n :] = pack_tail(x[:, 384:])


def load_packed(ref, n):
    parts = [ref[c * n : (c + 1) * n] for c in range(3)]
    return parts, unpack_tail(ref[3 * n :], n)


def remote(src, dst, send, recv, **device):
    return pltpu.make_async_remote_copy(
        src_ref=src, dst_ref=dst, send_sem=send, recv_sem=recv, device_id=device, device_id_type=MESH
    )


def greet(shards, groups, shard, group):
    barrier = pltpu.get_barrier_semaphore()

    def near(k, carried):
        pl.semaphore_signal(
            barrier, inc=1, device_id={"shard": lax.rem(shard + k, shards)}, device_id_type=MESH
        )
        return carried

    def far(k, carried):
        pl.semaphore_signal(
            barrier, inc=1, device_id={"group": lax.rem(group + k, groups)}, device_id_type=MESH
        )
        return carried

    lax.fori_loop(1, shards, near, 0)
    lax.fori_loop(1, groups, far, 0)
    pl.semaphore_wait(barrier, shards + groups - 2)


def back_kernel(
    sizes,
    target_ref, query_grad_ref, heads_ref, rels_ref, edge_source_ref, edge_relation_ref,
    relation_ref, relation_state_ref, moved_index_ref, source_index_ref, entity_ref, entity_state_ref,
    entity_new_ref, relation_new_ref,
    tsend, trecv, ssend, srecv, dense, moved, pick, values, grads, part_ref, last, dense_own,
    r0send, r0recv, r1, r1recv, r2, r2recv, r3, r3recv, r4, r5,
    t_s, t_r, s_s, s_r, p_s, p_r, r0_s, r0_r, r1_s, r1_r, r2_s, r2_r, r3_s, r3_r, r4_s, r4_r, r5_s, r5_r,
):
    shards, groups, block, owned, width = sizes
    chips = shards // 2
    shard, group = lax.axis_index("shard"), lax.axis_index("group")
    core, chip = lax.rem(shard, 2), lax.div(shard, 2)
    partner = shard + 1 - 2 * core
    after = lax.rem(group + 1, groups)
    rb = part_ref.shape[0] // shards
    piece = r2.shape[1]
    stages = ((0, block), (block, block), (2 * block, packed_rows(block) - 2 * block))
    moves = ((0, owned), (owned, owned), (2 * owned, packed_rows(owned) - 2 * owned))

    greet(shards, groups, shard, group)

    def pack_target(p, carried):
        rows = pl.ds(pl.multiple_of(p * block, block), block)
        store_packed(tsend.at[p], target_ref[rows])
        return carried

    lax.fori_loop(0, shards, pack_target, 0)

    def target_copy(stage, to, slot):
        first, size = stages[stage]
        rows = pl.ds(first, size)
        return remote(
            tsend.at[to, rows], trecv.at[slot, rows], t_s.at[stage, to], t_r.at[stage, slot], shard=to
        )

    for stage in range(3):
        def send_target(k, carried, stage=stage):
            to = lax.rem(shard + k, shards)
            target_copy(stage, to, shard).start()
            return carried

        lax.fori_loop(1, shards, send_target, 0)

    edges = query_grad_ref.shape[0]
    padded = part_ref.shape[0]
    tile = 256
    half_rows = padded // 2
    put_tile = half_rows // 2 if half_rows % 32 == 0 else half_rows

    def half_block(which, q):
        return pl.ds(pl.multiple_of((which * chips + q) * rb, rb), rb)

    def gradient_parts(other_ref):
        def turn(t, carried):
            rows = pl.ds(pl.multiple_of(t * tile, tile), tile)
            for k, part in enumerate(split2(conj_product(query_grad_ref[rows], other_ref[rows]))):
                grads[k, rows] = part
            return carried

        lax.fori_loop(0, edges // tile, turn, 0)

    def summed_rows(index_ref, first, count):
        number = lax.broadcasted_iota(jnp.int32, (count, edges), 0) + first
        ones = jnp.where(number == index_ref[...], 1.0, 0.0).astype(jnp.bfloat16)
        return mxu(ones, grads[1], NN) + mxu(ones, grads[0], NN)

    def half_sums(which):
        def turn(t, carried):
            first = pl.multiple_of(which * half_rows + t * put_tile, put_tile)
            part_ref[pl.ds(first, put_tile)] = summed_rows(edge_relation_ref, first, put_tile)
            return carried

        lax.fori_loop(0, half_rows // put_tile, turn, 0)

    gradient_parts(heads_ref)
    half_sums(1 - core)

    def pack_other(q, carried):
        store_packed(r0send.at[q], part_ref[half_block(1 - core, q)])
        return carried

    lax.fori_loop(0, chips, pack_other, 0)
    pair = remote(r0send, r0recv, r0_s, r0_r, shard=partner)
    pair.start()
    half_sums(core)

    def pack_own(q, carried):
        store_packed(r1.at[q], part_ref[half_block(core, q)])
        return carried

    lax.fori_loop(0, chips, pack_own, 0)
    trecv[shard] = tsend[shard]
    pick[...] = picked(moved_index_ref[...], owned)

    def placed(value):
        v0, v1 = split2(value)
        return mxu(pick[...], v1, NN) + mxu(pick[...], v0, NN)

    def tails(ref):
        def turn(p, carried):
            values[pl.ds(pl.multiple_of(p * block, block), block)] = unpack_tail(ref[p, 3 * block :], block)
            return carried

        lax.fori_loop(0, shards, turn, 0)
        return values[...]

    def move(stage):
        first, size = moves[stage]
        rows = pl.ds(first, size)
        return remote(dense.at[rows], moved.at[rows], p_s.at[stage], p_r.at[stage], group=after)

    def pass_on(stage):
        def wait_target(k, carried):
            frm = lax.rem(shard + k, shards)
            target_copy(stage, frm, frm).wait_recv()
            return carried

        lax.fori_loop(1, shards, wait_target, 0)
        chunk = trecv[:, stage * block : (stage + 1) * block].reshape(shards * block, 128)
        dense[stage * owned : (stage + 1) * owned] = placed(chunk)
        if stage == 2:
            dense[3 * owned :] = pack_tail(placed(tails(trecv)))
        move(stage).start()

    pass_on(0)
    pair.wait_recv()

    def add_pair(q, carried):
        r1[q] = r1[q] + r0recv[q]
        return carried

    lax.fori_loop(0, chips, add_pair, 0)

    def chip_copy(to, slot):
        return remote(r1.at[to], r1recv.at[slot], r1_s.at[to], r1_r.at[slot], shard=2 * to + core)

    def send_chip(k, carried):
        chip_copy(lax.rem(chip + k, chips), chip).start()
        return carried

    lax.fori_loop(1, chips, send_chip, 0)
    pass_on(1)

    gradient_parts(rels_ref)

    def put_source(t, carried):
        value = summed_rows(edge_source_ref, t * tile, tile)
        for j in range(tile // block):
            store_packed(ssend.at[t * (tile // block) + j], value[j * block : (j + 1) * block])
        return carried

    lax.fori_loop(0, shards * block // tile, put_source, 0)

    def source_copy(to, slot):
        return remote(ssend.at[to], srecv.at[slot], s_s.at[to], s_r.at[slot], shard=to)

    def send_source(k, carried):
        source_copy(lax.rem(shard + k, shards), shard).start()
        return carried

    lax.fori_loop(1, shards, send_source, 0)
    srecv[shard] = ssend[shard]
    pass_on(2)

    r2[...] = jnp.zeros_like(r2)

    def wait_chip(k, carried):
        frm = lax.rem(chip + k, chips)
        chip_copy(frm, frm).wait_recv()
        return carried

    lax.fori_loop(1, chips, wait_chip, 0)
    r1recv[chip] = r1[chip]
    total = r1recv[0]
    for q in range(1, chips):
        total = total + r1recv[q]
    size = total.shape[0]
    for h in range(groups):
        count = min(piece, size - h * piece)
        if count > 0:
            r2[h, :count] = total[h * piece : h * piece + count]

    def group_copy(to, slot):
        return remote(r2.at[to], r2recv.at[slot], r2_s.at[to], r2_r.at[slot], group=to)

    def send_group(k, carried):
        group_copy(lax.rem(group + k, groups), group).start()
        return carried

    def wait_group(k, carried):
        frm = lax.rem(group + k, groups)
        group_copy(frm, frm).wait_recv()
        return carried

    lax.fori_loop(1, groups, send_group, 0)
    r2recv[group] = r2[group]
    lax.fori_loop(1, groups, wait_group, 0)
    r3[...] = jnp.sum(r2recv[...], axis=0)

    def share_copy(to, slot):
        return remote(r3, r3recv.at[slot], r3_s.at[to], r3_r.at[slot], group=to)

    def send_share(k, carried):
        share_copy(lax.rem(group + k, groups), group).start()
        return carried

    def wait_share(k, carried):
        frm = lax.rem(group + k, groups)
        share_copy(frm, frm).wait_recv()
        return carried

    lax.fori_loop(1, groups, send_share, 0)
    r3recv[group] = r3[...]
    lax.fori_loop(1, groups, wait_share, 0)

    def updated(params_, state, gradient):
        squares = sum(jnp.sum(g * g, axis=1, keepdims=True) for g in gradient)
        root = jnp.sqrt(state + squares / width)
        return [p - LEARN_RATE * g / root for p, g in zip(params_, gradient)]

    summed = r3recv[...].reshape(groups * piece, 128)
    gradient = [summed[c * rb : (c + 1) * rb] for c in range(3)]
    gradient.append(unpack_tail(summed[3 * rb : size], rb))
    state = column_of(relation_state_ref, (core * chips + chip) * rb, rb)
    fresh = updated(load_wide(relation_ref, half_block(core, chip), rb, last), state, gradient)
    store_packed(r4.at[chip], jnp.concatenate(fresh, axis=1))

    def spread_copy(to, slot):
        return remote(r4.at[chip], r4.at[chip], r4_s.at[to], r4_r.at[chip], shard=2 * to + core)

    def spread_wait(frm):
        return remote(r4.at[frm], r4.at[frm], r4_s.at[frm], r4_r.at[frm], shard=2 * frm + core)

    def hand_copy(q):
        return remote(r4.at[q], r5.at[q], r5_s.at[q], r5_r.at[q], shard=partner)

    def send_spread(k, carried):
        spread_copy(lax.rem(chip + k, chips), chip).start()
        return carried

    lax.fori_loop(1, chips, send_spread, 0)
    hand_copy(chip).start()

    def wait_source(k, carried):
        frm = lax.rem(shard + k, shards)
        source_copy(frm, frm).wait_recv()
        return carried

    lax.fori_loop(1, shards, wait_source, 0)
    pick[...] = picked(source_index_ref[...], owned)
    for c in range(3):
        dense_own[c] = placed(srecv[:, c * block : (c + 1) * block].reshape(shards * block, 128))
    dense_own[3] = placed(tails(srecv))
    for stage in range(3):
        move(stage).wait_recv()
    parts, tail = load_packed(moved, owned)
    parts.append(tail)
    gradient = [dense_own[c] + parts[c] for c in range(4)]
    entity_wide = load_wide(entity_ref, slice(None), owned, last)
    fresh = updated(entity_wide, column_of(entity_state_ref, 0, owned), gradient)
    store_narrow(entity_new_ref, slice(None), fresh)

    def forward(k, carried):
        frm = lax.rem(chip + k, chips)
        spread_wait(frm).wait_recv()
        hand_copy(frm).start()
        return carried

    lax.fori_loop(1, chips, forward, 0)

    def put_out(which, ref):
        def turn(q, carried):
            got, tail_ = load_packed(ref.at[q], rb)
            store_narrow(relation_new_ref, half_block(which, q), (*got, tail_))
            return carried

        lax.fori_loop(0, chips, turn, 0)

    put_out(core, r4)

    def take_hand(q, carried):
        hand_copy(q).wait_recv()
        return carried

    lax.fori_loop(0, chips, take_hand, 0)
    put_out(1 - core, r5)

    for stage in range(3):
        def end_target(k, carried, stage=stage):
            to = lax.rem(shard + k, shards)
            target_copy(stage, to, shard).wait_send()
            return carried

        lax.fori_loop(1, shards, end_target, 0)
        move(stage).wait_send()

    def end_shard(k, carried):
        source_copy(lax.rem(shard + k, shards), shard).wait_send()
        return carried

    def end_chip(k, carried):
        to = lax.rem(chip + k, chips)
        chip_copy(to, chip).wait_send()
        spread_copy(to, chip).wait_send()
        return carried

    def end_group(k, carried):
        to = lax.rem(group + k, groups)
        group_copy(to, group).wait_send()
        share_copy(to, group).wait_send()
        return carried

    def end_hand(q, carried):
        hand_copy(q).wait_send()
        return carried

    lax.fori_loop(1, shards, end_shard, 0)
    lax.fori_loop(1, chips, end_chip, 0)
    lax.fori_loop(1, groups, end_group, 0)
    lax.fori_loop(0, chips, end_hand, 0)
    pair.wait_send()


def back_step(sizes, *operands):
    shards, groups, block, owned, width = sizes
    padded = operands[6].shape[0]
    edges = operands[1].shape[0]
    chips, rb = shards // 2, padded // shards
    size = packed_rows(rb)
    piece = 8 * (-(-size // (8 * groups)))
    f32 = jnp.float32
    table = pltpu.VMEM((shards, packed_rows(block), 128), f32)
    flat = pltpu.VMEM((packed_rows(owned), 128), f32)
    half = pltpu.VMEM((chips, size, 128), f32)
    pieces = pltpu.VMEM((groups, piece, 128), f32)
    dma = pltpu.SemaphoreType.DMA
    return pl.pallas_call(
        functools.partial(back_kernel, sizes),
        in_specs=[pl.BlockSpec(memory_space=pltpu.VMEM)] * len(operands),
        out_specs=[pl.BlockSpec(memory_space=pltpu.VMEM)] * 2,
        out_shape=[jax.ShapeDtypeStruct((owned, width), f32), jax.ShapeDtypeStruct((padded, width), f32)],
        scratch_shapes=[
            table, table, table, table, flat, flat,
            pltpu.VMEM((owned, shards * block), jnp.bfloat16),
            pltpu.VMEM((shards * block, 128), f32),
            pltpu.VMEM((2, edges, WIDE), jnp.bfloat16),
            pltpu.VMEM((padded, WIDE), f32),
            pltpu.VMEM((owned, 128), f32),
            pltpu.VMEM((4, owned, 128), f32),
            half, half, half, half, pieces, pieces, pltpu.VMEM((piece, 128), f32), pieces, half, half,
            dma((3, shards)), dma((3, shards)), dma((shards,)), dma((shards,)), dma((3,)), dma((3,)),
            dma, dma, dma((chips,)), dma((chips,)), dma((groups,)), dma((groups,)),
            dma((groups,)), dma((groups,)), dma((chips,)), dma((chips,)), dma((chips,)), dma((chips,)),
        ],
        compiler_params=pltpu.CompilerParams(
            collective_id=1, has_side_effects=True, vmem_limit_bytes=60 << 20
        ),
        name="back_step",
    )(*operands)


def front_kernel(
    sizes,
    entity_ref, relation_ref, source_index_ref, target_index_ref, edge_source_ref, edge_relation_ref,
    table_ref, heads_ref, rels_ref, queries_ref, moved_index_ref,
    esend, erecv, isend, irecv, eparts, rparts, sparts, pick, ssend, srecv, tsend, trecv, values, last,
    e_s, e_r, i_s, i_r, s_s, s_r, t_s, t_r,
):
    shards, groups, block, owned, width = sizes
    shard, group = lax.axis_index("shard"), lax.axis_index("group")
    before = lax.rem(group + groups - 1, groups)
    edges, padded = edge_source_ref.shape[1], relation_ref.shape[0]
    table_rows = shards * block
    tile = 256
    stages = ((0, block), (block, block), (2 * block, packed_rows(block) - 2 * block))
    moves = ((0, owned), (owned, owned), (2 * owned, packed_rows(owned) - 2 * owned))

    isend[...] = target_index_ref[...]
    wide = load_wide(entity_ref, slice(None), owned, last)
    for c in range(3):
        esend[c * owned : (c + 1) * owned] = wide[c]
    esend[3 * owned :] = pack_tail(wide[3])
    greet(shards, groups, shard, group)

    index_copy = remote(isend, irecv, i_s, i_r, group=before)
    index_copy.start()

    def move(stage):
        first, size = moves[stage]
        rows = pl.ds(first, size)
        return remote(esend.at[rows], erecv.at[rows], e_s.at[stage], e_r.at[stage], group=before)

    for stage in range(3):
        move(stage).start()

    for c in range(4):
        for k, part in enumerate(split3(wide[c])):
            eparts[k, :, 128 * c : 128 * c + 128] = part

    def taken(parts, index_ref, t, count):
        ones = picked(index_ref[:, pl.ds(pl.multiple_of(t * tile, tile), tile)], count)
        return (mxu(ones, parts[0], TN) + mxu(ones, parts[1], TN)) + mxu(ones, parts[2], TN)

    def take_source(t, carried):
        value = taken(eparts, source_index_ref, t, owned)
        for j in range(tile // block):
            store_packed(ssend.at[t * (tile // block) + j], value[j * block : (j + 1) * block])
        return carried

    lax.fori_loop(0, table_rows // tile, take_source, 0)

    def source_copy(to, slot):
        return remote(ssend.at[to], srecv.at[slot], s_s.at[to], s_r.at[slot], shard=to)

    def send_source(k, carried):
        source_copy(lax.rem(shard + k, shards), shard).start()
        return carried

    lax.fori_loop(1, shards, send_source, 0)
    srecv[shard] = ssend[shard]

    step = 128 if padded % 128 == 0 else 32

    def split_relation(t, carried):
        rows = pl.ds(pl.multiple_of(t * step, step), step)
        for c, x in enumerate(load_wide(relation_ref, rows, step, last)):
            for k, part in enumerate(split3(x)):
                rparts[k, rows, 128 * c : 128 * c + 128] = part
        return carried

    lax.fori_loop(0, padded // step, split_relation, 0)

    def take_relation(t, carried):
        rels_ref[pl.ds(pl.multiple_of(t * tile, tile), tile)] = taken(rparts, edge_relation_ref, t, padded)
        return carried

    lax.fori_loop(0, edges // tile, take_relation, 0)

    index_copy.wait_recv()
    moved_index_ref[...] = irecv[...]
    pick[...] = picked(irecv[...], owned)

    def found(chunk):
        value = mxu(pick[...], jnp.concatenate(split3(chunk), axis=1), TN)
        return (value[:, :128] + value[:, 128:256]) + value[:, 256:]

    def target_copy(stage, to, slot):
        first, size = stages[stage]
        rows = pl.ds(first, size)
        return remote(
            tsend.at[to, rows], trecv.at[slot, rows], t_s.at[stage, to], t_r.at[stage, slot], shard=to
        )

    for stage in range(3):
        move(stage).wait_recv()
        chunk = erecv[stage * owned : (stage + 1) * owned]
        tsend[:, stage * block : (stage + 1) * block] = found(chunk).reshape(shards, block, 128)
        if stage == 2:
            values[...] = found(unpack_tail(erecv[3 * owned :], owned))

            def pack_tails(p, carried):
                rows = pl.ds(pl.multiple_of(p * block, block), block)
                tsend[p, 3 * block :] = pack_tail(values[rows])
                return carried

            lax.fori_loop(0, shards, pack_tails, 0)

        def send_target(k, carried, stage=stage):
            target_copy(stage, lax.rem(shard + k, shards), shard).start()
            return carried

        lax.fori_loop(1, shards, send_target, 0)
    trecv[shard] = tsend[shard]

    def wait_source(k, carried):
        frm = lax.rem(shard + k, shards)
        source_copy(frm, frm).wait_recv()
        return carried

    lax.fori_loop(1, shards, wait_source, 0)

    def split_source(p, carried):
        rows = pl.ds(pl.multiple_of(p * block, block), block)
        parts, tail = load_packed(srecv.at[p], block)
        for c, x in enumerate((*parts, tail)):
            for k, part in enumerate(split3(x)):
                sparts[k, rows, 128 * c : 128 * c + 128] = part
        return carried

    lax.fori_loop(0, shards, split_source, 0)

    def make_queries(t, carried):
        rows = pl.ds(pl.multiple_of(t * tile, tile), tile)
        heads = taken(sparts, edge_source_ref, t, table_rows)
        heads_ref[rows] = heads
        queries_ref[rows] = product(heads, rels_ref[rows])
        return carried

    lax.fori_loop(0, edges // tile, make_queries, 0)

    for stage in range(3):
        def wait_target(k, carried, stage=stage):
            frm = lax.rem(shard + k, shards)
            target_copy(stage, frm, frm).wait_recv()
            return carried

        lax.fori_loop(1, shards, wait_target, 0)

    def put_table(p, carried):
        rows = pl.ds(pl.multiple_of(p * block, block), block)
        parts, tail = load_packed(trecv.at[p], block)
        for c, x in enumerate((*parts, tail)):
            table_ref[rows, 128 * c : 128 * c + 128] = x
        return carried

    lax.fori_loop(0, shards, put_table, 0)

    index_copy.wait_send()
    for stage in range(3):
        def end_target(k, carried, stage=stage):
            target_copy(stage, lax.rem(shard + k, shards), shard).wait_send()
            return carried

        lax.fori_loop(1, shards, end_target, 0)
        move(stage).wait_send()

    def end_source(k, carried):
        source_copy(lax.rem(shard + k, shards), shard).wait_send()
        return carried

    lax.fori_loop(1, shards, end_source, 0)


def front_step(sizes, *operands):
    shards, groups, block, owned, width = sizes
    padded, edges, table_rows = operands[1].shape[0], operands[4].shape[1], shards * block
    f32, bf16 = jnp.float32, jnp.bfloat16
    table = pltpu.VMEM((shards, packed_rows(block), 128), f32)
    flat = pltpu.VMEM((packed_rows(owned), 128), f32)
    index = pltpu.VMEM((1, table_rows), jnp.int32)
    dma = pltpu.SemaphoreType.DMA
    return pl.pallas_call(
        functools.partial(front_kernel, sizes),
        in_specs=[pl.BlockSpec(memory_space=pltpu.VMEM)] * len(operands),
        out_specs=[pl.BlockSpec(memory_space=pltpu.VMEM)] * 5,
        out_shape=[
            jax.ShapeDtypeStruct((table_rows, WIDE), f32),
            jax.ShapeDtypeStruct((edges, WIDE), f32),
            jax.ShapeDtypeStruct((edges, WIDE), f32),
            jax.ShapeDtypeStruct((edges, WIDE), f32),
            jax.ShapeDtypeStruct((1, table_rows), jnp.int32),
        ],
        scratch_shapes=[
            flat, flat, index, index,
            pltpu.VMEM((3, owned, WIDE), bf16),
            pltpu.VMEM((3, padded, WIDE), bf16),
            pltpu.VMEM((3, table_rows, WIDE), bf16),
            pltpu.VMEM((owned, table_rows), bf16),
            table, table, table, table,
            pltpu.VMEM((table_rows, 128), f32),
            pltpu.VMEM((owned, 128), f32),
            dma((3,)), dma((3,)), dma, dma, dma((shards,)), dma((shards,)), dma((3, shards)), dma((3, shards)),
        ],
        compiler_params=pltpu.CompilerParams(
            collective_id=0, has_side_effects=True, vmem_limit_bytes=60 << 20
        ),
        name="front_step",
    )(*operands)


def on_device(
    entity,
    entity_state,
    relation,
    relation_state,
    src_send,
    dst_send,
    edge_source,
    edge_relation,
    edge_target,
    neg_slots,
    edge_count,
):
    width = entity.shape[1]
    owned = entity.shape[0]
    relations = relation.shape[0]
    peers, block = src_send.shape[1], src_send.shape[2]
    table_rows = peers * block
    edges = edge_source.shape[0]
    spans = edges // SPAN
    groups, shards = lax.axis_size("group"), lax.axis_size("shard")
    padded = 8 * shards * (-(-relations // (8 * shards)))

    relation_rows = jnp.pad(relation, ((0, padded - relations), (0, 0)))
    relation_states = jnp.pad(relation_state, (0, padded - relations), constant_values=1.0).reshape(1, padded)
    sizes = (shards, groups, block, owned, width)
    source_index = src_send.reshape(1, table_rows)
    edge_sources, edge_relations = edge_source.reshape(1, edges), edge_relation.reshape(1, edges)
    target_table, heads, rels, queries, moved_index = front_step(
        sizes,
        entity,
        relation_rows,
        source_index,
        dst_send.reshape(1, table_rows),
        edge_sources,
        edge_relations,
    )
    loss, query_grad, target_grad = span_step(
        edge_count,
        edge_target.reshape(spans, 1, SPAN),
        neg_slots.reshape(spans, 1, neg_slots.shape[1]),
        queries,
        target_table,
    )
    entity_new, relation_new = back_step(
        sizes,
        target_grad,
        query_grad,
        heads,
        rels,
        edge_sources,
        edge_relations,
        relation_rows,
        relation_states,
        moved_index,
        source_index,
        entity,
        entity_state.reshape(1, owned),
    )
    return entity_new, relation_new[:relations], loss.reshape(edges)


def solution(mesh):
    return jax.shard_map(
        on_device,
        mesh=mesh,
        in_specs=(
            P(("group", "shard"), None),
            P(("group", "shard")),
            P(),
            P(),
            P(("group", "shard"), None, None),
            P(("group", "shard"), None, None),
            P(("group", "shard")),
            P(("group", "shard")),
            P(("group", "shard")),
            P(("group", "shard"), None),
            P(("group", "shard")),
        ),
        out_specs=(P(("group", "shard"), None), P(), P(("group", "shard"))),
        check_vma=False,
    )
```

```python
import functools

import jax
import jax.numpy as jnp
from jax import lax
from jax.experimental import pallas as pl
from jax.experimental.pallas import tpu as pltpu
from jax.sharding import PartitionSpec as P

SPAN = 512
LEARN_RATE = 0.5
WIDE = 512
TAIL = 8
ACROSS = 4
MESH = pl.DeviceIdType.MESH

NT = (((1,), (1,)), ((), ()))
NN = (((1,), (0,)), ((), ()))
TN = (((0,), (0,)), ((), ()))


def split2(x):
    hi = x.astype(jnp.bfloat16)
    lo = (x - hi.astype(jnp.float32)).astype(jnp.bfloat16)
    return hi, lo


def split3(x):
    hi = x.astype(jnp.bfloat16)
    rest = x - hi.astype(jnp.float32)
    mid = rest.astype(jnp.bfloat16)
    lo = (rest - mid.astype(jnp.float32)).astype(jnp.bfloat16)
    return hi, mid, lo


def mxu(a, b, dims):
    return lax.dot_general(a, b, dims, preferred_element_type=jnp.float32)


def lane_of(x):
    return lax.broadcasted_iota(jnp.int32, x.shape, 1)


def widened(x0, x1, x2, x3):
    lane = lane_of(x0)
    imag = jnp.where(lane < 56, pltpu.roll(x1, 56, 1), pltpu.roll(x2, 56, 1))
    both = jnp.where(
        lane < 64, x1, jnp.where(lane < 120, pltpu.roll(x2, 120, 1), pltpu.roll(x3, 120, 1))
    )
    tail = jnp.where(lane < 8, pltpu.roll(x1, 64, 1), jnp.where(lane < 16, x3, 0.0))
    return x0, imag, both, tail


def narrowed(real, imag, both, tail):
    lane = lane_of(real)
    imag_on, both_on = pltpu.roll(imag, 72, 1), pltpu.roll(both, 8, 1)
    x1 = jnp.where(lane < 64, both, jnp.where(lane < 72, pltpu.roll(tail, 64, 1), imag_on))
    x2 = jnp.where(lane < 72, imag_on, both_on)
    return real, x1, x2, jnp.where(lane < 8, both_on, tail)


def load_wide(ref, rows, count, last):
    last[:count] = jnp.zeros((count, 128), jnp.float32)
    last[:count, :16] = ref[rows, 384:400]
    return widened(ref[rows, 0:128], ref[rows, 128:256], ref[rows, 256:384], last[:count])


def store_narrow(ref, rows, parts):
    x = narrowed(*parts)
    for c in range(3):
        ref[rows, 128 * c : 128 * c + 128] = x[c]
    ref[rows, 384:400] = x[3][:, :16]


def column_of(row_ref, first, count):
    n = row_ref.shape[1]
    lane = lax.broadcasted_iota(jnp.int32, (count, n), 1)
    own = lax.broadcasted_iota(jnp.int32, (count, n), 0) + first
    return jnp.sum(jnp.where(lane == own, row_ref[...], 0.0), axis=1, keepdims=True)


def swapped(x, half):
    lane = lax.broadcasted_iota(jnp.int32, x.shape, 1)
    if half == 64:
        return pltpu.roll(x, 64, 1), lane < half
    left, right = pltpu.roll(x, 128 - half, 1), pltpu.roll(x, half, 1)
    mixed = jnp.where(lane < half, left, jnp.where(lane < 2 * half, right, 0.0))
    return mixed, lane < half


def mixed_product(a, b, half, sign):
    other_a, low = swapped(a, half)
    other_b, _ = swapped(b, half)
    real = jnp.where(low, b, other_b)
    imag = jnp.where(low, -other_b, b)
    return a * real + sign * (other_a * imag)


def product_of(a, b, sign):
    ar, ai, br, bi = a[:, :128], a[:, 128:256], b[:, :128], b[:, 128:256]
    return jnp.concatenate(
        [
            ar * br - sign * (ai * bi),
            ai * br + sign * (ar * bi),
            mixed_product(a[:, 256:384], b[:, 256:384], 64, sign),
            mixed_product(a[:, 384:], b[:, 384:], TAIL, sign),
        ],
        axis=1,
    )


def product(a, b):
    return product_of(a, b, 1.0)


def conj_product(a, b):
    return product_of(a, b, -1.0)


def picked(index, count):
    rows = lax.broadcasted_iota(jnp.int32, (count, index.shape[1]), 0)
    return jnp.where(rows == index, 1.0, 0.0).astype(jnp.bfloat16)


def vmem(shape, index_map):
    return pl.BlockSpec(shape, index_map, memory_space=pltpu.VMEM)


def params(limit=48 << 20):
    return pltpu.CompilerParams(vmem_limit_bytes=limit)


def span_kernel(
    count_ref, target_ref, slots_ref, query_ref, table_ref,
    loss_ref, query_grad_ref, target_grad_ref,
    score_ref, times_ref, parts_ref, query_parts_ref,
):
    span = pl.program_id(0)
    table_rows = table_ref.shape[0]
    tile = min(256, table_rows)
    tiles = table_rows // tile

    @pl.when(span == 0)
    def _():
        for k, part in enumerate(split3(table_ref[...])):
            parts_ref[k] = part

    for k, part in enumerate(split3(query_ref[...])):
        query_parts_ref[k] = part

    edge = lax.broadcasted_iota(jnp.int32, (1, SPAN), 1) + span * SPAN
    live = jnp.where(edge < count_ref[0], 1.0, 0.0)
    target = target_ref[0]
    slots = slots_ref[0]

    def score_turn(t, carried):
        peak, pos = carried
        rows = pl.ds(pl.multiple_of(t * tile, tile), tile)
        t0, t1, t2 = parts_ref[0, rows], parts_ref[1, rows], parts_ref[2, rows]
        q0, q1, q2 = query_parts_ref[0], query_parts_ref[1], query_parts_ref[2]
        small = mxu(t0, q2, NT) + mxu(t2, q0, NT) + mxu(t1, q1, NT)
        score = (small + (mxu(t0, q1, NT) + mxu(t1, q0, NT))) + mxu(t0, q0, NT)
        score_ref[rows] = score
        number = lax.broadcasted_iota(jnp.int32, (tile, 1), 0) + t * tile
        times = jnp.sum(jnp.where(slots == number, 1.0, 0.0), axis=1, keepdims=True)
        times_ref[rows] = times
        used = jnp.where(times > 0.0, score, -jnp.inf)
        peak = jnp.maximum(peak, jnp.max(used, axis=0, keepdims=True))
        pos = pos + jnp.sum(jnp.where(target == number, score, 0.0), axis=0, keepdims=True)
        return peak, pos

    start = (jnp.full((1, SPAN), -jnp.inf, jnp.float32), jnp.zeros((1, SPAN), jnp.float32))
    peak, pos = lax.fori_loop(0, tiles, score_turn, start)
    peak = jnp.maximum(peak, pos)

    def total_turn(t, total):
        rows = pl.ds(pl.multiple_of(t * tile, tile), tile)
        times = times_ref[rows]
        value = jnp.where(times > 0.0, times * jnp.exp(score_ref[rows] - peak), 0.0)
        score_ref[rows] = value
        return total + jnp.sum(value, axis=0, keepdims=True)

    total = lax.fori_loop(0, tiles, total_turn, jnp.exp(pos - peak))
    log_total = peak + jnp.log(total)
    loss_ref[0] = (log_total - pos) * live
    pos_grad = (jnp.exp(pos - log_total) - 1.0) * live
    scale = jnp.exp(peak - log_total) * live
    query_grad_ref[...] = jnp.zeros_like(query_grad_ref)

    @pl.when(span == 0)
    def _():
        target_grad_ref[...] = jnp.zeros_like(target_grad_ref)

    def grad_turn(t, carried):
        rows = pl.ds(pl.multiple_of(t * tile, tile), tile)
        number = lax.broadcasted_iota(jnp.int32, (tile, 1), 0) + t * tile
        weight = score_ref[rows] * scale + jnp.where(target == number, pos_grad, 0.0)
        w0, w1 = split2(weight)
        t0, t1 = parts_ref[0, rows], parts_ref[1, rows]
        q0, q1 = query_parts_ref[0], query_parts_ref[1]
        query_grad_ref[...] += (mxu(w0, t1, TN) + mxu(w1, t0, TN)) + mxu(w0, t0, TN)
        target_grad_ref[rows] += (mxu(w0, q1, NN) + mxu(w1, q0, NN)) + mxu(w0, q0, NN)
        return carried

    lax.fori_loop(0, tiles, grad_turn, 0)


def span_step(edge_count, target, slots, queries, table):
    spans, negatives = slots.shape[0], slots.shape[2]
    table_rows = table.shape[0]
    f32 = jnp.float32
    return pl.pallas_call(
        span_kernel,
        grid=(spans,),
        in_specs=[
            pl.BlockSpec(memory_space=pltpu.SMEM),
            vmem((1, 1, SPAN), lambda i: (i, 0, 0)),
            vmem((1, 1, negatives), lambda i: (i, 0, 0)),
            vmem((SPAN, WIDE), lambda i: (i, 0)),
            vmem((table_rows, WIDE), lambda i: (0, 0)),
        ],
        out_specs=[
            vmem((1, 1, SPAN), lambda i: (i, 0, 0)),
            vmem((SPAN, WIDE), lambda i: (i, 0)),
            vmem((table_rows, WIDE), lambda i: (0, 0)),
        ],
        out_shape=[
            jax.ShapeDtypeStruct((spans, 1, SPAN), f32),
            jax.ShapeDtypeStruct((spans * SPAN, WIDE), f32),
            jax.ShapeDtypeStruct((table_rows, WIDE), f32),
        ],
        scratch_shapes=[
            pltpu.VMEM((table_rows, SPAN), f32),
            pltpu.VMEM((table_rows, 1), f32),
            pltpu.VMEM((3, table_rows, WIDE), jnp.bfloat16),
            pltpu.VMEM((3, SPAN, WIDE), jnp.bfloat16),
        ],
        compiler_params=params(),
        cost_estimate=pl.CostEstimate(
            flops=24 * spans * SPAN * table_rows * WIDE,
            bytes_accessed=16 * table_rows * WIDE,
            transcendentals=spans * SPAN * table_rows,
        ),
        name="span_step",
    )(edge_count, target, slots, queries, table)


def pack_tail(x):
    rows = x.shape[0]
    packed = []
    for first in range(0, rows, 64):
        total = x[first : first + 8]
        for k in range(1, min(8, (rows - first) // 8)):
            total = total + pltpu.roll(x[first + 8 * k : first + 8 * k + 8], 16 * k, 1)
        packed.append(total)
    return packed[0] if len(packed) == 1 else jnp.concatenate(packed, axis=0)


def unpack_tail(x, rows):
    lane = lax.broadcasted_iota(jnp.int32, (8, 128), 1)
    tiles = []
    for t in range(rows // 8):
        part = x[8 * (t // 8) : 8 * (t // 8) + 8]
        k = t % 8
        part = part if k == 0 else pltpu.roll(part, 128 - 16 * k, 1)
        tiles.append(jnp.where(lane < 16, part, 0.0))
    return tiles[0] if len(tiles) == 1 else jnp.concatenate(tiles, axis=0)


def packed_rows(rows):
    return 3 * rows + 8 * (-(-rows // 64))


def store_packed(ref, x):
    n = x.shape[0]
    for c in range(3):
        ref[c * n : (c + 1) * n] = x[:, 128 * c : 128 * c + 128]
    ref[3 * n :] = pack_tail(x[:, 384:])


def load_packed(ref, n):
    parts = [ref[c * n : (c + 1) * n] for c in range(3)]
    return parts, unpack_tail(ref[3 * n :], n)


def remote(src, dst, send, recv, **device):
    return pltpu.make_async_remote_copy(
        src_ref=src, dst_ref=dst, send_sem=send, recv_sem=recv, device_id=device, device_id_type=MESH
    )


def greet(shards, groups, shard, group, team=None):
    barrier = pltpu.get_barrier_semaphore()

    def near(k, carried):
        pl.semaphore_signal(
            barrier, inc=1, device_id={"shard": lax.rem(shard + k, shards)}, device_id_type=MESH
        )
        return carried

    def far(k, carried):
        pl.semaphore_signal(
            barrier, inc=1, device_id={"group": lax.rem(group + k, groups)}, device_id_type=MESH
        )
        return carried

    lax.fori_loop(1, shards, near, 0)
    lax.fori_loop(1, groups, far, 0)
    met = shards + groups - 2
    if team is not None:
        count, place, member = team

        def wide_signal(k, carried):
            pl.semaphore_signal(
                barrier, inc=1, device_id=member(lax.rem(place + k, count)), device_id_type=MESH
            )
            return carried

        lax.fori_loop(1, count, wide_signal, 0)
        met = met + count - 1
    pl.semaphore_wait(barrier, met)


class Passing:
    def __init__(self, groups, group, by, owned, rows_ref, via_ref, out_ref, sent, came, via_came, handed):
        layers = groups // ACROSS
        x, layer = lax.rem(group, ACROSS), lax.div(group, ACROSS)
        ahead = lax.rem(layer + by + layers, layers)
        first, last = (ACROSS - 1, 0) if by > 0 else (0, ACROSS - 1)
        self.x, self.first, self.last = x, first, last
        self.direct = lax.rem(group + by + groups, groups)
        self.over = (layer * ACROSS + last, ahead * ACROSS + first)
        self.final = (ahead * ACROSS + last, layer * ACROSS + last)
        rest = packed_rows(owned) - 2 * owned
        part = 8 * (rest // 16)
        self.pieces = ((0, owned), (owned, owned), (2 * owned, part), (2 * owned + part, rest - part))
        self.refs = (rows_ref, via_ref, out_ref)
        self.sems = (sent, came, via_came, handed)

    def copy(self, i, kind):
        rows = pl.ds(*self.pieces[i])
        rows_ref, via_ref, out_ref = self.refs
        sent, came, via_came, handed = self.sems
        if kind == "direct":
            return remote(rows_ref.at[rows], out_ref.at[rows], sent.at[i], came.at[i], group=self.direct)
        if kind == "over":
            return remote(
                rows_ref.at[rows], via_ref.at[rows], sent.at[i], via_came.at[i], group=self.over[i % 2]
            )
        return remote(via_ref.at[rows], out_ref.at[rows], handed.at[i], came.at[i], group=self.final[i % 2])

    def send(self, i):
        @pl.when(self.x != self.first)
        def _():
            self.copy(i, "direct").start()

        @pl.when(self.x == self.first)
        def _():
            self.copy(i, "over").start()

    def relay(self, i):
        @pl.when(self.x == (self.last if i % 2 == 0 else self.first))
        def _():
            self.copy(i, "over").wait_recv()
            self.copy(i, "final").start()

    def wait(self, i):
        self.copy(i, "direct").wait_recv()

    def end(self):
        for i in range(4):
            self.copy(i, "direct").wait_send()

            @pl.when(self.x == (self.last if i % 2 == 0 else self.first))
            def _():
                self.copy(i, "final").wait_send()


def back_kernel(
    sizes,
    target_ref, query_grad_ref, heads_ref, rels_ref, edge_source_ref, edge_relation_ref,
    relation_ref, relation_state_ref, moved_index_ref, source_index_ref, entity_ref, entity_state_ref,
    entity_new_ref, relation_new_ref,
    tsend, trecv, ssend, srecv, dense, via, moved, pick, values, grads, part_ref, last, dense_own,
    r0send, r0recv, r1, r1recv, r2, r2recv, r3, r3recv, r4, r5,
    t_s, t_r, s_s, s_r, p_s, p_r, p_v, p_h, r0_s, r0_r, r1_s, r1_r, r2_s, r2_r, r3_s, r3_r, r4_s, r4_r, r5_s, r5_r,
):
    shards, groups, block, owned, width = sizes
    chips = shards // 2
    shard, group = lax.axis_index("shard"), lax.axis_index("group")
    core, chip = lax.rem(shard, 2), lax.div(shard, 2)
    partner = shard + 1 - 2 * core
    across, layer = lax.rem(group, ACROSS), lax.div(group, ACROSS)
    rb = part_ref.shape[0] // (2 * ACROSS)
    members = r2.shape[0]
    place = layer * chips + chip

    def member(m):
        return {"group": lax.div(m, chips) * ACROSS + across, "shard": 2 * lax.rem(m, chips) + core}

    piece = r2.shape[1]
    stages = ((0, block), (block, block), (2 * block, packed_rows(block) - 2 * block))
    passing = Passing(groups, group, 1, owned, dense, via, moved, p_s, p_r, p_v, p_h)

    greet(shards, groups, shard, group, (members, place, member))

    def pack_target(p, carried):
        rows = pl.ds(pl.multiple_of(p * block, block), block)
        store_packed(tsend.at[p], target_ref[rows])
        return carried

    lax.fori_loop(0, shards, pack_target, 0)

    def target_copy(stage, to, slot):
        first, size = stages[stage]
        rows = pl.ds(first, size)
        return remote(
            tsend.at[to, rows], trecv.at[slot, rows], t_s.at[stage, to], t_r.at[stage, slot], shard=to
        )

    for stage in range(3):
        def send_target(k, carried, stage=stage):
            to = lax.rem(shard + k, shards)
            target_copy(stage, to, shard).start()
            return carried

        lax.fori_loop(1, shards, send_target, 0)

    edges = query_grad_ref.shape[0]
    padded = part_ref.shape[0]
    tile = 256
    half_rows = padded // 2
    put_tile = half_rows // 2 if half_rows % 32 == 0 else half_rows

    def half_block(which, q):
        return pl.ds(pl.multiple_of((which * ACROSS + q) * rb, rb), rb)

    def gradient_parts(other_ref):
        def turn(t, carried):
            rows = pl.ds(pl.multiple_of(t * tile, tile), tile)
            for k, part in enumerate(split2(conj_product(query_grad_ref[rows], other_ref[rows]))):
                grads[k, rows] = part
            return carried

        lax.fori_loop(0, edges // tile, turn, 0)

    def summed_rows(index_ref, first, count):
        number = lax.broadcasted_iota(jnp.int32, (count, edges), 0) + first
        ones = jnp.where(number == index_ref[...], 1.0, 0.0).astype(jnp.bfloat16)
        return mxu(ones, grads[1], NN) + mxu(ones, grads[0], NN)

    def half_sums(which):
        def turn(t, carried):
            first = pl.multiple_of(which * half_rows + t * put_tile, put_tile)
            part_ref[pl.ds(first, put_tile)] = summed_rows(edge_relation_ref, first, put_tile)
            return carried

        lax.fori_loop(0, half_rows // put_tile, turn, 0)

    gradient_parts(heads_ref)
    half_sums(1 - core)

    def pack_other(q, carried):
        store_packed(r0send.at[q], part_ref[half_block(1 - core, q)])
        return carried

    lax.fori_loop(0, ACROSS, pack_other, 0)
    pair = remote(r0send, r0recv, r0_s, r0_r, shard=partner)
    pair.start()
    half_sums(core)

    def pack_own(q, carried):
        store_packed(r1.at[q], part_ref[half_block(core, q)])
        return carried

    lax.fori_loop(0, ACROSS, pack_own, 0)
    trecv[shard] = tsend[shard]
    pick[...] = picked(moved_index_ref[...], owned)

    def placed(value):
        v0, v1 = split2(value)
        return mxu(pick[...], v1, NN) + mxu(pick[...], v0, NN)

    def tails(ref):
        def turn(p, carried):
            values[pl.ds(pl.multiple_of(p * block, block), block)] = unpack_tail(ref[p, 3 * block :], block)
            return carried

        lax.fori_loop(0, shards, turn, 0)
        return values[...]

    def pass_on(stage):
        def wait_target(k, carried):
            frm = lax.rem(shard + k, shards)
            target_copy(stage, frm, frm).wait_recv()
            return carried

        lax.fori_loop(1, shards, wait_target, 0)
        chunk = trecv[:, stage * block : (stage + 1) * block].reshape(shards * block, 128)
        dense[stage * owned : (stage + 1) * owned] = placed(chunk)
        if stage == 2:
            dense[3 * owned :] = pack_tail(placed(tails(trecv)))
        passing.send(stage)
        if stage == 2:
            passing.send(3)

    pass_on(0)
    pair.wait_recv()

    def add_pair(q, carried):
        r1[q] = r1[q] + r0recv[q]
        return carried

    lax.fori_loop(0, ACROSS, add_pair, 0)

    def across_copy(to, slot):
        return remote(
            r1.at[to], r1recv.at[slot], r1_s.at[to], r1_r.at[slot], group=layer * ACROSS + to
        )

    def send_across(k, carried):
        across_copy(lax.rem(across + k, ACROSS), across).start()
        return carried

    lax.fori_loop(1, ACROSS, send_across, 0)
    pass_on(1)
    passing.relay(0)

    gradient_parts(rels_ref)

    def put_source(t, carried):
        value = summed_rows(edge_source_ref, t * tile, tile)
        for j in range(tile // block):
            store_packed(ssend.at[t * (tile // block) + j], value[j * block : (j + 1) * block])
        return carried

    lax.fori_loop(0, shards * block // tile, put_source, 0)

    def source_copy(to, slot):
        return remote(ssend.at[to], srecv.at[slot], s_s.at[to], s_r.at[slot], shard=to)

    def send_source(k, carried):
        source_copy(lax.rem(shard + k, shards), shard).start()
        return carried

    lax.fori_loop(1, shards, send_source, 0)
    srecv[shard] = ssend[shard]
    passing.relay(1)
    pass_on(2)

    r2[...] = jnp.zeros_like(r2)

    def wait_across(k, carried):
        frm = lax.rem(across + k, ACROSS)
        across_copy(frm, frm).wait_recv()
        return carried

    lax.fori_loop(1, ACROSS, wait_across, 0)
    r1recv[across] = r1[across]
    total = (r1recv[0] + r1recv[1]) + (r1recv[2] + r1recv[3])
    size, piece = total.shape[0], r2.shape[1]
    for m in range(members):
        count = min(piece, size - m * piece)
        if count > 0:
            r2[m, :count] = total[m * piece : m * piece + count]

    def member_copy(to, slot):
        return remote(r2.at[to], r2recv.at[slot], r2_s.at[to], r2_r.at[slot], **member(to))

    def send_member(k, carried):
        member_copy(lax.rem(place + k, members), place).start()
        return carried

    def wait_member(k, carried):
        frm = lax.rem(place + k, members)
        member_copy(frm, frm).wait_recv()
        return carried

    lax.fori_loop(1, members, send_member, 0)
    passing.relay(2)
    passing.relay(3)
    r2recv[place] = r2[place]
    lax.fori_loop(1, members, wait_member, 0)
    r3[...] = jnp.sum(r2recv[...], axis=0)

    def share_copy(to, slot):
        return remote(r3, r3recv.at[slot], r3_s.at[to], r3_r.at[slot], **member(to))

    def send_share(k, carried):
        share_copy(lax.rem(place + k, members), place).start()
        return carried

    def wait_share(k, carried):
        frm = lax.rem(place + k, members)
        share_copy(frm, frm).wait_recv()
        return carried

    lax.fori_loop(1, members, send_share, 0)
    r3recv[place] = r3[...]
    lax.fori_loop(1, members, wait_share, 0)

    def updated(params_, state, gradient):
        squares = sum(jnp.sum(g * g, axis=1, keepdims=True) for g in gradient)
        root = jnp.sqrt(state + squares / width)
        return [p - LEARN_RATE * g / root for p, g in zip(params_, gradient)]

    summed = r3recv[...].reshape(members * piece, 128)
    gradient = [summed[c * rb : (c + 1) * rb] for c in range(3)]
    gradient.append(unpack_tail(summed[3 * rb : size], rb))
    state = column_of(relation_state_ref, (core * ACROSS + across) * rb, rb)
    fresh = updated(load_wide(relation_ref, half_block(core, across), rb, last), state, gradient)
    store_packed(r4.at[across], jnp.concatenate(fresh, axis=1))

    def spread_copy(to):
        return remote(
            r4.at[across], r4.at[across], r4_s.at[to], r4_r.at[across], group=layer * ACROSS + to
        )

    def spread_wait(frm):
        return remote(r4.at[frm], r4.at[frm], r4_s.at[frm], r4_r.at[frm], group=layer * ACROSS + frm)

    def hand_copy(q):
        return remote(r4.at[q], r5.at[q], r5_s.at[q], r5_r.at[q], shard=partner)

    def send_spread(k, carried):
        spread_copy(lax.rem(across + k, ACROSS)).start()
        return carried

    lax.fori_loop(1, ACROSS, send_spread, 0)
    hand_copy(across).start()

    def wait_source(k, carried):
        frm = lax.rem(shard + k, shards)
        source_copy(frm, frm).wait_recv()
        return carried

    lax.fori_loop(1, shards, wait_source, 0)
    pick[...] = picked(source_index_ref[...], owned)
    for c in range(3):
        dense_own[c] = placed(srecv[:, c * block : (c + 1) * block].reshape(shards * block, 128))
    dense_own[3] = placed(tails(srecv))
    for i in range(4):
        passing.wait(i)
    parts, tail = load_packed(moved, owned)
    parts.append(tail)
    gradient = [dense_own[c] + parts[c] for c in range(4)]
    entity_wide = load_wide(entity_ref, slice(None), owned, last)
    fresh = updated(entity_wide, column_of(entity_state_ref, 0, owned), gradient)
    store_narrow(entity_new_ref, slice(None), fresh)

    def forward(k, carried):
        frm = lax.rem(across + k, ACROSS)
        spread_wait(frm).wait_recv()
        hand_copy(frm).start()
        return carried

    lax.fori_loop(1, ACROSS, forward, 0)

    def put_out(which, ref):
        def turn(q, carried):
            got, tail_ = load_packed(ref.at[q], rb)
            store_narrow(relation_new_ref, half_block(which, q), (*got, tail_))
            return carried

        lax.fori_loop(0, ACROSS, turn, 0)

    put_out(core, r4)

    def take_hand(q, carried):
        hand_copy(q).wait_recv()
        return carried

    lax.fori_loop(0, ACROSS, take_hand, 0)
    put_out(1 - core, r5)

    for stage in range(3):
        def end_target(k, carried, stage=stage):
            to = lax.rem(shard + k, shards)
            target_copy(stage, to, shard).wait_send()
            return carried

        lax.fori_loop(1, shards, end_target, 0)
    passing.end()

    def end_shard(k, carried):
        source_copy(lax.rem(shard + k, shards), shard).wait_send()
        return carried

    def end_across(k, carried):
        to = lax.rem(across + k, ACROSS)
        across_copy(to, across).wait_send()
        spread_copy(to).wait_send()
        return carried

    def end_member(k, carried):
        to = lax.rem(place + k, members)
        member_copy(to, place).wait_send()
        share_copy(to, place).wait_send()
        return carried

    def end_hand(q, carried):
        hand_copy(q).wait_send()
        return carried

    lax.fori_loop(1, shards, end_shard, 0)
    lax.fori_loop(1, ACROSS, end_across, 0)
    lax.fori_loop(1, members, end_member, 0)
    lax.fori_loop(0, ACROSS, end_hand, 0)
    pair.wait_send()


def back_step(sizes, *operands):
    shards, groups, block, owned, width = sizes
    padded = operands[6].shape[0]
    edges = operands[1].shape[0]
    members = shards // 2 * groups // ACROSS
    size = packed_rows(padded // (2 * ACROSS))
    piece = 8 * (-(-size // (8 * members)))
    f32 = jnp.float32
    table = pltpu.VMEM((shards, packed_rows(block), 128), f32)
    flat = pltpu.VMEM((packed_rows(owned), 128), f32)
    half = pltpu.VMEM((ACROSS, size, 128), f32)
    pieces = pltpu.VMEM((members, piece, 128), f32)
    dma = pltpu.SemaphoreType.DMA
    return pl.pallas_call(
        functools.partial(back_kernel, sizes),
        in_specs=[pl.BlockSpec(memory_space=pltpu.VMEM)] * len(operands),
        out_specs=[pl.BlockSpec(memory_space=pltpu.VMEM)] * 2,
        out_shape=[jax.ShapeDtypeStruct((owned, width), f32), jax.ShapeDtypeStruct((padded, width), f32)],
        scratch_shapes=[
            table, table, table, table, flat, flat, flat,
            pltpu.VMEM((owned, shards * block), jnp.bfloat16),
            pltpu.VMEM((shards * block, 128), f32),
            pltpu.VMEM((2, edges, WIDE), jnp.bfloat16),
            pltpu.VMEM((padded, WIDE), f32),
            pltpu.VMEM((owned, 128), f32),
            pltpu.VMEM((4, owned, 128), f32),
            half, half, half, half, pieces, pieces, pltpu.VMEM((piece, 128), f32), pieces, half, half,
            dma((3, shards)), dma((3, shards)), dma((shards,)), dma((shards,)),
            dma((4,)), dma((4,)), dma((4,)), dma((4,)), dma, dma, dma((ACROSS,)), dma((ACROSS,)),
            dma((members,)), dma((members,)), dma((members,)), dma((members,)),
            dma((ACROSS,)), dma((ACROSS,)), dma((ACROSS,)), dma((ACROSS,)),
        ],
        compiler_params=pltpu.CompilerParams(
            collective_id=1, has_side_effects=True, vmem_limit_bytes=60 << 20
        ),
        name="back_step",
    )(*operands)


def front_kernel(
    sizes,
    entity_ref, relation_ref, source_index_ref, target_index_ref, edge_source_ref, edge_relation_ref,
    table_ref, heads_ref, rels_ref, queries_ref, moved_index_ref,
    esend, evia, erecv, isend, irecv, eparts, rparts, sparts, pick, ssend, srecv, tsend, trecv, values, last,
    e_s, e_r, e_v, e_h, i_s, i_r, s_s, s_r, t_s, t_r,
):
    shards, groups, block, owned, width = sizes
    shard, group = lax.axis_index("shard"), lax.axis_index("group")
    before = lax.rem(group + groups - 1, groups)
    edges, padded = edge_source_ref.shape[1], relation_ref.shape[0]
    table_rows = shards * block
    tile = 256
    stages = ((0, block), (block, block), (2 * block, packed_rows(block) - 2 * block))

    isend[...] = target_index_ref[...]
    wide = load_wide(entity_ref, slice(None), owned, last)
    for c in range(3):
        esend[c * owned : (c + 1) * owned] = wide[c]
    esend[3 * owned :] = pack_tail(wide[3])
    greet(shards, groups, shard, group)

    index_copy = remote(isend, irecv, i_s, i_r, group=before)
    index_copy.start()

    passing = Passing(groups, group, -1, owned, esend, evia, erecv, e_s, e_r, e_v, e_h)
    for i in range(4):
        passing.send(i)

    for c in range(4):
        for k, part in enumerate(split3(wide[c])):
            eparts[k, :, 128 * c : 128 * c + 128] = part

    def taken(parts, index_ref, t, count):
        ones = picked(index_ref[:, pl.ds(pl.multiple_of(t * tile, tile), tile)], count)
        return (mxu(ones, parts[0], TN) + mxu(ones, parts[1], TN)) + mxu(ones, parts[2], TN)

    def take_source(t, carried):
        value = taken(eparts, source_index_ref, t, owned)
        for j in range(tile // block):
            store_packed(ssend.at[t * (tile // block) + j], value[j * block : (j + 1) * block])
        return carried

    lax.fori_loop(0, table_rows // tile, take_source, 0)

    def source_copy(to, slot):
        return remote(ssend.at[to], srecv.at[slot], s_s.at[to], s_r.at[slot], shard=to)

    def send_source(k, carried):
        source_copy(lax.rem(shard + k, shards), shard).start()
        return carried

    lax.fori_loop(1, shards, send_source, 0)
    srecv[shard] = ssend[shard]
    passing.relay(0)
    passing.relay(1)

    step = 128 if padded % 128 == 0 else 32

    def split_relation(t, carried):
        rows = pl.ds(pl.multiple_of(t * step, step), step)
        for c, x in enumerate(load_wide(relation_ref, rows, step, last)):
            for k, part in enumerate(split3(x)):
                rparts[k, rows, 128 * c : 128 * c + 128] = part
        return carried

    lax.fori_loop(0, padded // step, split_relation, 0)
    passing.relay(2)
    passing.relay(3)

    def take_relation(t, carried):
        rels_ref[pl.ds(pl.multiple_of(t * tile, tile), tile)] = taken(rparts, edge_relation_ref, t, padded)
        return carried

    lax.fori_loop(0, edges // tile, take_relation, 0)

    index_copy.wait_recv()
    moved_index_ref[...] = irecv[...]
    pick[...] = picked(irecv[...], owned)

    def found(chunk):
        value = mxu(pick[...], jnp.concatenate(split3(chunk), axis=1), TN)
        return (value[:, :128] + value[:, 128:256]) + value[:, 256:]

    def target_copy(stage, to, slot):
        first, size = stages[stage]
        rows = pl.ds(first, size)
        return remote(
            tsend.at[to, rows], trecv.at[slot, rows], t_s.at[stage, to], t_r.at[stage, slot], shard=to
        )

    for stage in range(3):
        passing.wait(stage)
        if stage == 2:
            passing.wait(3)
        chunk = erecv[stage * owned : (stage + 1) * owned]
        tsend[:, stage * block : (stage + 1) * block] = found(chunk).reshape(shards, block, 128)
        if stage == 2:
            values[...] = found(unpack_tail(erecv[3 * owned :], owned))

            def pack_tails(p, carried):
                rows = pl.ds(pl.multiple_of(p * block, block), block)
                tsend[p, 3 * block :] = pack_tail(values[rows])
                return carried

            lax.fori_loop(0, shards, pack_tails, 0)

        def send_target(k, carried, stage=stage):
            target_copy(stage, lax.rem(shard + k, shards), shard).start()
            return carried

        lax.fori_loop(1, shards, send_target, 0)
    trecv[shard] = tsend[shard]

    def wait_source(k, carried):
        frm = lax.rem(shard + k, shards)
        source_copy(frm, frm).wait_recv()
        return carried

    lax.fori_loop(1, shards, wait_source, 0)

    def split_source(p, carried):
        rows = pl.ds(pl.multiple_of(p * block, block), block)
        parts, tail = load_packed(srecv.at[p], block)
        for c, x in enumerate((*parts, tail)):
            for k, part in enumerate(split3(x)):
                sparts[k, rows, 128 * c : 128 * c + 128] = part
        return carried

    lax.fori_loop(0, shards, split_source, 0)

    def make_queries(t, carried):
        rows = pl.ds(pl.multiple_of(t * tile, tile), tile)
        heads = taken(sparts, edge_source_ref, t, table_rows)
        heads_ref[rows] = heads
        queries_ref[rows] = product(heads, rels_ref[rows])
        return carried

    lax.fori_loop(0, edges // tile, make_queries, 0)

    for stage in range(3):
        def wait_target(k, carried, stage=stage):
            frm = lax.rem(shard + k, shards)
            target_copy(stage, frm, frm).wait_recv()
            return carried

        lax.fori_loop(1, shards, wait_target, 0)

    def put_table(p, carried):
        rows = pl.ds(pl.multiple_of(p * block, block), block)
        parts, tail = load_packed(trecv.at[p], block)
        for c, x in enumerate((*parts, tail)):
            table_ref[rows, 128 * c : 128 * c + 128] = x
        return carried

    lax.fori_loop(0, shards, put_table, 0)

    index_copy.wait_send()
    for stage in range(3):
        def end_target(k, carried, stage=stage):
            target_copy(stage, lax.rem(shard + k, shards), shard).wait_send()
            return carried

        lax.fori_loop(1, shards, end_target, 0)
    passing.end()

    def end_source(k, carried):
        source_copy(lax.rem(shard + k, shards), shard).wait_send()
        return carried

    lax.fori_loop(1, shards, end_source, 0)


def front_step(sizes, *operands):
    shards, groups, block, owned, width = sizes
    padded, edges, table_rows = operands[1].shape[0], operands[4].shape[1], shards * block
    f32, bf16 = jnp.float32, jnp.bfloat16
    table = pltpu.VMEM((shards, packed_rows(block), 128), f32)
    flat = pltpu.VMEM((packed_rows(owned), 128), f32)
    index = pltpu.VMEM((1, table_rows), jnp.int32)
    dma = pltpu.SemaphoreType.DMA
    return pl.pallas_call(
        functools.partial(front_kernel, sizes),
        in_specs=[pl.BlockSpec(memory_space=pltpu.VMEM)] * len(operands),
        out_specs=[pl.BlockSpec(memory_space=pltpu.VMEM)] * 5,
        out_shape=[
            jax.ShapeDtypeStruct((table_rows, WIDE), f32),
            jax.ShapeDtypeStruct((edges, WIDE), f32),
            jax.ShapeDtypeStruct((edges, WIDE), f32),
            jax.ShapeDtypeStruct((edges, WIDE), f32),
            jax.ShapeDtypeStruct((1, table_rows), jnp.int32),
        ],
        scratch_shapes=[
            flat, flat, flat, index, index,
            pltpu.VMEM((3, owned, WIDE), bf16),
            pltpu.VMEM((3, padded, WIDE), bf16),
            pltpu.VMEM((3, table_rows, WIDE), bf16),
            pltpu.VMEM((owned, table_rows), bf16),
            table, table, table, table,
            pltpu.VMEM((table_rows, 128), f32),
            pltpu.VMEM((owned, 128), f32),
            dma((4,)), dma((4,)), dma((4,)), dma((4,)), dma, dma,
            dma((shards,)), dma((shards,)), dma((3, shards)), dma((3, shards)),
        ],
        compiler_params=pltpu.CompilerParams(
            collective_id=0, has_side_effects=True, vmem_limit_bytes=60 << 20
        ),
        name="front_step",
    )(*operands)


def on_device(
    entity,
    entity_state,
    relation,
    relation_state,
    src_send,
    dst_send,
    edge_source,
    edge_relation,
    edge_target,
    neg_slots,
    edge_count,
):
    width = entity.shape[1]
    owned = entity.shape[0]
    relations = relation.shape[0]
    peers, block = src_send.shape[1], src_send.shape[2]
    table_rows = peers * block
    edges = edge_source.shape[0]
    spans = edges // SPAN
    groups, shards = lax.axis_size("group"), lax.axis_size("shard")
    unit = max(8 * shards, 16 * ACROSS)
    padded = unit * (-(-relations // unit))

    relation_rows = jnp.pad(relation, ((0, padded - relations), (0, 0)))
    relation_states = jnp.pad(relation_state, (0, padded - relations), constant_values=1.0).reshape(1, padded)
    sizes = (shards, groups, block, owned, width)
    source_index = src_send.reshape(1, table_rows)
    edge_sources, edge_relations = edge_source.reshape(1, edges), edge_relation.reshape(1, edges)
    target_table, heads, rels, queries, moved_index = front_step(
        sizes,
        entity,
        relation_rows,
        source_index,
        dst_send.reshape(1, table_rows),
        edge_sources,
        edge_relations,
    )
    loss, query_grad, target_grad = span_step(
        edge_count,
        edge_target.reshape(spans, 1, SPAN),
        neg_slots.reshape(spans, 1, neg_slots.shape[1]),
        queries,
        target_table,
    )
    entity_new, relation_new = back_step(
        sizes,
        target_grad,
        query_grad,
        heads,
        rels,
        edge_sources,
        edge_relations,
        relation_rows,
        relation_states,
        moved_index,
        source_index,
        entity,
        entity_state.reshape(1, owned),
    )
    return entity_new, relation_new[:relations], loss.reshape(edges)


def solution(mesh):
    return jax.shard_map(
        on_device,
        mesh=mesh,
        in_specs=(
            P(("group", "shard"), None),
            P(("group", "shard")),
            P(),
            P(),
            P(("group", "shard"), None, None),
            P(("group", "shard"), None, None),
            P(("group", "shard")),
            P(("group", "shard")),
            P(("group", "shard")),
            P(("group", "shard"), None),
            P(("group", "shard")),
        ),
        out_specs=(P(("group", "shard"), None), P(), P(("group", "shard"))),
        check_vma=False,
    )
```

```python
import functools

import jax
import jax.numpy as jnp
from jax import lax
from jax.experimental import pallas as pl
from jax.experimental.pallas import tpu as pltpu
from jax.sharding import PartitionSpec as P

SPAN = 512
LEARN_RATE = 0.5
WIDE = 512
TAIL = 8
ACROSS = 4
MESH = pl.DeviceIdType.MESH

NT = (((1,), (1,)), ((), ()))
NN = (((1,), (0,)), ((), ()))
TN = (((0,), (0,)), ((), ()))


def split2(x):
    hi = x.astype(jnp.bfloat16)
    lo = (x - hi.astype(jnp.float32)).astype(jnp.bfloat16)
    return hi, lo


def split3(x):
    hi = x.astype(jnp.bfloat16)
    rest = x - hi.astype(jnp.float32)
    mid = rest.astype(jnp.bfloat16)
    lo = (rest - mid.astype(jnp.float32)).astype(jnp.bfloat16)
    return hi, mid, lo


def mxu(a, b, dims):
    return lax.dot_general(a, b, dims, preferred_element_type=jnp.float32)


def lane_of(x):
    return lax.broadcasted_iota(jnp.int32, x.shape, 1)


def widened(x0, x1, x2, x3):
    lane = lane_of(x0)
    imag = jnp.where(lane < 56, pltpu.roll(x1, 56, 1), pltpu.roll(x2, 56, 1))
    both = jnp.where(
        lane < 64, x1, jnp.where(lane < 120, pltpu.roll(x2, 120, 1), pltpu.roll(x3, 120, 1))
    )
    tail = jnp.where(lane < 8, pltpu.roll(x1, 64, 1), jnp.where(lane < 16, x3, 0.0))
    return x0, imag, both, tail


def narrowed(real, imag, both, tail):
    lane = lane_of(real)
    imag_on, both_on = pltpu.roll(imag, 72, 1), pltpu.roll(both, 8, 1)
    x1 = jnp.where(lane < 64, both, jnp.where(lane < 72, pltpu.roll(tail, 64, 1), imag_on))
    x2 = jnp.where(lane < 72, imag_on, both_on)
    return real, x1, x2, jnp.where(lane < 8, both_on, tail)


def load_wide(ref, rows, count, last):
    last[:count] = jnp.zeros((count, 128), jnp.float32)
    last[:count, :16] = ref[rows, 384:400]
    return widened(ref[rows, 0:128], ref[rows, 128:256], ref[rows, 256:384], last[:count])


def store_narrow(ref, rows, parts):
    x = narrowed(*parts)
    for c in range(3):
        ref[rows, 128 * c : 128 * c + 128] = x[c]
    ref[rows, 384:400] = x[3][:, :16]


def column_of(row_ref, first, count):
    n = row_ref.shape[1]
    lane = lax.broadcasted_iota(jnp.int32, (count, n), 1)
    own = lax.broadcasted_iota(jnp.int32, (count, n), 0) + first
    return jnp.sum(jnp.where(lane == own, row_ref[...], 0.0), axis=1, keepdims=True)


def swapped(x, half):
    lane = lax.broadcasted_iota(jnp.int32, x.shape, 1)
    if half == 64:
        return pltpu.roll(x, 64, 1), lane < half
    left, right = pltpu.roll(x, 128 - half, 1), pltpu.roll(x, half, 1)
    mixed = jnp.where(lane < half, left, jnp.where(lane < 2 * half, right, 0.0))
    return mixed, lane < half


def mixed_product(a, b, half, sign):
    other_a, low = swapped(a, half)
    other_b, _ = swapped(b, half)
    real = jnp.where(low, b, other_b)
    imag = jnp.where(low, -other_b, b)
    return a * real + sign * (other_a * imag)


def product_of(a, b, sign):
    ar, ai, br, bi = a[:, :128], a[:, 128:256], b[:, :128], b[:, 128:256]
    return jnp.concatenate(
        [
            ar * br - sign * (ai * bi),
            ai * br + sign * (ar * bi),
            mixed_product(a[:, 256:384], b[:, 256:384], 64, sign),
            mixed_product(a[:, 384:], b[:, 384:], TAIL, sign),
        ],
        axis=1,
    )


def product(a, b):
    return product_of(a, b, 1.0)


def conj_product(a, b):
    return product_of(a, b, -1.0)


def picked(index, count):
    rows = lax.broadcasted_iota(jnp.int32, (count, index.shape[1]), 0)
    return jnp.where(rows == index, 1.0, 0.0).astype(jnp.bfloat16)


def span_part(
    span, count_ref, target_ref, slots_ref, query_ref, table_ref,
    loss_ref, query_grad_ref, target_grad_ref,
    score_ref, times_ref, parts_ref, query_parts_ref,
):
    table_rows = table_ref.shape[0]
    tile = min(256, table_rows)
    tiles = table_rows // tile

    edges_here = pl.ds(pl.multiple_of(span * SPAN, SPAN), SPAN)

    for k, part in enumerate(split3(query_ref[edges_here])):
        query_parts_ref[k] = part

    edge = lax.broadcasted_iota(jnp.int32, (1, SPAN), 1) + span * SPAN
    live = jnp.where(edge < count_ref[0], 1.0, 0.0)
    target = target_ref[span]
    slots = slots_ref[span]

    def score_turn(t, carried):
        peak, pos = carried
        rows = pl.ds(pl.multiple_of(t * tile, tile), tile)
        t0, t1, t2 = parts_ref[0, rows], parts_ref[1, rows], parts_ref[2, rows]
        q0, q1, q2 = query_parts_ref[0], query_parts_ref[1], query_parts_ref[2]
        small = mxu(t0, q2, NT) + mxu(t2, q0, NT) + mxu(t1, q1, NT)
        score = (small + (mxu(t0, q1, NT) + mxu(t1, q0, NT))) + mxu(t0, q0, NT)
        score_ref[rows] = score
        number = lax.broadcasted_iota(jnp.int32, (tile, 1), 0) + t * tile
        times = jnp.sum(jnp.where(slots == number, 1.0, 0.0), axis=1, keepdims=True)
        times_ref[rows] = times
        used = jnp.where(times > 0.0, score, -jnp.inf)
        peak = jnp.maximum(peak, jnp.max(used, axis=0, keepdims=True))
        pos = pos + jnp.sum(jnp.where(target == number, score, 0.0), axis=0, keepdims=True)
        return peak, pos

    start = (jnp.full((1, SPAN), -jnp.inf, jnp.float32), jnp.zeros((1, SPAN), jnp.float32))
    peak, pos = lax.fori_loop(0, tiles, score_turn, start)
    peak = jnp.maximum(peak, pos)

    def total_turn(t, total):
        rows = pl.ds(pl.multiple_of(t * tile, tile), tile)
        times = times_ref[rows]
        value = jnp.where(times > 0.0, times * jnp.exp(score_ref[rows] - peak), 0.0)
        score_ref[rows] = value
        return total + jnp.sum(value, axis=0, keepdims=True)

    total = lax.fori_loop(0, tiles, total_turn, jnp.exp(pos - peak))
    log_total = peak + jnp.log(total)
    loss_ref[span] = (log_total - pos) * live
    pos_grad = (jnp.exp(pos - log_total) - 1.0) * live
    scale = jnp.exp(peak - log_total) * live
    query_grad_ref[edges_here] = jnp.zeros((SPAN, WIDE), jnp.float32)

    def grad_turn(t, carried):
        rows = pl.ds(pl.multiple_of(t * tile, tile), tile)
        number = lax.broadcasted_iota(jnp.int32, (tile, 1), 0) + t * tile
        weight = score_ref[rows] * scale + jnp.where(target == number, pos_grad, 0.0)
        w0, w1 = split2(weight)
        t0, t1 = parts_ref[0, rows], parts_ref[1, rows]
        q0, q1 = query_parts_ref[0], query_parts_ref[1]
        query_grad_ref[edges_here] += (mxu(w0, t1, TN) + mxu(w1, t0, TN)) + mxu(w0, t0, TN)
        target_grad_ref[rows] += (mxu(w0, q1, NN) + mxu(w1, q0, NN)) + mxu(w0, q0, NN)
        return carried

    lax.fori_loop(0, tiles, grad_turn, 0)


def pack_tail(x):
    rows = x.shape[0]
    packed = []
    for first in range(0, rows, 64):
        total = x[first : first + 8]
        for k in range(1, min(8, (rows - first) // 8)):
            total = total + pltpu.roll(x[first + 8 * k : first + 8 * k + 8], 16 * k, 1)
        packed.append(total)
    return packed[0] if len(packed) == 1 else jnp.concatenate(packed, axis=0)


def unpack_tail(x, rows):
    lane = lax.broadcasted_iota(jnp.int32, (8, 128), 1)
    tiles = []
    for t in range(rows // 8):
        part = x[8 * (t // 8) : 8 * (t // 8) + 8]
        k = t % 8
        part = part if k == 0 else pltpu.roll(part, 128 - 16 * k, 1)
        tiles.append(jnp.where(lane < 16, part, 0.0))
    return tiles[0] if len(tiles) == 1 else jnp.concatenate(tiles, axis=0)


def packed_rows(rows):
    return 3 * rows + 8 * (-(-rows // 64))


def store_packed(ref, x):
    n = x.shape[0]
    for c in range(3):
        ref[c * n : (c + 1) * n] = x[:, 128 * c : 128 * c + 128]
    ref[3 * n :] = pack_tail(x[:, 384:])


def load_packed(ref, n):
    parts = [ref[c * n : (c + 1) * n] for c in range(3)]
    return parts, unpack_tail(ref[3 * n :], n)


def remote(src, dst, send, recv, **device):
    return pltpu.make_async_remote_copy(
        src_ref=src, dst_ref=dst, send_sem=send, recv_sem=recv, device_id=device, device_id_type=MESH
    )


def greet(shards, groups, shard, group, team=None):
    barrier = pltpu.get_barrier_semaphore()

    def near(k, carried):
        pl.semaphore_signal(
            barrier, inc=1, device_id={"shard": lax.rem(shard + k, shards)}, device_id_type=MESH
        )
        return carried

    def far(k, carried):
        pl.semaphore_signal(
            barrier, inc=1, device_id={"group": lax.rem(group + k, groups)}, device_id_type=MESH
        )
        return carried

    lax.fori_loop(1, shards, near, 0)
    lax.fori_loop(1, groups, far, 0)
    met = shards + groups - 2
    if team is not None:
        count, place, member = team

        def wide_signal(k, carried):
            pl.semaphore_signal(
                barrier, inc=1, device_id=member(lax.rem(place + k, count)), device_id_type=MESH
            )
            return carried

        lax.fori_loop(1, count, wide_signal, 0)
        met = met + count - 1
    pl.semaphore_wait(barrier, met)


class Passing:
    def __init__(self, groups, group, by, owned, rows_ref, via_ref, out_ref, sent, came, via_came, handed):
        layers = groups // ACROSS
        x, layer = lax.rem(group, ACROSS), lax.div(group, ACROSS)
        ahead = lax.rem(layer + by + layers, layers)
        first, last = (ACROSS - 1, 0) if by > 0 else (0, ACROSS - 1)
        self.x, self.first, self.last = x, first, last
        self.direct = lax.rem(group + by + groups, groups)
        self.over = (layer * ACROSS + last, ahead * ACROSS + first)
        self.final = (ahead * ACROSS + last, layer * ACROSS + last)
        rest = packed_rows(owned) - 2 * owned
        part = 8 * (rest // 16)
        self.pieces = ((0, owned), (owned, owned), (2 * owned, part), (2 * owned + part, rest - part))
        self.refs = (rows_ref, via_ref, out_ref)
        self.sems = (sent, came, via_came, handed)

    def copy(self, i, kind):
        rows = pl.ds(*self.pieces[i])
        rows_ref, via_ref, out_ref = self.refs
        sent, came, via_came, handed = self.sems
        if kind == "direct":
            return remote(rows_ref.at[rows], out_ref.at[rows], sent.at[i], came.at[i], group=self.direct)
        if kind == "over":
            return remote(
                rows_ref.at[rows], via_ref.at[rows], sent.at[i], via_came.at[i], group=self.over[i % 2]
            )
        return remote(via_ref.at[rows], out_ref.at[rows], handed.at[i], came.at[i], group=self.final[i % 2])

    def send(self, i):
        @pl.when(self.x != self.first)
        def _():
            self.copy(i, "direct").start()

        @pl.when(self.x == self.first)
        def _():
            self.copy(i, "over").start()

    def relay(self, i):
        @pl.when(self.x == (self.last if i % 2 == 0 else self.first))
        def _():
            self.copy(i, "over").wait_recv()
            self.copy(i, "final").start()

    def wait(self, i):
        self.copy(i, "direct").wait_recv()

    def end(self):
        for i in range(4):
            self.copy(i, "direct").wait_send()

            @pl.when(self.x == (self.last if i % 2 == 0 else self.first))
            def _():
                self.copy(i, "final").wait_send()


def back_part(
    sizes, team,
    target_ref, query_grad_ref, heads_ref, rels_ref, edge_source_ref, edge_relation_ref,
    relation_ref, relation_state_ref, moved_index_ref, source_index_ref, entity_ref, entity_state_ref,
    entity_new_ref, relation_new_ref,
    tsend, trecv, ssend, srecv, dense, via, moved, pick, values, grads, part_ref, last, dense_own,
    r0send, r0recv, r1, r1recv, r2, r2recv, r3, r3recv, r4, r5,
    t_s, t_r, s_s, s_r, p_s, p_r, p_v, p_h, r0_s, r0_r, r1_s, r1_r, r2_s, r2_r, r3_s, r3_r, r4_s, r4_r, r5_s, r5_r,
):
    shards, groups, block, owned, width = sizes
    chips = shards // 2
    shard, group = lax.axis_index("shard"), lax.axis_index("group")
    core, chip = lax.rem(shard, 2), lax.div(shard, 2)
    partner = shard + 1 - 2 * core
    rb = relation_ref.shape[0] // (2 * ACROSS)
    members = r2.shape[0]
    across, layer = lax.rem(group, ACROSS), lax.div(group, ACROSS)
    _, place, member = team
    stages = ((0, block), (block, block), (2 * block, packed_rows(block) - 2 * block))
    passing = Passing(groups, group, 1, owned, dense, via, moved, p_s, p_r, p_v, p_h)

    def pack_target(p, carried):
        rows = pl.ds(pl.multiple_of(p * block, block), block)
        store_packed(tsend.at[p], target_ref[rows])
        return carried

    lax.fori_loop(0, shards, pack_target, 0)

    def target_copy(stage, to, slot):
        first, size = stages[stage]
        rows = pl.ds(first, size)
        return remote(
            tsend.at[to, rows], trecv.at[slot, rows], t_s.at[stage, to], t_r.at[stage, slot], shard=to
        )

    for stage in range(3):
        def send_target(k, carried, stage=stage):
            to = lax.rem(shard + k, shards)
            target_copy(stage, to, shard).start()
            return carried

        lax.fori_loop(1, shards, send_target, 0)

    edges = query_grad_ref.shape[0]
    padded = relation_ref.shape[0]
    tile = 256
    half_rows = padded // 2
    put_tile = half_rows // 2 if half_rows % 32 == 0 else half_rows

    def half_block(which, q):
        return pl.ds(pl.multiple_of((which * ACROSS + q) * rb, rb), rb)

    def gradient_parts(other_ref):
        def turn(t, carried):
            rows = pl.ds(pl.multiple_of(t * tile, tile), tile)
            for k, part in enumerate(split2(conj_product(query_grad_ref[rows], other_ref[rows]))):
                grads[k, rows] = part
            return carried

        lax.fori_loop(0, edges // tile, turn, 0)

    def summed_rows(index_ref, first, count):
        number = lax.broadcasted_iota(jnp.int32, (count, edges), 0) + first
        ones = jnp.where(number == index_ref[...], 1.0, 0.0).astype(jnp.bfloat16)
        return mxu(ones, grads[1, :edges], NN) + mxu(ones, grads[0, :edges], NN)

    def half_sums(which):
        def turn(t, carried):
            first = pl.multiple_of(which * half_rows + t * put_tile, put_tile)
            part_ref[pl.ds(first, put_tile)] = summed_rows(edge_relation_ref, first, put_tile)
            return carried

        lax.fori_loop(0, half_rows // put_tile, turn, 0)

    gradient_parts(heads_ref)
    half_sums(1 - core)

    def pack_other(q, carried):
        store_packed(r0send.at[q], part_ref[half_block(1 - core, q)])
        return carried

    lax.fori_loop(0, ACROSS, pack_other, 0)
    pair = remote(r0send, r0recv, r0_s, r0_r, shard=partner)
    pair.start()
    half_sums(core)

    def pack_own(q, carried):
        store_packed(r1.at[q], part_ref[half_block(core, q)])
        return carried

    lax.fori_loop(0, ACROSS, pack_own, 0)
    trecv[shard] = tsend[shard]
    pick[...] = picked(moved_index_ref[...], owned)

    def placed(value):
        v0, v1 = split2(value)
        return mxu(pick[...], v1, NN) + mxu(pick[...], v0, NN)

    def tails(ref):
        def turn(p, carried):
            values[pl.ds(pl.multiple_of(p * block, block), block)] = unpack_tail(ref[p, 3 * block :], block)
            return carried

        lax.fori_loop(0, shards, turn, 0)
        return values[...]

    def pass_on(stage):
        def wait_target(k, carried):
            frm = lax.rem(shard + k, shards)
            target_copy(stage, frm, frm).wait_recv()
            return carried

        lax.fori_loop(1, shards, wait_target, 0)
        chunk = trecv[:, stage * block : (stage + 1) * block].reshape(shards * block, 128)
        dense[stage * owned : (stage + 1) * owned] = placed(chunk)
        if stage == 2:
            dense[3 * owned :] = pack_tail(placed(tails(trecv)))
        passing.send(stage)
        if stage == 2:
            passing.send(3)

    pass_on(0)
    pair.wait_recv()

    def add_pair(q, carried):
        r1[q] = r1[q] + r0recv[q]
        return carried

    lax.fori_loop(0, ACROSS, add_pair, 0)

    def across_copy(to, slot):
        return remote(
            r1.at[to], r1recv.at[slot], r1_s.at[to], r1_r.at[slot], group=layer * ACROSS + to
        )

    def send_across(k, carried):
        across_copy(lax.rem(across + k, ACROSS), across).start()
        return carried

    lax.fori_loop(1, ACROSS, send_across, 0)
    pass_on(1)
    passing.relay(0)

    gradient_parts(rels_ref)

    def put_source(t, carried):
        value = summed_rows(edge_source_ref, t * tile, tile)
        for j in range(tile // block):
            store_packed(ssend.at[t * (tile // block) + j], value[j * block : (j + 1) * block])
        return carried

    lax.fori_loop(0, shards * block // tile, put_source, 0)

    def source_copy(to, slot):
        return remote(ssend.at[to], srecv.at[slot], s_s.at[to], s_r.at[slot], shard=to)

    def send_source(k, carried):
        source_copy(lax.rem(shard + k, shards), shard).start()
        return carried

    lax.fori_loop(1, shards, send_source, 0)
    srecv[shard] = ssend[shard]
    passing.relay(1)
    pass_on(2)

    r2[...] = jnp.zeros_like(r2)

    def wait_across(k, carried):
        frm = lax.rem(across + k, ACROSS)
        across_copy(frm, frm).wait_recv()
        return carried

    lax.fori_loop(1, ACROSS, wait_across, 0)
    r1recv[across] = r1[across]
    total = (r1recv[0] + r1recv[1]) + (r1recv[2] + r1recv[3])
    size, piece = total.shape[0], r2.shape[1]
    for m in range(members):
        count = min(piece, size - m * piece)
        if count > 0:
            r2[m, :count] = total[m * piece : m * piece + count]

    def member_copy(to, slot):
        return remote(r2.at[to], r2recv.at[slot], r2_s.at[to], r2_r.at[slot], **member(to))

    def send_member(k, carried):
        member_copy(lax.rem(place + k, members), place).start()
        return carried

    def wait_member(k, carried):
        frm = lax.rem(place + k, members)
        member_copy(frm, frm).wait_recv()
        return carried

    lax.fori_loop(1, members, send_member, 0)
    passing.relay(2)
    passing.relay(3)
    r2recv[place] = r2[place]
    lax.fori_loop(1, members, wait_member, 0)
    r3[...] = jnp.sum(r2recv[...], axis=0)

    def share_copy(to, slot):
        return remote(r3, r3recv.at[slot], r3_s.at[to], r3_r.at[slot], **member(to))

    def send_share(k, carried):
        share_copy(lax.rem(place + k, members), place).start()
        return carried

    def wait_share(k, carried):
        frm = lax.rem(place + k, members)
        share_copy(frm, frm).wait_recv()
        return carried

    lax.fori_loop(1, members, send_share, 0)
    r3recv[place] = r3[...]
    lax.fori_loop(1, members, wait_share, 0)

    def updated(params_, state, gradient):
        squares = sum(jnp.sum(g * g, axis=1, keepdims=True) for g in gradient)
        root = jnp.sqrt(state + squares / width)
        return [p - LEARN_RATE * g / root for p, g in zip(params_, gradient)]

    summed = r3recv[...].reshape(members * piece, 128)
    gradient = [summed[c * rb : (c + 1) * rb] for c in range(3)]
    gradient.append(unpack_tail(summed[3 * rb : size], rb))
    state = column_of(relation_state_ref, (core * ACROSS + across) * rb, rb)
    fresh = updated(load_wide(relation_ref, half_block(core, across), rb, last), state, gradient)
    store_packed(r4.at[across], jnp.concatenate(fresh, axis=1))

    def spread_copy(to):
        return remote(
            r4.at[across], r4.at[across], r4_s.at[to], r4_r.at[across], group=layer * ACROSS + to
        )

    def spread_wait(frm):
        return remote(r4.at[frm], r4.at[frm], r4_s.at[frm], r4_r.at[frm], group=layer * ACROSS + frm)

    def hand_copy(q):
        return remote(r4.at[q], r5.at[q], r5_s.at[q], r5_r.at[q], shard=partner)

    def send_spread(k, carried):
        spread_copy(lax.rem(across + k, ACROSS)).start()
        return carried

    lax.fori_loop(1, ACROSS, send_spread, 0)
    hand_copy(across).start()

    def wait_source(k, carried):
        frm = lax.rem(shard + k, shards)
        source_copy(frm, frm).wait_recv()
        return carried

    lax.fori_loop(1, shards, wait_source, 0)
    pick[...] = picked(source_index_ref[...], owned)
    for c in range(3):
        dense_own[c] = placed(srecv[:, c * block : (c + 1) * block].reshape(shards * block, 128))
    dense_own[3] = placed(tails(srecv))
    for i in range(4):
        passing.wait(i)
    parts, tail = load_packed(moved, owned)
    parts.append(tail)
    gradient = [dense_own[c] + parts[c] for c in range(4)]
    entity_wide = load_wide(entity_ref, slice(None), owned, last)
    fresh = updated(entity_wide, column_of(entity_state_ref, 0, owned), gradient)
    store_narrow(entity_new_ref, slice(None), fresh)

    def forward(k, carried):
        frm = lax.rem(across + k, ACROSS)
        spread_wait(frm).wait_recv()
        hand_copy(frm).start()
        return carried

    lax.fori_loop(1, ACROSS, forward, 0)

    def put_out(which, ref):
        def turn(q, carried):
            got, tail_ = load_packed(ref.at[q], rb)
            store_narrow(relation_new_ref, half_block(which, q), (*got, tail_))
            return carried

        lax.fori_loop(0, ACROSS, turn, 0)

    put_out(core, r4)

    def take_hand(q, carried):
        hand_copy(q).wait_recv()
        return carried

    lax.fori_loop(0, ACROSS, take_hand, 0)
    put_out(1 - core, r5)

    for stage in range(3):
        def end_target(k, carried, stage=stage):
            to = lax.rem(shard + k, shards)
            target_copy(stage, to, shard).wait_send()
            return carried

        lax.fori_loop(1, shards, end_target, 0)
    passing.end()

    def end_shard(k, carried):
        source_copy(lax.rem(shard + k, shards), shard).wait_send()
        return carried

    def end_across(k, carried):
        to = lax.rem(across + k, ACROSS)
        across_copy(to, across).wait_send()
        spread_copy(to).wait_send()
        return carried

    def end_member(k, carried):
        to = lax.rem(place + k, members)
        member_copy(to, place).wait_send()
        share_copy(to, place).wait_send()
        return carried

    def end_hand(q, carried):
        hand_copy(q).wait_send()
        return carried

    lax.fori_loop(1, shards, end_shard, 0)
    lax.fori_loop(1, ACROSS, end_across, 0)
    lax.fori_loop(1, members, end_member, 0)
    lax.fori_loop(0, ACROSS, end_hand, 0)
    pair.wait_send()


def front_part(
    sizes, team,
    entity_ref, relation_ref, source_index_ref, target_index_ref, edge_source_ref, edge_relation_ref,
    table_ref, heads_ref, rels_ref, queries_ref, moved_index_ref,
    esend, evia, erecv, isend, irecv, eparts, rparts, sparts, pick, ssend, srecv, tsend, trecv, values, last,
    e_s, e_r, e_v, e_h, i_s, i_r, s_s, s_r, t_s, t_r,
):
    shards, groups, block, owned, width = sizes
    shard, group = lax.axis_index("shard"), lax.axis_index("group")
    before = lax.rem(group + groups - 1, groups)
    edges, padded = edge_source_ref.shape[1], relation_ref.shape[0]
    table_rows = shards * block
    tile = 256
    stages = ((0, block), (block, block), (2 * block, packed_rows(block) - 2 * block))

    isend[...] = target_index_ref[...]
    wide = load_wide(entity_ref, slice(None), owned, last)
    for c in range(3):
        esend[c * owned : (c + 1) * owned] = wide[c]
    esend[3 * owned :] = pack_tail(wide[3])
    greet(shards, groups, shard, group, team)

    index_copy = remote(isend, irecv, i_s, i_r, group=before)
    index_copy.start()

    passing = Passing(groups, group, -1, owned, esend, evia, erecv, e_s, e_r, e_v, e_h)
    for i in range(4):
        passing.send(i)

    for c in range(4):
        for k, part in enumerate(split3(wide[c])):
            eparts[k, :, 128 * c : 128 * c + 128] = part

    def taken(parts, index_ref, t, count):
        ones = picked(index_ref[:, pl.ds(pl.multiple_of(t * tile, tile), tile)], count)
        p0, p1, p2 = (parts[k, :count] for k in range(3))
        return (mxu(ones, p0, TN) + mxu(ones, p1, TN)) + mxu(ones, p2, TN)

    def take_source(t, carried):
        value = taken(eparts, source_index_ref, t, owned)
        for j in range(tile // block):
            store_packed(ssend.at[t * (tile // block) + j], value[j * block : (j + 1) * block])
        return carried

    lax.fori_loop(0, table_rows // tile, take_source, 0)

    def source_copy(to, slot):
        return remote(ssend.at[to], srecv.at[slot], s_s.at[to], s_r.at[slot], shard=to)

    def send_source(k, carried):
        source_copy(lax.rem(shard + k, shards), shard).start()
        return carried

    lax.fori_loop(1, shards, send_source, 0)
    srecv[shard] = ssend[shard]
    passing.relay(0)
    passing.relay(1)

    step = 128 if padded % 128 == 0 else 32

    def split_relation(t, carried):
        rows = pl.ds(pl.multiple_of(t * step, step), step)
        for c, x in enumerate(load_wide(relation_ref, rows, step, last)):
            for k, part in enumerate(split3(x)):
                rparts[k, rows, 128 * c : 128 * c + 128] = part
        return carried

    lax.fori_loop(0, padded // step, split_relation, 0)
    passing.relay(2)
    passing.relay(3)

    def take_relation(t, carried):
        rels_ref[pl.ds(pl.multiple_of(t * tile, tile), tile)] = taken(rparts, edge_relation_ref, t, padded)
        return carried

    lax.fori_loop(0, edges // tile, take_relation, 0)

    index_copy.wait_recv()
    moved_index_ref[...] = irecv[...]
    pick[...] = picked(irecv[...], owned)

    def found(chunk):
        value = mxu(pick[...], jnp.concatenate(split3(chunk), axis=1), TN)
        return (value[:, :128] + value[:, 128:256]) + value[:, 256:]

    def target_copy(stage, to, slot):
        first, size = stages[stage]
        rows = pl.ds(first, size)
        return remote(
            tsend.at[to, rows], trecv.at[slot, rows], t_s.at[stage, to], t_r.at[stage, slot], shard=to
        )

    for stage in range(3):
        passing.wait(stage)
        if stage == 2:
            passing.wait(3)
        chunk = erecv[stage * owned : (stage + 1) * owned]
        tsend[:, stage * block : (stage + 1) * block] = found(chunk).reshape(shards, block, 128)
        if stage == 2:
            values[...] = found(unpack_tail(erecv[3 * owned :], owned))

            def pack_tails(p, carried):
                rows = pl.ds(pl.multiple_of(p * block, block), block)
                tsend[p, 3 * block :] = pack_tail(values[rows])
                return carried

            lax.fori_loop(0, shards, pack_tails, 0)

        def send_target(k, carried, stage=stage):
            target_copy(stage, lax.rem(shard + k, shards), shard).start()
            return carried

        lax.fori_loop(1, shards, send_target, 0)
    trecv[shard] = tsend[shard]

    def wait_source(k, carried):
        frm = lax.rem(shard + k, shards)
        source_copy(frm, frm).wait_recv()
        return carried

    lax.fori_loop(1, shards, wait_source, 0)

    def split_source(p, carried):
        rows = pl.ds(pl.multiple_of(p * block, block), block)
        parts, tail = load_packed(srecv.at[p], block)
        for c, x in enumerate((*parts, tail)):
            for k, part in enumerate(split3(x)):
                sparts[k, rows, 128 * c : 128 * c + 128] = part
        return carried

    lax.fori_loop(0, shards, split_source, 0)

    def make_queries(t, carried):
        rows = pl.ds(pl.multiple_of(t * tile, tile), tile)
        heads = taken(sparts, edge_source_ref, t, table_rows)
        heads_ref[rows] = heads
        queries_ref[rows] = product(heads, rels_ref[rows])
        return carried

    lax.fori_loop(0, edges // tile, make_queries, 0)

    for stage in range(3):
        def wait_target(k, carried, stage=stage):
            frm = lax.rem(shard + k, shards)
            target_copy(stage, frm, frm).wait_recv()
            return carried

        lax.fori_loop(1, shards, wait_target, 0)

    def put_table(p, carried):
        rows = pl.ds(pl.multiple_of(p * block, block), block)
        parts, tail = load_packed(trecv.at[p], block)
        for c, x in enumerate((*parts, tail)):
            table_ref[rows, 128 * c : 128 * c + 128] = x
        return carried

    lax.fori_loop(0, shards, put_table, 0)

    index_copy.wait_send()
    for stage in range(3):
        def end_target(k, carried, stage=stage):
            target_copy(stage, lax.rem(shard + k, shards), shard).wait_send()
            return carried

        lax.fori_loop(1, shards, end_target, 0)
    passing.end()

    def end_source(k, carried):
        source_copy(lax.rem(shard + k, shards), shard).wait_send()
        return carried

    lax.fori_loop(1, shards, end_source, 0)


def step_kernel(
    sizes,
    count_ref, entity_ref, entity_state_ref, relation_ref, relation_state_ref,
    source_index_ref, target_index_ref, edge_source_ref, edge_relation_ref, edge_target_ref, slots_ref,
    entity_new_ref, relation_new_ref, loss_ref,
    table, heads, rels, queries, query_grad, target_grad, moved_index,
    esend, evia, erecv, isend, irecv, eparts, rparts, tparts, query_parts, pick, ssend, srecv, tsend, trecv,
    values, last, part, times,
    trecv_back, srecv_back, via_back, moved, own,
    r0send, r0recv, r1, r1recv, r2, r2recv, r3, r3recv, r4, r5,
    *sems,
):
    shards, groups, block, owned, width = sizes
    chips = shards // 2
    shard, group = lax.axis_index("shard"), lax.axis_index("group")
    core, chip = lax.rem(shard, 2), lax.div(shard, 2)
    across, layer = lax.rem(group, ACROSS), lax.div(group, ACROSS)

    def member(m):
        return {"group": lax.div(m, chips) * ACROSS + across, "shard": 2 * lax.rem(m, chips) + core}

    team = (r2.shape[0], layer * chips + chip, member)
    front_part(
        sizes, team,
        entity_ref, relation_ref, source_index_ref, target_index_ref, edge_source_ref, edge_relation_ref,
        table, heads, rels, queries, moved_index,
        esend, evia, erecv, isend, irecv, eparts, rparts, tparts, pick, ssend, srecv, tsend, trecv,
        values, last,
        *sems[:10],
    )

    target_grad[...] = jnp.zeros_like(target_grad)
    table_rows = table.shape[0]
    tile = min(256, table_rows)

    def split_table(t, carried):
        rows = pl.ds(pl.multiple_of(t * tile, tile), tile)
        for k, piece in enumerate(split3(table[rows])):
            tparts[k, rows] = piece
        return carried

    lax.fori_loop(0, table_rows // tile, split_table, 0)

    def span_turn(span, carried):
        span_part(
            span, count_ref, edge_target_ref, slots_ref, queries, table,
            loss_ref, query_grad, target_grad, part, times, tparts, query_parts,
        )
        return carried

    lax.fori_loop(0, loss_ref.shape[0], span_turn, 0)

    back_part(
        sizes, team,
        target_grad, query_grad, heads, rels, edge_source_ref, edge_relation_ref,
        relation_ref, relation_state_ref, moved_index, source_index_ref, entity_ref, entity_state_ref,
        entity_new_ref, relation_new_ref,
        tsend, trecv_back, ssend, srecv_back, esend, via_back, moved, pick, values, rparts, part, last, own,
        r0send, r0recv, r1, r1recv, r2, r2recv, r3, r3recv, r4, r5,
        *sems[10:],
    )


def whole_step(sizes, *operands):
    shards, groups, block, owned, width = sizes
    relation, edge_target = operands[3], operands[9]
    padded, spans = relation.shape[0], edge_target.shape[0]
    edges, table_rows = spans * SPAN, shards * block
    members = shards // 2 * groups // ACROSS
    size = packed_rows(padded // (2 * ACROSS))
    piece = 8 * (-(-size // (8 * members)))
    f32, bf16 = jnp.float32, jnp.bfloat16
    blocks = pltpu.VMEM((shards, packed_rows(block), 128), f32)
    flat = pltpu.VMEM((packed_rows(owned), 128), f32)
    index = pltpu.VMEM((1, table_rows), jnp.int32)
    of_edges, of_table = pltpu.VMEM((edges, WIDE), f32), pltpu.VMEM((table_rows, WIDE), f32)
    half = pltpu.VMEM((ACROSS, size, 128), f32)
    pieces = pltpu.VMEM((members, piece, 128), f32)

    def dma(*shape):
        return [pltpu.SemaphoreType.DMA(shape), pltpu.SemaphoreType.DMA(shape)]

    in_vmem = pl.BlockSpec(memory_space=pltpu.VMEM)
    return pl.pallas_call(
        functools.partial(step_kernel, sizes),
        in_specs=[pl.BlockSpec(memory_space=pltpu.SMEM)] + [in_vmem] * (len(operands) - 1),
        out_specs=[in_vmem] * 3,
        out_shape=[
            jax.ShapeDtypeStruct((owned, width), f32),
            jax.ShapeDtypeStruct((padded, width), f32),
            jax.ShapeDtypeStruct((spans, 1, SPAN), f32),
        ],
        scratch_shapes=[
            of_table, of_edges, of_edges, of_edges, of_edges, of_table, index,
            flat, flat, flat, index, index,
            pltpu.VMEM((3, owned, WIDE), bf16),
            pltpu.VMEM((3, max(padded, edges), WIDE), bf16),
            pltpu.VMEM((3, table_rows, WIDE), bf16),
            pltpu.VMEM((3, SPAN, WIDE), bf16),
            pltpu.VMEM((owned, table_rows), bf16),
            blocks, blocks, blocks, blocks,
            pltpu.VMEM((table_rows, 128), f32),
            pltpu.VMEM((owned, 128), f32),
            pltpu.VMEM((max(padded, table_rows), WIDE), f32),
            pltpu.VMEM((table_rows, 1), f32),
            blocks, blocks, flat, flat,
            pltpu.VMEM((4, owned, 128), f32),
            half, half, half, half, pieces, pieces, pltpu.VMEM((piece, 128), f32), pieces, half, half,
            *dma(4), *dma(4), *dma(), *dma(shards), *dma(3, shards),
            *dma(3, shards), *dma(shards), *dma(4), *dma(4), *dma(), *dma(ACROSS),
            *dma(members), *dma(members), *dma(ACROSS), *dma(ACROSS),
        ],
        compiler_params=pltpu.CompilerParams(
            collective_id=0, has_side_effects=True, vmem_limit_bytes=67043328
        ),
        name="whole_step",
    )(*operands)


def on_device(
    entity,
    entity_state,
    relation,
    relation_state,
    src_send,
    dst_send,
    edge_source,
    edge_relation,
    edge_target,
    neg_slots,
    edge_count,
):
    width = entity.shape[1]
    owned = entity.shape[0]
    relations = relation.shape[0]
    peers, block = src_send.shape[1], src_send.shape[2]
    table_rows = peers * block
    edges = edge_source.shape[0]
    spans = edges // SPAN
    groups, shards = lax.axis_size("group"), lax.axis_size("shard")
    unit = max(8 * shards, 16 * ACROSS)
    padded = unit * (-(-relations // unit))

    relation_rows = jnp.pad(relation, ((0, padded - relations), (0, 0)))
    relation_states = jnp.pad(relation_state, (0, padded - relations), constant_values=1.0).reshape(1, padded)
    sizes = (shards, groups, block, owned, width)
    source_index = src_send.reshape(1, table_rows)
    edge_sources, edge_relations = edge_source.reshape(1, edges), edge_relation.reshape(1, edges)
    entity_new, relation_new, loss = whole_step(
        sizes,
        edge_count,
        entity,
        entity_state.reshape(1, owned),
        relation_rows,
        relation_states,
        source_index,
        dst_send.reshape(1, table_rows),
        edge_sources,
        edge_relations,
        edge_target.reshape(spans, 1, SPAN),
        neg_slots.reshape(spans, 1, neg_slots.shape[1]),
    )
    return entity_new, relation_new[:relations], loss.reshape(edges)


def solution(mesh):
    return jax.shard_map(
        on_device,
        mesh=mesh,
        in_specs=(
            P(("group", "shard"), None),
            P(("group", "shard")),
            P(),
            P(),
            P(("group", "shard"), None, None),
            P(("group", "shard"), None, None),
            P(("group", "shard")),
            P(("group", "shard")),
            P(("group", "shard")),
            P(("group", "shard"), None),
            P(("group", "shard")),
        ),
        out_specs=(P(("group", "shard"), None), P(), P(("group", "shard"))),
        check_vma=False,
    )
```

```python
import functools

import jax
import jax.numpy as jnp
from jax import lax
from jax.experimental import pallas as pl
from jax.experimental.pallas import tpu as pltpu
from jax.sharding import PartitionSpec as P

SPAN = 512
LEARN_RATE = 0.5
WIDE = 512
TAIL = 8
ACROSS = 4
MESH = pl.DeviceIdType.MESH

NT = (((1,), (1,)), ((), ()))
NN = (((1,), (0,)), ((), ()))
TN = (((0,), (0,)), ((), ()))


def split2(x):
    hi = x.astype(jnp.bfloat16)
    lo = (x - hi.astype(jnp.float32)).astype(jnp.bfloat16)
    return hi, lo


def split3(x):
    hi = x.astype(jnp.bfloat16)
    rest = x - hi.astype(jnp.float32)
    mid = rest.astype(jnp.bfloat16)
    lo = (rest - mid.astype(jnp.float32)).astype(jnp.bfloat16)
    return hi, mid, lo


def mxu(a, b, dims):
    return lax.dot_general(a, b, dims, preferred_element_type=jnp.float32)


def lane_of(x):
    return lax.broadcasted_iota(jnp.int32, x.shape, 1)


def widened(x0, x1, x2, x3):
    lane = lane_of(x0)
    imag = jnp.where(lane < 56, pltpu.roll(x1, 56, 1), pltpu.roll(x2, 56, 1))
    both = jnp.where(
        lane < 64, x1, jnp.where(lane < 120, pltpu.roll(x2, 120, 1), pltpu.roll(x3, 120, 1))
    )
    tail = jnp.where(lane < 8, pltpu.roll(x1, 64, 1), jnp.where(lane < 16, x3, 0.0))
    return x0, imag, both, tail


def narrowed(real, imag, both, tail):
    lane = lane_of(real)
    imag_on, both_on = pltpu.roll(imag, 72, 1), pltpu.roll(both, 8, 1)
    x1 = jnp.where(lane < 64, both, jnp.where(lane < 72, pltpu.roll(tail, 64, 1), imag_on))
    x2 = jnp.where(lane < 72, imag_on, both_on)
    return real, x1, x2, jnp.where(lane < 8, both_on, tail)


def load_wide(ref, rows, count, last):
    last[:count] = jnp.zeros((count, 128), jnp.float32)
    last[:count, :16] = ref[rows, 384:400]
    return widened(ref[rows, 0:128], ref[rows, 128:256], ref[rows, 256:384], last[:count])


def store_narrow(ref, rows, parts):
    x = narrowed(*parts)
    for c in range(3):
        ref[rows, 128 * c : 128 * c + 128] = x[c]
    ref[rows, 384:400] = x[3][:, :16]


def load_turned(ref):
    n = ref.shape[1]
    both = jnp.concatenate([ref[128:192], ref[328:392]], axis=0)
    tail = jnp.concatenate([ref[192:200], ref[392:400], jnp.zeros((112, n), jnp.float32)], axis=0)
    return ref[0:128].T, ref[200:328].T, both.T, tail.T


def store_turned(ref, parts):
    real, imag, both, tail = (x.T for x in parts)
    ref[0:128] = real
    ref[200:328] = imag
    ref[128:192], ref[328:392] = both[:64], both[64:]
    ref[192:200], ref[392:400] = tail[:8], tail[8:16]


def column_of(row_ref, first, count):
    n = row_ref.shape[1]
    lane = lax.broadcasted_iota(jnp.int32, (count, n), 1)
    own = lax.broadcasted_iota(jnp.int32, (count, n), 0) + first
    return jnp.sum(jnp.where(lane == own, row_ref[...], 0.0), axis=1, keepdims=True)


def swapped(x, half):
    lane = lax.broadcasted_iota(jnp.int32, x.shape, 1)
    if half == 64:
        return pltpu.roll(x, 64, 1), lane < half
    left, right = pltpu.roll(x, 128 - half, 1), pltpu.roll(x, half, 1)
    mixed = jnp.where(lane < half, left, jnp.where(lane < 2 * half, right, 0.0))
    return mixed, lane < half


def mixed_product(a, b, half, sign):
    other_a, low = swapped(a, half)
    other_b, _ = swapped(b, half)
    real = jnp.where(low, b, other_b)
    imag = jnp.where(low, -other_b, b)
    return a * real + sign * (other_a * imag)


def product_of(a, b, sign):
    ar, ai, br, bi = a[:, :128], a[:, 128:256], b[:, :128], b[:, 128:256]
    return jnp.concatenate(
        [
            ar * br - sign * (ai * bi),
            ai * br + sign * (ar * bi),
            mixed_product(a[:, 256:384], b[:, 256:384], 64, sign),
            mixed_product(a[:, 384:], b[:, 384:], TAIL, sign),
        ],
        axis=1,
    )


def product(a, b):
    return product_of(a, b, 1.0)


def conj_product(a, b):
    return product_of(a, b, -1.0)


def picked(index, count):
    rows = lax.broadcasted_iota(jnp.int32, (count, index.shape[1]), 0)
    return jnp.where(rows == index, 1.0, 0.0).astype(jnp.bfloat16)


def span_part(
    span, count_ref, target_ref, slots_ref, query_ref, table_ref,
    loss_ref, query_grad_ref, target_grad_ref,
    score_ref, times_ref, parts_ref, query_parts_ref,
):
    table_rows = table_ref.shape[0]
    tile = min(256, table_rows)
    tiles = table_rows // tile

    edges_here = pl.ds(pl.multiple_of(span * SPAN, SPAN), SPAN)

    for k, part in enumerate(split2(query_ref[edges_here])):
        query_parts_ref[k] = part

    edge = lax.broadcasted_iota(jnp.int32, (1, SPAN), 1) + span * SPAN
    live = jnp.where(edge < count_ref[0], 1.0, 0.0)
    target = target_ref[span]
    slots = slots_ref[pl.ds(span, 1)]

    def score_turn(t, carried):
        peak, pos = carried
        rows = pl.ds(pl.multiple_of(t * tile, tile), tile)
        t0, t1 = parts_ref[0, rows], parts_ref[1, rows]
        q0, q1 = query_parts_ref[0], query_parts_ref[1]
        score = (mxu(t0, q1, NT) + mxu(t1, q0, NT)) + mxu(t0, q0, NT)
        score_ref[rows] = score
        number = lax.broadcasted_iota(jnp.int32, (tile, 1), 0) + t * tile
        times = jnp.sum(jnp.where(slots == number, 1.0, 0.0), axis=1, keepdims=True)
        times_ref[rows] = times
        used = jnp.where(times > 0.0, score, -jnp.inf)
        peak = jnp.maximum(peak, jnp.max(used, axis=0, keepdims=True))
        pos = pos + jnp.sum(jnp.where(target == number, score, 0.0), axis=0, keepdims=True)
        return peak, pos

    start = (jnp.full((1, SPAN), -jnp.inf, jnp.float32), jnp.zeros((1, SPAN), jnp.float32))
    peak, pos = lax.fori_loop(0, tiles, score_turn, start)
    peak = jnp.maximum(peak, pos)

    def total_turn(t, total):
        rows = pl.ds(pl.multiple_of(t * tile, tile), tile)
        times = times_ref[rows]
        value = jnp.where(times > 0.0, times * jnp.exp(score_ref[rows] - peak), 0.0)
        score_ref[rows] = value
        return total + jnp.sum(value, axis=0, keepdims=True)

    total = lax.fori_loop(0, tiles, total_turn, jnp.exp(pos - peak))
    log_total = peak + jnp.log(total)
    loss_ref[span] = (log_total - pos) * live
    pos_grad = (jnp.exp(pos - log_total) - 1.0) * live
    scale = jnp.exp(peak - log_total) * live
    query_grad_ref[edges_here] = jnp.zeros((SPAN, WIDE), jnp.float32)

    def grad_turn(t, carried):
        rows = pl.ds(pl.multiple_of(t * tile, tile), tile)
        number = lax.broadcasted_iota(jnp.int32, (tile, 1), 0) + t * tile
        weight = score_ref[rows] * scale + jnp.where(target == number, pos_grad, 0.0)
        w0, w1 = split2(weight)
        t0, t1 = parts_ref[0, rows], parts_ref[1, rows]
        q0, q1 = query_parts_ref[0], query_parts_ref[1]
        query_grad_ref[edges_here] += (mxu(w0, t1, TN) + mxu(w1, t0, TN)) + mxu(w0, t0, TN)
        target_grad_ref[rows] += (mxu(w0, q1, NN) + mxu(w1, q0, NN)) + mxu(w0, q0, NN)
        return carried

    lax.fori_loop(0, tiles, grad_turn, 0)


def pack_tail(x):
    rows = x.shape[0]
    packed = []
    for first in range(0, rows, 64):
        total = x[first : first + 8]
        for k in range(1, min(8, (rows - first) // 8)):
            total = total + pltpu.roll(x[first + 8 * k : first + 8 * k + 8], 16 * k, 1)
        packed.append(total)
    return packed[0] if len(packed) == 1 else jnp.concatenate(packed, axis=0)


def unpack_tail(x, rows):
    lane = lax.broadcasted_iota(jnp.int32, (8, 128), 1)
    tiles = []
    for t in range(rows // 8):
        part = x[8 * (t // 8) : 8 * (t // 8) + 8]
        k = t % 8
        part = part if k == 0 else pltpu.roll(part, 128 - 16 * k, 1)
        tiles.append(jnp.where(lane < 16, part, 0.0))
    return tiles[0] if len(tiles) == 1 else jnp.concatenate(tiles, axis=0)


def packed_rows(rows):
    return 3 * rows + 8 * (-(-rows // 64))


def store_packed(ref, x):
    n = x.shape[0]
    for c in range(3):
        ref[c * n : (c + 1) * n] = x[:, 128 * c : 128 * c + 128]
    ref[3 * n :] = pack_tail(x[:, 384:])


def load_packed(ref, n):
    parts = [ref[c * n : (c + 1) * n] for c in range(3)]
    return parts, unpack_tail(ref[3 * n :], n)


def remote(src, dst, send, recv, **device):
    return pltpu.make_async_remote_copy(
        src_ref=src, dst_ref=dst, send_sem=send, recv_sem=recv, device_id=device, device_id_type=MESH
    )


def greet(shards, groups, shard, group, team=None):
    barrier = pltpu.get_barrier_semaphore()

    def near(k, carried):
        pl.semaphore_signal(
            barrier, inc=1, device_id={"shard": lax.rem(shard + k, shards)}, device_id_type=MESH
        )
        return carried

    def far(k, carried):
        pl.semaphore_signal(
            barrier, inc=1, device_id={"group": lax.rem(group + k, groups)}, device_id_type=MESH
        )
        return carried

    lax.fori_loop(1, shards, near, 0)
    lax.fori_loop(1, groups, far, 0)
    met = shards + groups - 2
    if team is not None:
        count, place, member = team

        def wide_signal(k, carried):
            pl.semaphore_signal(
                barrier, inc=1, device_id=member(lax.rem(place + k, count)), device_id_type=MESH
            )
            return carried

        lax.fori_loop(1, count, wide_signal, 0)
        met = met + count - 1
    pl.semaphore_wait(barrier, met)


class Passing:
    def __init__(self, groups, group, by, owned, rows_ref, via_ref, out_ref, sent, came, via_came, handed):
        layers = groups // ACROSS
        x, layer = lax.rem(group, ACROSS), lax.div(group, ACROSS)
        ahead = lax.rem(layer + by + layers, layers)
        first, last = (ACROSS - 1, 0) if by > 0 else (0, ACROSS - 1)
        self.x, self.first, self.last = x, first, last
        self.direct = lax.rem(group + by + groups, groups)
        self.over = (layer * ACROSS + last, ahead * ACROSS + first)
        self.final = (ahead * ACROSS + last, layer * ACROSS + last)
        rest = packed_rows(owned) - 2 * owned
        part = 8 * (rest // 16)
        self.pieces = ((0, owned), (owned, owned), (2 * owned, part), (2 * owned + part, rest - part))
        self.refs = (rows_ref, via_ref, out_ref)
        self.sems = (sent, came, via_came, handed)

    def copy(self, i, kind):
        rows = pl.ds(*self.pieces[i])
        rows_ref, via_ref, out_ref = self.refs
        sent, came, via_came, handed = self.sems
        if kind == "direct":
            return remote(rows_ref.at[rows], out_ref.at[rows], sent.at[i], came.at[i], group=self.direct)
        if kind == "over":
            return remote(
                rows_ref.at[rows], via_ref.at[rows], sent.at[i], via_came.at[i], group=self.over[i % 2]
            )
        return remote(via_ref.at[rows], out_ref.at[rows], handed.at[i], came.at[i], group=self.final[i % 2])

    def send(self, i):
        @pl.when(self.x != self.first)
        def _():
            self.copy(i, "direct").start()

        @pl.when(self.x == self.first)
        def _():
            self.copy(i, "over").start()

    def relay(self, i):
        @pl.when(self.x == (self.last if i % 2 == 0 else self.first))
        def _():
            self.copy(i, "over").wait_recv()
            self.copy(i, "final").start()

    def wait(self, i):
        self.copy(i, "direct").wait_recv()

    def end(self):
        for i in range(4):
            self.copy(i, "direct").wait_send()

            @pl.when(self.x == (self.last if i % 2 == 0 else self.first))
            def _():
                self.copy(i, "final").wait_send()


def back_part(
    sizes, team,
    target_ref, query_grad_ref, heads_ref, rels_ref, edge_source_ref, edge_relation_ref,
    relation_ref, relation_state_ref, moved_index_ref, source_index_ref, entity_ref, entity_state_ref,
    entity_new_ref, relation_new_ref,
    tsend, trecv, ssend, srecv, dense, via, moved, pick, values, grads, part_ref, last, dense_own,
    r0send, r0recv, r1, r1recv, r2, r2recv, r3, r3recv, r4, r5,
    t_s, t_r, s_s, s_r, p_s, p_r, p_v, p_h, r0_s, r0_r, r1_s, r1_r, r2_s, r2_r, r3_s, r3_r, r4_s, r4_r, r5_s, r5_r,
):
    shards, groups, block, owned, width = sizes
    chips = shards // 2
    shard, group = lax.axis_index("shard"), lax.axis_index("group")
    core, chip = lax.rem(shard, 2), lax.div(shard, 2)
    partner = shard + 1 - 2 * core
    rb = relation_ref.shape[0] // (2 * ACROSS)
    members = r2.shape[0]
    across, layer = lax.rem(group, ACROSS), lax.div(group, ACROSS)
    _, place, member = team
    stages = ((0, block), (block, block), (2 * block, packed_rows(block) - 2 * block))
    passing = Passing(groups, group, 1, owned, dense, via, moved, p_s, p_r, p_v, p_h)

    def pack_target(p, carried):
        rows = pl.ds(pl.multiple_of(p * block, block), block)
        store_packed(tsend.at[p], target_ref[rows])
        return carried

    lax.fori_loop(0, shards, pack_target, 0)

    def target_copy(stage, to, slot):
        first, size = stages[stage]
        rows = pl.ds(first, size)
        return remote(
            tsend.at[to, rows], trecv.at[slot, rows], t_s.at[stage, to], t_r.at[stage, slot], shard=to
        )

    for stage in range(3):
        def send_target(k, carried, stage=stage):
            to = lax.rem(shard + k, shards)
            target_copy(stage, to, shard).start()
            return carried

        lax.fori_loop(1, shards, send_target, 0)

    edges = query_grad_ref.shape[0]
    padded = relation_ref.shape[0]
    tile = 256
    half_rows = padded // 2
    put_tile = half_rows // 2 if half_rows % 32 == 0 else half_rows

    def half_block(which, q):
        return pl.ds(pl.multiple_of((which * ACROSS + q) * rb, rb), rb)

    def gradient_parts(other_ref):
        def turn(t, carried):
            rows = pl.ds(pl.multiple_of(t * tile, tile), tile)
            for k, part in enumerate(split2(conj_product(query_grad_ref[rows], other_ref[rows]))):
                grads[k, rows] = part
            return carried

        lax.fori_loop(0, edges // tile, turn, 0)

    def summed_rows(index_ref, first, count):
        number = lax.broadcasted_iota(jnp.int32, (count, edges), 0) + first
        ones = jnp.where(number == index_ref[...], 1.0, 0.0).astype(jnp.bfloat16)
        return mxu(ones, grads[1, :edges], NN) + mxu(ones, grads[0, :edges], NN)

    def half_sums(which):
        def turn(t, carried):
            first = pl.multiple_of(which * half_rows + t * put_tile, put_tile)
            part_ref[pl.ds(first, put_tile)] = summed_rows(edge_relation_ref, first, put_tile)
            return carried

        lax.fori_loop(0, half_rows // put_tile, turn, 0)

    gradient_parts(heads_ref)
    half_sums(1 - core)

    def pack_other(q, carried):
        store_packed(r0send.at[q], part_ref[half_block(1 - core, q)])
        return carried

    lax.fori_loop(0, ACROSS, pack_other, 0)
    pair = remote(r0send, r0recv, r0_s, r0_r, shard=partner)
    pair.start()
    half_sums(core)

    def pack_own(q, carried):
        store_packed(r1.at[q], part_ref[half_block(core, q)])
        return carried

    lax.fori_loop(0, ACROSS, pack_own, 0)
    trecv[shard] = tsend[shard]
    pick[...] = picked(moved_index_ref[...], owned)

    def placed(value):
        v0, v1 = split2(value)
        return mxu(pick[...], v1, NN) + mxu(pick[...], v0, NN)

    def tails(ref):
        def turn(p, carried):
            values[pl.ds(pl.multiple_of(p * block, block), block)] = unpack_tail(ref[p, 3 * block :], block)
            return carried

        lax.fori_loop(0, shards, turn, 0)
        return values[...]

    def pass_on(stage):
        def wait_target(k, carried):
            frm = lax.rem(shard + k, shards)
            target_copy(stage, frm, frm).wait_recv()
            return carried

        lax.fori_loop(1, shards, wait_target, 0)
        chunk = trecv[:, stage * block : (stage + 1) * block].reshape(shards * block, 128)
        dense[stage * owned : (stage + 1) * owned] = placed(chunk)
        if stage == 2:
            dense[3 * owned :] = pack_tail(placed(tails(trecv)))
        passing.send(stage)
        if stage == 2:
            passing.send(3)

    pass_on(0)
    pair.wait_recv()

    def add_pair(q, carried):
        r1[q] = r1[q] + r0recv[q]
        return carried

    lax.fori_loop(0, ACROSS, add_pair, 0)

    def across_copy(to, slot):
        return remote(
            r1.at[to], r1recv.at[slot], r1_s.at[to], r1_r.at[slot], group=layer * ACROSS + to
        )

    def send_across(k, carried):
        across_copy(lax.rem(across + k, ACROSS), across).start()
        return carried

    lax.fori_loop(1, ACROSS, send_across, 0)
    pass_on(1)
    passing.relay(0)

    gradient_parts(rels_ref)

    def put_source(t, carried):
        value = summed_rows(edge_source_ref, t * tile, tile)
        for j in range(tile // block):
            store_packed(ssend.at[t * (tile // block) + j], value[j * block : (j + 1) * block])
        return carried

    lax.fori_loop(0, shards * block // tile, put_source, 0)

    def source_copy(to, slot):
        return remote(ssend.at[to], srecv.at[slot], s_s.at[to], s_r.at[slot], shard=to)

    def send_source(k, carried):
        source_copy(lax.rem(shard + k, shards), shard).start()
        return carried

    lax.fori_loop(1, shards, send_source, 0)
    srecv[shard] = ssend[shard]
    passing.relay(1)
    pass_on(2)

    r2[...] = jnp.zeros_like(r2)

    def wait_across(k, carried):
        frm = lax.rem(across + k, ACROSS)
        across_copy(frm, frm).wait_recv()
        return carried

    lax.fori_loop(1, ACROSS, wait_across, 0)
    r1recv[across] = r1[across]
    total = (r1recv[0] + r1recv[1]) + (r1recv[2] + r1recv[3])
    size, piece = total.shape[0], r2.shape[1]
    for m in range(members):
        count = min(piece, size - m * piece)
        if count > 0:
            r2[m, :count] = total[m * piece : m * piece + count]

    def member_copy(to, slot):
        return remote(r2.at[to], r2recv.at[slot], r2_s.at[to], r2_r.at[slot], **member(to))

    def send_member(k, carried):
        member_copy(lax.rem(place + k, members), place).start()
        return carried

    def wait_member(k, carried):
        frm = lax.rem(place + k, members)
        member_copy(frm, frm).wait_recv()
        return carried

    lax.fori_loop(1, members, send_member, 0)
    passing.relay(2)
    passing.relay(3)
    r2recv[place] = r2[place]
    lax.fori_loop(1, members, wait_member, 0)
    r3[...] = jnp.sum(r2recv[...], axis=0)

    def share_copy(to, slot):
        return remote(r3, r3recv.at[slot], r3_s.at[to], r3_r.at[slot], **member(to))

    def send_share(k, carried):
        share_copy(lax.rem(place + k, members), place).start()
        return carried

    def wait_share(k, carried):
        frm = lax.rem(place + k, members)
        share_copy(frm, frm).wait_recv()
        return carried

    lax.fori_loop(1, members, send_share, 0)
    r3recv[place] = r3[...]
    lax.fori_loop(1, members, wait_share, 0)

    def updated(params_, state, gradient):
        squares = sum(jnp.sum(g * g, axis=1, keepdims=True) for g in gradient)
        root = jnp.sqrt(state + squares / width)
        return [p - LEARN_RATE * g / root for p, g in zip(params_, gradient)]

    summed = r3recv[...].reshape(members * piece, 128)
    gradient = [summed[c * rb : (c + 1) * rb] for c in range(3)]
    gradient.append(unpack_tail(summed[3 * rb : size], rb))
    state = column_of(relation_state_ref, (core * ACROSS + across) * rb, rb)
    fresh = updated(load_wide(relation_ref, half_block(core, across), rb, last), state, gradient)
    store_packed(r4.at[across], jnp.concatenate(fresh, axis=1))

    def spread_copy(to):
        return remote(
            r4.at[across], r4.at[across], r4_s.at[to], r4_r.at[across], group=layer * ACROSS + to
        )

    def spread_wait(frm):
        return remote(r4.at[frm], r4.at[frm], r4_s.at[frm], r4_r.at[frm], group=layer * ACROSS + frm)

    def hand_copy(q):
        return remote(r4.at[q], r5.at[q], r5_s.at[q], r5_r.at[q], shard=partner)

    def send_spread(k, carried):
        spread_copy(lax.rem(across + k, ACROSS)).start()
        return carried

    lax.fori_loop(1, ACROSS, send_spread, 0)
    hand_copy(across).start()

    def wait_source(k, carried):
        frm = lax.rem(shard + k, shards)
        source_copy(frm, frm).wait_recv()
        return carried

    lax.fori_loop(1, shards, wait_source, 0)
    pick[...] = picked(source_index_ref[...], owned)
    for c in range(3):
        dense_own[c] = placed(srecv[:, c * block : (c + 1) * block].reshape(shards * block, 128))
    dense_own[3] = placed(tails(srecv))
    for i in range(4):
        passing.wait(i)
    parts, tail = load_packed(moved, owned)
    parts.append(tail)
    gradient = [dense_own[c] + parts[c] for c in range(4)]
    entity_wide = load_turned(entity_ref)
    fresh = updated(entity_wide, column_of(entity_state_ref, 0, owned), gradient)
    store_turned(entity_new_ref, fresh)

    def forward(k, carried):
        frm = lax.rem(across + k, ACROSS)
        spread_wait(frm).wait_recv()
        hand_copy(frm).start()
        return carried

    lax.fori_loop(1, ACROSS, forward, 0)

    def put_out(which, ref):
        def turn(q, carried):
            got, tail_ = load_packed(ref.at[q], rb)
            store_narrow(relation_new_ref, half_block(which, q), (*got, tail_))
            return carried

        lax.fori_loop(0, ACROSS, turn, 0)

    put_out(core, r4)

    def take_hand(q, carried):
        hand_copy(q).wait_recv()
        return carried

    lax.fori_loop(0, ACROSS, take_hand, 0)
    put_out(1 - core, r5)

    for stage in range(3):
        def end_target(k, carried, stage=stage):
            to = lax.rem(shard + k, shards)
            target_copy(stage, to, shard).wait_send()
            return carried

        lax.fori_loop(1, shards, end_target, 0)
    passing.end()

    def end_shard(k, carried):
        source_copy(lax.rem(shard + k, shards), shard).wait_send()
        return carried

    def end_across(k, carried):
        to = lax.rem(across + k, ACROSS)
        across_copy(to, across).wait_send()
        spread_copy(to).wait_send()
        return carried

    def end_member(k, carried):
        to = lax.rem(place + k, members)
        member_copy(to, place).wait_send()
        share_copy(to, place).wait_send()
        return carried

    def end_hand(q, carried):
        hand_copy(q).wait_send()
        return carried

    lax.fori_loop(1, shards, end_shard, 0)
    lax.fori_loop(1, ACROSS, end_across, 0)
    lax.fori_loop(1, members, end_member, 0)
    lax.fori_loop(0, ACROSS, end_hand, 0)
    pair.wait_send()


def front_part(
    sizes, team,
    entity_ref, relation_ref, source_index_ref, edge_source_ref, edge_relation_ref,
    table_ref, heads_ref, rels_ref, queries_ref, moved_index_ref,
    esend, evia, erecv, isend, irecv, eparts, rparts, sparts, pick, ssend, srecv, tsend, trecv, values, last,
    e_s, e_r, e_v, e_h, i_s, i_r, s_s, s_r, t_s, t_r,
):
    shards, groups, block, owned, width = sizes
    shard, group = lax.axis_index("shard"), lax.axis_index("group")
    before = lax.rem(group + groups - 1, groups)
    edges, padded = edge_source_ref.shape[1], relation_ref.shape[0]
    table_rows = shards * block
    tile = 256
    stages = ((0, block), (block, block), (2 * block, packed_rows(block) - 2 * block))

    wide = load_turned(entity_ref)
    for c in range(3):
        esend[c * owned : (c + 1) * owned] = wide[c]
    esend[3 * owned :] = pack_tail(wide[3])
    greet(shards, groups, shard, group, team)

    index_copy = remote(isend, irecv, i_s, i_r, group=before)
    index_copy.start()

    passing = Passing(groups, group, -1, owned, esend, evia, erecv, e_s, e_r, e_v, e_h)
    for i in range(4):
        passing.send(i)

    for c in range(4):
        for k, part in enumerate(split3(wide[c])):
            eparts[k, :, 128 * c : 128 * c + 128] = part

    def taken(parts, index_ref, t, count):
        ones = picked(index_ref[:, pl.ds(pl.multiple_of(t * tile, tile), tile)], count)
        p0, p1, p2 = (parts[k, :count] for k in range(3))
        return (mxu(ones, p0, TN) + mxu(ones, p1, TN)) + mxu(ones, p2, TN)

    def take_source(t, carried):
        value = taken(eparts, source_index_ref, t, owned)
        for j in range(tile // block):
            store_packed(ssend.at[t * (tile // block) + j], value[j * block : (j + 1) * block])
        return carried

    lax.fori_loop(0, table_rows // tile, take_source, 0)

    def source_copy(to, slot):
        return remote(ssend.at[to], srecv.at[slot], s_s.at[to], s_r.at[slot], shard=to)

    def send_source(k, carried):
        source_copy(lax.rem(shard + k, shards), shard).start()
        return carried

    lax.fori_loop(1, shards, send_source, 0)
    srecv[shard] = ssend[shard]
    passing.relay(0)
    passing.relay(1)

    step = 128 if padded % 128 == 0 else 32

    def split_relation(t, carried):
        rows = pl.ds(pl.multiple_of(t * step, step), step)
        for c, x in enumerate(load_wide(relation_ref, rows, step, last)):
            for k, part in enumerate(split3(x)):
                rparts[k, rows, 128 * c : 128 * c + 128] = part
        return carried

    lax.fori_loop(0, padded // step, split_relation, 0)
    passing.relay(2)
    passing.relay(3)

    def take_relation(t, carried):
        rels_ref[pl.ds(pl.multiple_of(t * tile, tile), tile)] = taken(rparts, edge_relation_ref, t, padded)
        return carried

    lax.fori_loop(0, edges // tile, take_relation, 0)

    index_copy.wait_recv()
    moved_index_ref[...] = irecv[...]
    pick[...] = picked(irecv[...], owned)

    def found(chunk):
        value = mxu(pick[...], jnp.concatenate(split3(chunk), axis=1), TN)
        return (value[:, :128] + value[:, 128:256]) + value[:, 256:]

    def target_copy(stage, to, slot):
        first, size = stages[stage]
        rows = pl.ds(first, size)
        return remote(
            tsend.at[to, rows], trecv.at[slot, rows], t_s.at[stage, to], t_r.at[stage, slot], shard=to
        )

    for stage in range(3):
        passing.wait(stage)
        if stage == 2:
            passing.wait(3)
        chunk = erecv[stage * owned : (stage + 1) * owned]
        tsend[:, stage * block : (stage + 1) * block] = found(chunk).reshape(shards, block, 128)
        if stage == 2:
            values[...] = found(unpack_tail(erecv[3 * owned :], owned))

            def pack_tails(p, carried):
                rows = pl.ds(pl.multiple_of(p * block, block), block)
                tsend[p, 3 * block :] = pack_tail(values[rows])
                return carried

            lax.fori_loop(0, shards, pack_tails, 0)

        def send_target(k, carried, stage=stage):
            target_copy(stage, lax.rem(shard + k, shards), shard).start()
            return carried

        lax.fori_loop(1, shards, send_target, 0)
    trecv[shard] = tsend[shard]

    def wait_source(k, carried):
        frm = lax.rem(shard + k, shards)
        source_copy(frm, frm).wait_recv()
        return carried

    lax.fori_loop(1, shards, wait_source, 0)

    def split_source(p, carried):
        rows = pl.ds(pl.multiple_of(p * block, block), block)
        parts, tail = load_packed(srecv.at[p], block)
        for c, x in enumerate((*parts, tail)):
            for k, part in enumerate(split3(x)):
                sparts[k, rows, 128 * c : 128 * c + 128] = part
        return carried

    lax.fori_loop(0, shards, split_source, 0)

    def make_queries(t, carried):
        rows = pl.ds(pl.multiple_of(t * tile, tile), tile)
        heads = taken(sparts, edge_source_ref, t, table_rows)
        heads_ref[rows] = heads
        queries_ref[rows] = product(heads, rels_ref[rows])
        return carried

    lax.fori_loop(0, edges // tile, make_queries, 0)

    for stage in range(3):
        def wait_target(k, carried, stage=stage):
            frm = lax.rem(shard + k, shards)
            target_copy(stage, frm, frm).wait_recv()
            return carried

        lax.fori_loop(1, shards, wait_target, 0)

    def put_table(p, carried):
        rows = pl.ds(pl.multiple_of(p * block, block), block)
        parts, tail = load_packed(trecv.at[p], block)
        for c, x in enumerate((*parts, tail)):
            table_ref[rows, 128 * c : 128 * c + 128] = x
        return carried

    lax.fori_loop(0, shards, put_table, 0)

    index_copy.wait_send()
    for stage in range(3):
        def end_target(k, carried, stage=stage):
            target_copy(stage, lax.rem(shard + k, shards), shard).wait_send()
            return carried

        lax.fori_loop(1, shards, end_target, 0)
    passing.end()

    def end_source(k, carried):
        source_copy(lax.rem(shard + k, shards), shard).wait_send()
        return carried

    lax.fori_loop(1, shards, end_source, 0)


def step_kernel(
    sizes,
    count_ref, entity_ref, entity_state_ref, relation_ref, relation_state_ref,
    source_index_ref, target_index_ref, edge_source_ref, edge_relation_ref, edge_target_ref, slots_ref,
    entity_new_ref, relation_new_ref, loss_ref,
    table, heads, rels, queries, query_grad, target_grad, moved_index, source_index,
    esend, evia, erecv, isend, irecv, eparts, rparts, tparts, query_parts, pick, ssend, srecv, tsend, trecv,
    values, last, part, times,
    trecv_back, srecv_back, via_back, moved, own,
    r0send, r0recv, r1, r1recv, r2, r2recv, r3, r3recv, r4, r5,
    *sems,
):
    shards, groups, block, owned, width = sizes
    chips = shards // 2
    shard, group = lax.axis_index("shard"), lax.axis_index("group")
    core, chip = lax.rem(shard, 2), lax.div(shard, 2)
    across, layer = lax.rem(group, ACROSS), lax.div(group, ACROSS)

    def member(m):
        return {"group": lax.div(m, chips) * ACROSS + across, "shard": 2 * lax.rem(m, chips) + core}

    team = (r2.shape[0], layer * chips + chip, member)
    for r in range(shards // 2):
        both = slice(2 * block * r, 2 * block * (r + 1))
        source_index[:, both] = jnp.concatenate(
            [source_index_ref[2 * r : 2 * r + 1], source_index_ref[2 * r + 1 : 2 * r + 2]], axis=1
        )
        isend[:, both] = jnp.concatenate(
            [target_index_ref[2 * r : 2 * r + 1], target_index_ref[2 * r + 1 : 2 * r + 2]], axis=1
        )
    front_part(
        sizes, team,
        entity_ref, relation_ref, source_index, edge_source_ref, edge_relation_ref,
        table, heads, rels, queries, moved_index,
        esend, evia, erecv, isend, irecv, eparts, rparts, tparts, pick, ssend, srecv, tsend, trecv,
        values, last,
        *sems[:10],
    )

    target_grad[...] = jnp.zeros_like(target_grad)
    table_rows = table.shape[0]
    tile = min(256, table_rows)

    def split_table(t, carried):
        rows = pl.ds(pl.multiple_of(t * tile, tile), tile)
        for k, piece in enumerate(split2(table[rows])):
            tparts[k, rows] = piece
        return carried

    lax.fori_loop(0, table_rows // tile, split_table, 0)

    def span_turn(span, carried):
        span_part(
            span, count_ref, edge_target_ref, slots_ref, queries, table,
            loss_ref, query_grad, target_grad, part, times, tparts, query_parts,
        )
        return carried

    lax.fori_loop(0, loss_ref.shape[0], span_turn, 0)

    back_part(
        sizes, team,
        target_grad, query_grad, heads, rels, edge_source_ref, edge_relation_ref,
        relation_ref, relation_state_ref, moved_index, source_index, entity_ref, entity_state_ref,
        entity_new_ref, relation_new_ref,
        tsend, trecv_back, ssend, srecv_back, esend, via_back, moved, pick, values, rparts, part, last, own,
        r0send, r0recv, r1, r1recv, r2, r2recv, r3, r3recv, r4, r5,
        *sems[10:],
    )


def whole_step(sizes, *operands):
    shards, groups, block, owned, width = sizes
    relation, edge_target = operands[3], operands[9]
    padded, spans = relation.shape[0], edge_target.shape[0]
    edges, table_rows = spans * SPAN, shards * block
    members = shards // 2 * groups // ACROSS
    size = packed_rows(padded // (2 * ACROSS))
    piece = 8 * (-(-size // (8 * members)))
    f32, bf16 = jnp.float32, jnp.bfloat16
    blocks = pltpu.VMEM((shards, packed_rows(block), 128), f32)
    flat = pltpu.VMEM((packed_rows(owned), 128), f32)
    index = pltpu.VMEM((1, table_rows), jnp.int32)
    of_edges, of_table = pltpu.VMEM((edges, WIDE), f32), pltpu.VMEM((table_rows, WIDE), f32)
    half = pltpu.VMEM((ACROSS, size, 128), f32)
    pieces = pltpu.VMEM((members, piece, 128), f32)

    def dma(*shape):
        return [pltpu.SemaphoreType.DMA(shape), pltpu.SemaphoreType.DMA(shape)]

    in_vmem = pl.BlockSpec(memory_space=pltpu.VMEM)
    return pl.pallas_call(
        functools.partial(step_kernel, sizes),
        in_specs=[pl.BlockSpec(memory_space=pltpu.SMEM)] + [in_vmem] * (len(operands) - 1),
        out_specs=[in_vmem] * 3,
        out_shape=[
            jax.ShapeDtypeStruct((width, owned), f32),
            jax.ShapeDtypeStruct((padded, width), f32),
            jax.ShapeDtypeStruct((spans, 1, SPAN), f32),
        ],
        scratch_shapes=[
            of_table, of_edges, of_edges, of_edges, of_edges, of_table, index, index,
            flat, flat, flat, index, index,
            pltpu.VMEM((3, owned, WIDE), bf16),
            pltpu.VMEM((3, max(padded, edges), WIDE), bf16),
            pltpu.VMEM((3, table_rows, WIDE), bf16),
            pltpu.VMEM((3, SPAN, WIDE), bf16),
            pltpu.VMEM((owned, table_rows), bf16),
            blocks, blocks, blocks, blocks,
            pltpu.VMEM((table_rows, 128), f32),
            pltpu.VMEM((owned, 128), f32),
            pltpu.VMEM((max(padded, table_rows), WIDE), f32),
            pltpu.VMEM((table_rows, 1), f32),
            blocks, blocks, flat, flat,
            pltpu.VMEM((4, owned, 128), f32),
            half, half, half, half, pieces, pieces, pltpu.VMEM((piece, 128), f32), pieces, half, half,
            *dma(4), *dma(4), *dma(), *dma(shards), *dma(3, shards),
            *dma(3, shards), *dma(shards), *dma(4), *dma(4), *dma(), *dma(ACROSS),
            *dma(members), *dma(members), *dma(ACROSS), *dma(ACROSS),
        ],
        compiler_params=pltpu.CompilerParams(
            collective_id=0, has_side_effects=True, vmem_limit_bytes=67043328
        ),
        name="whole_step",
    )(*operands)


def on_device(
    entity,
    entity_state,
    relation,
    relation_state,
    src_send,
    dst_send,
    edge_source,
    edge_relation,
    edge_target,
    neg_slots,
    edge_count,
):
    width = entity.shape[1]
    owned = entity.shape[0]
    relations = relation.shape[0]
    peers, block = src_send.shape[1], src_send.shape[2]
    table_rows = peers * block
    edges = edge_source.shape[0]
    spans = edges // SPAN
    groups, shards = lax.axis_size("group"), lax.axis_size("shard")
    unit = max(8 * shards, 16 * ACROSS)
    padded = unit * (-(-relations // unit))

    relation_rows = jnp.pad(relation, ((0, padded - relations), (0, 0)))
    relation_states = jnp.pad(relation_state, (0, padded - relations), constant_values=1.0).reshape(1, padded)
    sizes = (shards, groups, block, owned, width)
    source_index = src_send.reshape(peers, block)
    edge_sources, edge_relations = edge_source.reshape(1, edges), edge_relation.reshape(1, edges)
    entity_new, relation_new, loss = whole_step(
        sizes,
        edge_count,
        entity.T,
        entity_state.reshape(1, owned),
        relation_rows,
        relation_states,
        source_index,
        dst_send.reshape(peers, block),
        edge_sources,
        edge_relations,
        edge_target.reshape(spans, 1, SPAN),
        neg_slots,
    )
    return entity_new.T, relation_new[:relations], loss.reshape(edges)


def solution(mesh):
    return jax.shard_map(
        on_device,
        mesh=mesh,
        in_specs=(
            P(("group", "shard"), None),
            P(("group", "shard")),
            P(),
            P(),
            P(("group", "shard"), None, None),
            P(("group", "shard"), None, None),
            P(("group", "shard")),
            P(("group", "shard")),
            P(("group", "shard")),
            P(("group", "shard"), None),
            P(("group", "shard")),
        ),
        out_specs=(P(("group", "shard"), None), P(), P(("group", "shard"))),
        check_vma=False,
    )
```
